8 devices in a mesh: data: 8 (over z, y, x, core).
Axes of the slice: x: 2, y: 2, z: 1, core: 2. Of those that a mesh axis runs over, the one named last changes fastest.
Arguments:
- h_a: bfloat16 [8192, 512], P('data')
- h_b: bfloat16 [8192, 512], P('data')
- w_one: bfloat16 [512, 2048], replicated
- w_two: bfloat16 [2048, 2048], replicated
- w_three: bfloat16 [2048, 2048], replicated
- gain_one: float32 [2048], replicated
- bias_one: float32 [2048], replicated
- gain_two: float32 [2048], replicated
- bias_two: float32 [2048], replicated
Outputs:
- output 1: float32 [], replicated
- output 2: float32 [512, 2048], replicated
- output 3: float32 [2048, 2048], replicated
- output 4: float32 [2048, 2048], replicated
- output 5: float32 [2048], replicated
- output 6: float32 [2048], replicated
- output 7: float32 [2048], replicated
- output 8: float32 [2048], replicated
All inputs are finite; a program needn't handle non-finite values.
Results may differ from the reference program's by a relative error of at most 0.001.
Values are sent between devices in bfloat16 or wider.
A program may use at most 1 GiB of HBM per device.

```python
import jax
import jax.numpy as jnp
from jax import lax

GROUP_DEVS = 8
ROWS_DEV = 1024
FEAT_DIM = 512
PROJ_DIM = 2048

ALL_ROWS = GROUP_DEVS * ROWS_DEV
BN_EPS = 1e-5
STD_EPS = 1e-4
INV_WEIGHT = 2.0
VAR_WEIGHT = 1.0
COV_WEIGHT = 2.0


def setup_inputs(seed: int = 0) -> dict:
    key_list = jax.random.split(jax.random.key(seed), 11)
    shard_shape = (GROUP_DEVS, ROWS_DEV, FEAT_DIM)
    stat_shape = (GROUP_DEVS, 1, FEAT_DIM)
    base_a = jax.random.normal(key_list[0], shard_shape, jnp.float32)
    base_b = 0.8 * base_a + 0.6 * jax.random.normal(key_list[1], shard_shape, jnp.float32)
    shard_off = 0.6 * jax.random.normal(key_list[2], stat_shape, jnp.float32)
    shard_scale = jnp.exp(0.3 * jax.random.normal(key_list[3], stat_shape, jnp.float32))
    h_a = ((base_a + shard_off) * shard_scale).reshape(ALL_ROWS, FEAT_DIM).astype(jnp.bfloat16)
    h_b = ((base_b + shard_off) * shard_scale).reshape(ALL_ROWS, FEAT_DIM).astype(jnp.bfloat16)
    w_one = (jax.random.normal(key_list[4], (FEAT_DIM, PROJ_DIM), jnp.float32) * FEAT_DIM ** -0.5).astype(jnp.bfloat16)
    w_two = (jax.random.normal(key_list[5], (PROJ_DIM, PROJ_DIM), jnp.float32) * PROJ_DIM ** -0.5).astype(jnp.bfloat16)
    w_three = (jax.random.normal(key_list[6], (PROJ_DIM, PROJ_DIM), jnp.float32) * (0.7 * PROJ_DIM ** -0.5)).astype(jnp.bfloat16)
    gain_one = 1.0 + 0.3 * jax.random.normal(key_list[7], (PROJ_DIM,), jnp.float32)
    bias_one = 0.3 * jax.random.normal(key_list[8], (PROJ_DIM,), jnp.float32)
    gain_two = 1.0 + 0.3 * jax.random.normal(key_list[9], (PROJ_DIM,), jnp.float32)
    bias_two = 0.3 * jax.random.normal(key_list[10], (PROJ_DIM,), jnp.float32)
    return {'h_a': h_a, 'h_b': h_b, 'w_one': w_one, 'w_two': w_two, 'w_three': w_three,
            'gain_one': gain_one, 'bias_one': bias_one, 'gain_two': gain_two, 'bias_two': bias_two}


def layer_forward(x_in, weight, gain_vec, bias_vec):
    pre_act = jnp.dot(x_in, weight, preferred_element_type=jnp.float32)
    centered = pre_act - jnp.mean(pre_act, axis=0)
    inv_std = lax.rsqrt(jnp.mean(centered * centered, axis=0) + BN_EPS)
    normed = centered * inv_std
    act_val = gain_vec * normed + bias_vec
    return jnp.maximum(act_val, 0.0).astype(jnp.bfloat16), normed, act_val, inv_std


def layer_backward(d_out, normed, act_val, inv_std, gain_vec):
    d_act = jnp.where(act_val > 0.0, d_out, 0.0)
    sum_d = jnp.sum(d_act, axis=0)
    sum_dn = jnp.sum(d_act * normed, axis=0)
    d_pre = inv_std * gain_vec * (d_act - sum_d / ALL_ROWS - normed * (sum_dn / ALL_ROWS))
    return d_pre.astype(jnp.bfloat16), sum_dn, sum_d


def view_forward(view_feats, w_one, w_two, w_three, gain_one, bias_one, gain_two, bias_two):
    hidden_one, normed_one, act_one, inv_one = layer_forward(view_feats, w_one, gain_one, bias_one)
    hidden_two, normed_two, act_two, inv_two = layer_forward(hidden_one, w_two, gain_two, bias_two)
    z_view = jnp.dot(hidden_two, w_three, preferred_element_type=jnp.float32).astype(jnp.bfloat16)
    return z_view, (hidden_one, normed_one, act_one, inv_one, hidden_two, normed_two, act_two, inv_two)


def branch_terms(z_view):
    z_float = z_view.astype(jnp.float32)
    centered = z_float - jnp.mean(z_float, axis=0)
    cov_mat = jnp.dot(centered.T, centered) / (ALL_ROWS - 1)
    diag_var = jnp.diagonal(cov_mat)
    std_vec = jnp.sqrt(diag_var + STD_EPS)
    off_diag = cov_mat - jnp.diag(diag_var)
    hinge_on = (std_vec < 1.0).astype(jnp.float32)
    term_val = VAR_WEIGHT * jnp.sum(jnp.maximum(1.0 - std_vec, 0.0)) + COV_WEIGHT * jnp.sum(off_diag * off_diag)
    grad_cov = 2.0 * COV_WEIGHT * off_diag - jnp.diag(VAR_WEIGHT * hinge_on / (2.0 * std_vec))
    grad_hat = grad_cov.astype(jnp.bfloat16).astype(jnp.float32)
    grad_z = (2.0 / (ALL_ROWS - 1)) * jnp.dot(centered, grad_hat)
    return term_val, grad_z


def view_backward(view_feats, d_z, saved, w_two, w_three, gain_one, gain_two):
    hidden_one, normed_one, act_one, inv_one, hidden_two, normed_two, act_two, inv_two = saved
    grad_three = jnp.dot(hidden_two.T, d_z, preferred_element_type=jnp.float32)
    d_hidden_two = jnp.dot(d_z, w_three.T, preferred_element_type=jnp.float32)
    d_pre_two, gain_grad_two, bias_grad_two = layer_backward(d_hidden_two, normed_two, act_two, inv_two, gain_two)
    grad_two = jnp.dot(hidden_one.T, d_pre_two, preferred_element_type=jnp.float32)
    d_hidden_one = jnp.dot(d_pre_two, w_two.T, preferred_element_type=jnp.float32)
    d_pre_one, gain_grad_one, bias_grad_one = layer_backward(d_hidden_one, normed_one, act_one, inv_one, gain_one)
    grad_one = jnp.dot(view_feats.T, d_pre_one, preferred_element_type=jnp.float32)
    return grad_one, grad_two, grad_three, gain_grad_one, bias_grad_one, gain_grad_two, bias_grad_two


def reference(h_a, h_b, w_one, w_two, w_three, gain_one, bias_one, gain_two, bias_two):
    z_a, saved_a = view_forward(h_a, w_one, w_two, w_three, gain_one, bias_one, gain_two, bias_two)
    z_b, saved_b = view_forward(h_b, w_one, w_two, w_three, gain_one, bias_one, gain_two, bias_two)
    term_a, grad_za = branch_terms(z_a)
    term_b, grad_zb = branch_terms(z_b)
    z_diff = z_a.astype(jnp.float32) - z_b.astype(jnp.float32)
    loss_val = INV_WEIGHT * jnp.sum(z_diff * z_diff) / ALL_ROWS + term_a + term_b
    d_inv = (2.0 * INV_WEIGHT / ALL_ROWS) * z_diff
    d_za = (grad_za + d_inv).astype(jnp.bfloat16)
    d_zb = (grad_zb - d_inv).astype(jnp.bfloat16)
    back_a = view_backward(h_a, d_za, saved_a, w_two, w_three, gain_one, gain_two)
    back_b = view_backward(h_b, d_zb, saved_b, w_two, w_three, gain_one, gain_two)
    summed = [part_a + part_b for part_a, part_b in zip(back_a, back_b)]
    return (loss_val, summed[0], summed[1], summed[2], summed[3], summed[4], summed[5], summed[6])
```

```python
import jax
import jax.numpy as jnp
from jax import lax
from jax.experimental import pallas as pl
from jax.experimental.pallas import tpu as pltpu
from jax.sharding import PartitionSpec as P

BN_EPS = 1e-5
STD_EPS = 1e-4
INV_WEIGHT = 2.0
VAR_WEIGHT = 1.0
COV_WEIGHT = 2.0
BLK = 256


F32 = jnp.float32
BF16 = jnp.bfloat16


def mm(a, b, dims):
    return lax.dot_general(a, b, (dims, ((), ())), preferred_element_type=F32)


class Topo:
    def __init__(self):
        idx = lax.axis_index('data')
        self.c = idx % 2
        self.x = (idx // 2) % 2
        self.y = idx // 4
        self.q = idx // 2


def swap(arr, bit):
    return lax.ppermute(arr, 'data', [(i, i ^ bit) for i in range(8)])


def pick(arr, bit):
    return lax.dynamic_index_in_dim(arr, bit, 0, keepdims=False)


def halve(arr, my_bit, link):
    got = swap(pick(arr, 1 - my_bit), link)
    return pick(arr, my_bit) + got


def double(part, my_bit, link):
    got = swap(part, link)
    return jnp.where(my_bit == 0, jnp.stack([part, got]), jnp.stack([got, part]))


def chip_sum(vec):
    vec = vec + swap(vec, 2)
    return vec + swap(vec, 4)


def gram_kernel(z_ref, o_ref, zt_ref):
    q = pl.program_id(0)
    p = pl.program_id(1)
    first = p < 8 - q
    i = jnp.where(first, q, 7 - q)
    j = jnp.where(first, q + p, p - 1)

    @pl.when(jnp.logical_or(p == 0, p == 8 - q))
    def _():
        zt_ref[...] = z_ref[:, pl.ds(pl.multiple_of(i * BLK, BLK), BLK)].T

    o_ref[0] = jnp.dot(zt_ref[...], z_ref[:, pl.ds(pl.multiple_of(j * BLK, BLK), BLK)],
                       preferred_element_type=F32)


def gram_upper(z):
    rows, dim = z.shape
    return pl.pallas_call(
        gram_kernel,
        grid=(4, 9),
        out_shape=jax.ShapeDtypeStruct((4, BLK, 9 * BLK), F32),
        in_specs=[pl.BlockSpec((rows, dim), lambda q, p: (0, 0), pipeline_mode=pl.Buffered(1))],
        out_specs=pl.BlockSpec((1, BLK, BLK), lambda q, p: (q, 0, p)),
        scratch_shapes=[pltpu.VMEM((BLK, rows), BF16)],
        compiler_params=pltpu.CompilerParams(dimension_semantics=("arbitrary", "arbitrary"),
                                             vmem_limit_bytes=48 << 20),
        cost_estimate=pl.CostEstimate(flops=36 * 2 * BLK * BLK * rows, bytes_accessed=18 << 20, transcendentals=0),
    )(z)


def reduce_scatter_chips(part, t):
    w = part.shape[-1]
    half = BLK // 2
    xs = part[:, :, :half].transpose(1, 0, 2, 3)
    ys = part[:, :, half:]
    xs = halve(halve(xs, t.x, 2), t.y, 4)
    ys = halve(halve(ys, t.y, 4), t.x, 2)
    return xs, ys


def gather_chips(xs, ys, t):
    xs = double(double(xs, t.y, 4), t.x, 2)
    ys = double(double(ys, t.x, 2), t.y, 4)
    return xs, ys


def all_reduce_group(p, t):
    rows, w = p.shape
    h = halve(p.reshape(2, rows // 2, w), t.c, 1)
    e = rows // 16
    xs = h[:rows // 4].reshape(2, 2, e, w)
    ys = h[rows // 4:].reshape(2, 2, e, w)
    xs = halve(halve(xs, t.x, 2), t.y, 4)
    ys = halve(halve(ys, t.y, 4), t.x, 2)
    xs = double(double(xs, t.y, 4), t.x, 2).reshape(rows // 4, w)
    ys = double(double(ys, t.x, 2), t.y, 4).reshape(rows // 4, w)
    full = double(jnp.concatenate([xs, ys]), t.c, 1)
    return full.reshape(rows, w)


def layer_forward(x_in, weight, gain, bias, all_rows):
    u = mm(x_in, weight, ((1,), (0,)))
    sums = chip_sum(jnp.stack([jnp.sum(u, axis=0), jnp.sum(u * u, axis=0)]))
    mean = sums[0] / all_rows
    var = sums[1] / all_rows - mean * mean
    inv = lax.rsqrt(var + BN_EPS)
    return u, mean, inv


def normed_of(u, mean, inv):
    return (u - mean) * inv


def act_of(u, mean, inv, gain, bias):
    return gain * normed_of(u, mean, inv) + bias


def layer_backward(d_out, u, mean, inv, gain, bias, all_rows):
    n = normed_of(u, mean, inv)
    d_act = jnp.where(gain * n + bias > 0.0, d_out, 0.0)
    sums = chip_sum(jnp.stack([jnp.sum(d_act, axis=0), jnp.sum(d_act * n, axis=0)]))
    d_pre = inv * gain * (d_act - sums[0] / all_rows - n * (sums[1] / all_rows))
    both = sums + swap(sums, 1)
    return d_pre.astype(BF16), both[1], both[0]


def assemble(g4):
    rows = []
    for i in range(8):
        if i < 4:
            piece = g4[i, :, :(8 - i) * BLK]
        else:
            piece = g4[7 - i, :, (i + 1) * BLK:]
        rows.append(jnp.pad(piece, ((0, 0), (i * BLK, 0))))
    upper = jnp.concatenate(rows)
    dim = upper.shape[0]
    r = lax.broadcasted_iota(jnp.int32, (dim, dim), 0)
    k = lax.broadcasted_iota(jnp.int32, (dim, dim), 1)
    return jnp.where(r <= k, upper, upper.T)


def solution(mesh):
    group_devs = mesh.shape['data']

    def local_step(h_a, h_b, w_one, w_two, w_three, gain_one, bias_one, gain_two, bias_two):
        t = Topo()
        all_rows = h_a.shape[0] * group_devs
        rows = h_a.shape[0]
        dim = w_two.shape[0]
        is_a = t.c == 0
        keep = jnp.where(is_a, h_a, h_b)
        got = swap(jnp.where(is_a, h_b, h_a), 1)
        h = jnp.concatenate([keep, got])

        u1, m1, r1 = layer_forward(h, w_one, gain_one, bias_one, all_rows)
        x1 = jnp.maximum(act_of(u1, m1, r1, gain_one, bias_one), 0.0).astype(BF16)
        u2, m2, r2 = layer_forward(x1, w_two, gain_two, bias_two, all_rows)
        x2 = jnp.maximum(act_of(u2, m2, r2, gain_two, bias_two), 0.0).astype(BF16)
        z = mm(x2, w_three, ((1,), (0,))).astype(BF16)
        z = lax.optimization_barrier(z)
        z_other = jnp.concatenate([swap(z[rows:], 1), swap(z[:rows], 1)])
        zf = z.astype(F32)
        col_sum = chip_sum(jnp.sum(zf, axis=0)[None])[0]
        mu = col_sum / all_rows
        z_diff = zf - z_other.astype(F32)
        sq_part = 0.5 * jnp.sum(z_diff * z_diff)

        gram = gram_upper(z)
        nchunk = 3
        wch = 9 * BLK // nchunk
        q = t.q
        mu8 = mu.reshape(8, BLK)
        mu_q = pick(mu8, q)
        mu_r = pick(mu8, 7 - q)
        loss_part = INV_WEIGHT * sq_part / all_rows
        pieces = []
        for ch in range(nchunk):
            part = gram[:, :, ch * wch:(ch + 1) * wch].reshape(2, 2, BLK, wch)
            xs, ys = reduce_scatter_chips(part, t)
            outs = []
            for off, blk in ((0, xs), (BLK // 2, ys)):
                r_in = lax.broadcasted_iota(jnp.int32, blk.shape, 0) + off
                k_in = lax.broadcasted_iota(jnp.int32, blk.shape, 1) + ch * wch
                first = k_in < (8 - q) * BLK
                row_g = r_in + jnp.where(first, q, 7 - q) * BLK
                col_g = jnp.where(first, q * BLK + k_in, k_in - BLK)
                cols = []
                for b in range(wch // BLK):
                    p = ch * (wch // BLK) + b
                    cols.append(pick(mu8, jnp.where(p < 8 - q, q + p, p - 1)))
                mu_c = jnp.concatenate(cols)
                mu_rw = jnp.where(first, mu_q[off:off + BLK // 2][:, None], mu_r[off:off + BLK // 2][:, None])
                cov = (blk - all_rows * mu_rw * mu_c[None, :]) / (all_rows - 1)
                diag = row_g == col_g
                std = jnp.sqrt(jnp.where(diag, cov, 1.0) + STD_EPS)
                g_diag = -VAR_WEIGHT * (std < 1.0).astype(F32) / (2.0 * std)
                g = jnp.where(diag, g_diag, (2.0 * COV_WEIGHT) * cov)
                on_band = (row_g // BLK) == (col_g // BLK)
                weight = jnp.where(on_band, 1.0, 2.0) * COV_WEIGHT
                terms = jnp.where(diag, VAR_WEIGHT * jnp.maximum(1.0 - std, 0.0), weight * cov * cov)
                loss_part = loss_part + jnp.sum(terms)
                outs.append(g.astype(BF16))
            gx, gy = gather_chips(outs[0], outs[1], t)
            gx = gx.transpose(1, 0, 2, 3)
            pieces.append(jnp.concatenate([gx, gy], axis=2).reshape(4, BLK, wch))
        g_hat = assemble(jnp.concatenate(pieces, axis=2))
        loss_sum = loss_part[None]
        loss_sum = chip_sum(loss_sum)
        loss_val = (loss_sum + swap(loss_sum, 1))[0]

        mean_part = jnp.sum(mu[:, None] * g_hat.astype(F32), axis=0)
        d_inv = 2.0 * INV_WEIGHT / all_rows
        ngrp = 4
        wg = dim // ngrp
        d_z, grad_three = [], []
        for g in range(ngrp):
            s = slice(g * wg, (g + 1) * wg)
            rp = mm(z, g_hat[:, s], ((1,), (0,)))
            dz = ((2.0 / (all_rows - 1)) * (rp - mean_part[s]) + d_inv * z_diff[:, s]).astype(BF16)
            d_z.append(dz)
            grad_three.append(all_reduce_group(mm(x2, dz, ((0,), (0,))), t))
        d_z = jnp.concatenate(d_z, axis=1)
        d_x2 = mm(d_z, w_three, ((1,), (1,)))
        d_u2, gg2, gb2 = layer_backward(d_x2, u2, m2, r2, gain_two, bias_two, all_rows)
        grad_two = [all_reduce_group(mm(x1, d_u2[:, g * wg:(g + 1) * wg], ((0,), (0,))), t) for g in range(ngrp)]
        d_x1 = mm(d_u2, w_two, ((1,), (1,)))
        d_u1, gg1, gb1 = layer_backward(d_x1, u1, m1, r1, gain_one, bias_one, all_rows)
        grad_one = all_reduce_group(mm(h, d_u1, ((0,), (0,))), t)
        return (loss_val, grad_one, jnp.concatenate(grad_two, axis=1), jnp.concatenate(grad_three, axis=1),
                gg1, gb1, gg2, gb2)

    row_spec = P('data', None)
    return jax.shard_map(local_step, mesh=mesh,
                         in_specs=(row_spec, row_spec, P(), P(), P(), P(), P(), P(), P()),
                         out_specs=(P(), P(), P(), P(), P(), P(), P(), P()),
                         check_vma=False)
```

```python
import functools

import jax
import jax.numpy as jnp
from jax import lax
from jax.experimental import pallas as pl
from jax.experimental.pallas import tpu as pltpu
from jax.sharding import PartitionSpec as P

BN_EPS = 1e-5
STD_EPS = 1e-4
INV_WEIGHT = 2.0
VAR_WEIGHT = 1.0
COV_WEIGHT = 2.0
BLK = 256


F32 = jnp.float32
BF16 = jnp.bfloat16


def mm(a, b, dims):
    return lax.dot_general(a, b, (dims, ((), ())), preferred_element_type=F32)


class Topo:
    def __init__(self):
        idx = lax.axis_index('data')
        self.c = idx % 2
        self.x = (idx // 2) % 2
        self.y = idx // 4
        self.q = idx // 2


def swap(arr, bit):
    return lax.ppermute(arr, 'data', [(i, i ^ bit) for i in range(8)])


def pick(arr, bit):
    return lax.dynamic_index_in_dim(arr, bit, 0, keepdims=False)


def halve(arr, my_bit, link):
    got = swap(pick(arr, 1 - my_bit), link)
    return pick(arr, my_bit) + got


def double(part, my_bit, link):
    got = swap(part, link)
    return jnp.where(my_bit == 0, jnp.stack([part, got]), jnp.stack([got, part]))


def chip_sum(vec):
    vec = vec + swap(vec, 2)
    return vec + swap(vec, 4)


MESH_ID = pl.DeviceIdType.MESH


def remote(src, dst, send_sem, recv_sem, dev):
    return pltpu.make_async_remote_copy(src_ref=src, dst_ref=dst, send_sem=send_sem, recv_sem=recv_sem,
                                        device_id=(dev,), device_id_type=MESH_ID)


def meet(devs):
    barrier = pltpu.get_barrier_semaphore()
    for dev in devs:
        pl.semaphore_signal(barrier, inc=1, device_id=(dev,), device_id_type=MESH_ID)
    pl.semaphore_wait(barrier, len(devs))


def blk_ds(i):
    return pl.ds(pl.multiple_of(i * BLK, BLK), BLK)


def gram_kernel(all_rows, z_ref, mu_ref, muc_ref, gh_ref, mp_ref, loss_ref, zo_ref,
                zt, part, r1x, r1y, r2x, r2y, s2x, s2y, kx, ky, gb, ssem, rsem, zsem):
    idx = lax.axis_index('data')
    c, x, y, q = idx % 2, (idx // 2) % 2, idx // 4, idx // 2
    flip = lambda b: idx + b - 2 * b * ((idx // b) % 2)
    nc, nx, ny = flip(1), flip(2), flip(4)
    half = BLK // 2
    rows = z_ref.shape[0]
    lo, hi = pl.ds(0, half), pl.ds(half, half)

    meet((nc, nx, ny))
    z_out = [remote(z_ref.at[pl.ds(rows // 2, rows // 2)], zo_ref.at[pl.ds(0, rows // 2)], zsem.at[0], zsem.at[1], nc),
             remote(z_ref.at[pl.ds(0, rows // 2)], zo_ref.at[pl.ds(rows // 2, rows // 2)], zsem.at[2], zsem.at[3], nc)]
    for cp in z_out:
        cp.start()

    def band_of(o, p):
        first = p < 8 - o
        return jnp.where(first, o, 7 - o), jnp.where(first, o + p, p - 1)

    def s1(t):
        slot = t % 2
        return (remote(part.at[slot, :, 1 - x, lo, :], r1x.at[t], ssem.at[0, 0, t], rsem.at[0, 0, t], nx),
                remote(part.at[slot, 1 - y, :, hi, :], r1y.at[t], ssem.at[0, 1, t], rsem.at[0, 1, t], ny))

    def s2(t):
        slot = t % 2
        return (remote(s2x.at[slot], r2x.at[t], ssem.at[1, 0, t], rsem.at[1, 0, t], ny),
                remote(s2y.at[slot], r2y.at[t], ssem.at[1, 1, t], rsem.at[1, 1, t], nx))

    def a1(t):
        bx, by = gb.at[t, y, x, lo, :], gb.at[t, y, x, hi, :]
        return (remote(bx, bx, ssem.at[2, 0, t], rsem.at[2, 0, t], ny),
                remote(by, by, ssem.at[2, 1, t], rsem.at[2, 1, t], nx))

    def a2(t):
        bx, by = gb.at[t, :, x, lo, :], gb.at[t, y, :, hi, :]
        return (remote(bx, bx, ssem.at[3, 0, t], rsem.at[3, 0, t], nx),
                remote(by, by, ssem.at[3, 1, t], rsem.at[3, 1, t], ny))

    mp_ref[...] = jnp.zeros_like(mp_ref)
    loss_ref[...] = jnp.zeros_like(loss_ref)
    for o in range(4):
        zt[o] = z_ref[:, o * BLK:(o + 1) * BLK].T

    def body(t, carry):
        slot = t % 2
        old = (t + 1) % 2

        @pl.when(t < 9)
        def _():
            @pl.when(t >= 5)
            def _():
                zt[t - 1] = z_ref[:, blk_ds(t - 1)].T

            for o in range(4):
                i, j = band_of(o, t)
                part[slot, o // 2, o % 2] = jnp.dot(zt[i], z_ref[:, blk_ds(j)], preferred_element_type=F32)
            for cp in s1(t):
                cp.start()

        @pl.when(jnp.logical_and(t >= 1, t < 10))
        def _():
            g = t - 1
            for cp in s1(g):
                cp.wait()
            s2x[old] = part[old, 1 - y, x, lo, :] + r1x[g, 1 - y]
            s2y[old] = part[old, y, 1 - x, hi, :] + r1y[g, 1 - x]
            for cp in s2(g):
                cp.start()
            kx[old] = part[old, y, x, lo, :] + r1x[g, y]
            ky[old] = part[old, y, x, hi, :] + r1y[g, x]

        @pl.when(jnp.logical_and(t >= 2, t < 11))
        def _():
            g = t - 2
            for cp in s2(g):
                cp.wait()
            i, j = band_of(q, g)
            mu_j = mu_ref[:, blk_ds(j)]
            on_diag = i == j
            r_i = lax.broadcasted_iota(jnp.int32, (half, BLK), 0)
            k_i = lax.broadcasted_iota(jnp.int32, (half, BLK), 1)
            for off, k_ref, r_ref in ((0, kx, r2x), (half, ky, r2y)):
                mu_i = muc_ref[pl.ds(pl.multiple_of(i * BLK + off, half), half), :]
                cov = (k_ref[slot] + r_ref[g] - all_rows * (mu_i * mu_j)) / (all_rows - 1)
                diag = jnp.logical_and(r_i + off == k_i, on_diag)
                std = jnp.sqrt(jnp.where(diag, cov, 1.0) + STD_EPS)
                g_diag = jnp.where(std < 1.0, -VAR_WEIGHT, 0.0) / (2.0 * std)
                g_val = jnp.where(diag, g_diag, (2.0 * COV_WEIGHT) * cov)
                gb[g, y, x, pl.ds(off, half), :] = g_val.astype(BF16)
                weight = jnp.where(on_diag, COV_WEIGHT, 2.0 * COV_WEIGHT)
                terms = jnp.where(diag, VAR_WEIGHT * jnp.maximum(1.0 - std, 0.0), weight * cov * cov)
                loss_ref[...] += jnp.sum(terms, axis=0, keepdims=True)
            for cp in a1(g):
                cp.start()

        @pl.when(jnp.logical_and(t >= 3, t < 12))
        def _():
            for cp in a1(t - 3):
                cp.wait()
            for cp in a2(t - 3):
                cp.start()

        @pl.when(t >= 4)
        def _():
            g = t - 4
            for cp in a2(g):
                cp.wait()
            for o in range(4):
                i, j = band_of(o, g)
                blk = gb[g, o // 2, o % 2]
                gh_ref[blk_ds(i), blk_ds(j)] = blk
                mp_ref[:, blk_ds(j)] += jnp.sum(muc_ref[blk_ds(i), :] * blk.astype(F32), axis=0, keepdims=True)

                @pl.when(i != j)
                def _():
                    blk_t = gb[g, o // 2, o % 2].T
                    gh_ref[blk_ds(j), blk_ds(i)] = blk_t
                    mp_ref[:, blk_ds(i)] += jnp.sum(muc_ref[blk_ds(j), :] * blk_t.astype(F32), axis=0, keepdims=True)

        return carry

    lax.fori_loop(0, 13, body, 0)
    for cp in z_out:
        cp.wait()


def gram_exchange(z, mu, all_rows):
    rows, dim = z.shape
    vmem = pl.BlockSpec(memory_space=pltpu.VMEM)
    half = BLK // 2
    return pl.pallas_call(
        functools.partial(gram_kernel, all_rows),
        out_shape=(jax.ShapeDtypeStruct((dim, dim), BF16), jax.ShapeDtypeStruct((1, dim), F32),
                   jax.ShapeDtypeStruct((1, BLK), F32), jax.ShapeDtypeStruct((rows, dim), BF16)),
        in_specs=[vmem, vmem, vmem],
        out_specs=(vmem, vmem, vmem, pl.BlockSpec(memory_space=pl.ANY)),
        scratch_shapes=[
            pltpu.VMEM((8, BLK, rows), BF16),
            pltpu.VMEM((2, 2, 2, BLK, BLK), F32),
            pltpu.VMEM((9, 2, half, BLK), F32),
            pltpu.VMEM((9, 2, half, BLK), F32),
            pltpu.VMEM((9, half, BLK), F32),
            pltpu.VMEM((9, half, BLK), F32),
            pltpu.VMEM((2, half, BLK), F32),
            pltpu.VMEM((2, half, BLK), F32),
            pltpu.VMEM((2, half, BLK), F32),
            pltpu.VMEM((2, half, BLK), F32),
            pltpu.VMEM((9, 2, 2, BLK, BLK), BF16),
            pltpu.SemaphoreType.DMA((4, 2, 9)),
            pltpu.SemaphoreType.DMA((4, 2, 9)),
            pltpu.SemaphoreType.DMA((4,)),
        ],
        compiler_params=pltpu.CompilerParams(collective_id=1, has_side_effects=True, vmem_limit_bytes=60 << 20),
        cost_estimate=pl.CostEstimate(flops=36 * 2 * BLK * BLK * rows, bytes_accessed=30 << 20, transcendentals=0),
    )(z, mu.reshape(1, dim), mu.reshape(dim, 1))


def all_reduce_group(p, t):
    rows, w = p.shape
    h = halve(p.reshape(2, rows // 2, w), t.c, 1)
    e = rows // 16
    xs = h[:rows // 4].reshape(2, 2, e, w)
    ys = h[rows // 4:].reshape(2, 2, e, w)
    xs = halve(halve(xs, t.x, 2), t.y, 4)
    ys = halve(halve(ys, t.y, 4), t.x, 2)
    xs = double(double(xs, t.y, 4), t.x, 2).reshape(rows // 4, w)
    ys = double(double(ys, t.x, 2), t.y, 4).reshape(rows // 4, w)
    full = double(jnp.concatenate([xs, ys]), t.c, 1)
    return full.reshape(rows, w)


def layer_forward(x_in, weight, gain, bias, all_rows):
    u = mm(x_in, weight, ((1,), (0,)))
    sums = chip_sum(jnp.stack([jnp.sum(u, axis=0), jnp.sum(u * u, axis=0)]))
    mean = sums[0] / all_rows
    var = sums[1] / all_rows - mean * mean
    inv = lax.rsqrt(var + BN_EPS)
    return u, mean, inv


def normed_of(u, mean, inv):
    return (u - mean) * inv


def act_of(u, mean, inv, gain, bias):
    return gain * normed_of(u, mean, inv) + bias


def layer_backward(d_out, u, mean, inv, gain, bias, all_rows):
    n = normed_of(u, mean, inv)
    d_act = jnp.where(gain * n + bias > 0.0, d_out, 0.0)
    sums = chip_sum(jnp.stack([jnp.sum(d_act, axis=0), jnp.sum(d_act * n, axis=0)]))
    d_pre = inv * gain * (d_act - sums[0] / all_rows - n * (sums[1] / all_rows))
    both = sums + swap(sums, 1)
    return d_pre.astype(BF16), both[1], both[0]


def solution(mesh):
    group_devs = mesh.shape['data']

    def local_step(h_a, h_b, w_one, w_two, w_three, gain_one, bias_one, gain_two, bias_two):
        t = Topo()
        all_rows = h_a.shape[0] * group_devs
        rows = h_a.shape[0]
        dim = w_two.shape[0]
        is_a = t.c == 0
        keep = jnp.where(is_a, h_a, h_b)
        got = swap(jnp.where(is_a, h_b, h_a), 1)
        h = jnp.concatenate([keep, got])

        u1, m1, r1 = layer_forward(h, w_one, gain_one, bias_one, all_rows)
        x1 = jnp.maximum(act_of(u1, m1, r1, gain_one, bias_one), 0.0).astype(BF16)
        u2, m2, r2 = layer_forward(x1, w_two, gain_two, bias_two, all_rows)
        x2 = jnp.maximum(act_of(u2, m2, r2, gain_two, bias_two), 0.0).astype(BF16)
        z = mm(x2, w_three, ((1,), (0,))).astype(BF16)
        z = lax.optimization_barrier(z)
        col_sum = chip_sum(jnp.sum(z.astype(F32), axis=0)[None])[0]
        mu = col_sum / all_rows
        g_hat, mean_part, loss_vec, z_other = gram_exchange(z, mu, all_rows)
        mean_part = mean_part[0]
        z_diff = z.astype(F32) - z_other.astype(F32)
        sq_part = 0.5 * jnp.sum(z_diff * z_diff)
        loss_part = INV_WEIGHT * sq_part / all_rows + jnp.sum(loss_vec)
        loss_sum = loss_part[None]
        loss_sum = chip_sum(loss_sum)
        loss_val = (loss_sum + swap(loss_sum, 1))[0]

        d_inv = 2.0 * INV_WEIGHT / all_rows
        ngrp = 4
        wg = dim // ngrp
        d_z, grad_three = [], []
        for g in range(ngrp):
            s = slice(g * wg, (g + 1) * wg)
            rp = mm(z, g_hat[:, s], ((1,), (0,)))
            dz = ((2.0 / (all_rows - 1)) * (rp - mean_part[s]) + d_inv * z_diff[:, s]).astype(BF16)
            d_z.append(dz)
            grad_three.append(all_reduce_group(mm(x2, dz, ((0,), (0,))), t))
        d_z = jnp.concatenate(d_z, axis=1)
        d_x2 = mm(d_z, w_three, ((1,), (1,)))
        d_u2, gg2, gb2 = layer_backward(d_x2, u2, m2, r2, gain_two, bias_two, all_rows)
        grad_two = [all_reduce_group(mm(x1, d_u2[:, g * wg:(g + 1) * wg], ((0,), (0,))), t) for g in range(ngrp)]
        d_x1 = mm(d_u2, w_two, ((1,), (1,)))
        d_u1, gg1, gb1 = layer_backward(d_x1, u1, m1, r1, gain_one, bias_one, all_rows)
        grad_one = all_reduce_group(mm(h, d_u1, ((0,), (0,))), t)
        return (loss_val, grad_one, jnp.concatenate(grad_two, axis=1), jnp.concatenate(grad_three, axis=1),
                gg1, gb1, gg2, gb2)

    row_spec = P('data', None)
    return jax.shard_map(local_step, mesh=mesh,
                         in_specs=(row_spec, row_spec, P(), P(), P(), P(), P(), P(), P()),
                         out_specs=(P(), P(), P(), P(), P(), P(), P(), P()),
                         check_vma=False)
```

```python
import functools

import jax
import jax.numpy as jnp
from jax import lax
from jax.experimental import pallas as pl
from jax.experimental.pallas import tpu as pltpu
from jax.sharding import PartitionSpec as P

BN_EPS = 1e-5
STD_EPS = 1e-4
INV_WEIGHT = 2.0
VAR_WEIGHT = 1.0
COV_WEIGHT = 2.0
BLK = 256


F32 = jnp.float32
BF16 = jnp.bfloat16


def mm(a, b, dims):
    return lax.dot_general(a, b, (dims, ((), ())), preferred_element_type=F32)


class Topo:
    def __init__(self):
        idx = lax.axis_index('data')
        self.c = idx % 2
        self.x = (idx // 2) % 2
        self.y = idx // 4
        self.q = idx // 2


def swap(arr, bit):
    return lax.ppermute(arr, 'data', [(i, i ^ bit) for i in range(8)])


def chip_sum(vec):
    vec = vec + swap(vec, 2)
    return vec + swap(vec, 4)


MESH_ID = pl.DeviceIdType.MESH


def remote(src, dst, send_sem, recv_sem, dev):
    return pltpu.make_async_remote_copy(src_ref=src, dst_ref=dst, send_sem=send_sem, recv_sem=recv_sem,
                                        device_id=(dev,), device_id_type=MESH_ID)


def meet(devs):
    barrier = pltpu.get_barrier_semaphore()
    for dev in devs:
        pl.semaphore_signal(barrier, inc=1, device_id=(dev,), device_id_type=MESH_ID)
    pl.semaphore_wait(barrier, len(devs))


def blk_ds(i):
    return pl.ds(pl.multiple_of(i * BLK, BLK), BLK)


def gram_kernel(all_rows, z_ref, mu_ref, muc_ref, x2_hbm, x1_hbm, h_hbm, gh_ref, mp_ref, loss_ref, zo_ref,
                x2t_hbm, x1t_hbm, ht_hbm, tin, tout, tsem, zt, part, r1x, r1y, r2x, r2y, s2x, s2y, kx, ky, gb, ssem, rsem, zsem):
    idx = lax.axis_index('data')
    c, x, y, q = idx % 2, (idx // 2) % 2, idx // 4, idx // 2
    flip = lambda b: idx + b - 2 * b * ((idx // b) % 2)
    nc, nx, ny = flip(1), flip(2), flip(4)
    half = BLK // 2
    rows = z_ref.shape[0]
    lo, hi = pl.ds(0, half), pl.ds(half, half)

    meet((nc, nx, ny))
    z_out = [remote(z_ref.at[pl.ds(rows // 2, rows // 2)], zo_ref.at[pl.ds(0, rows // 2)], zsem.at[0], zsem.at[1], nc),
             remote(z_ref.at[pl.ds(0, rows // 2)], zo_ref.at[pl.ds(rows // 2, rows // 2)], zsem.at[2], zsem.at[3], nc)]
    for cp in z_out:
        cp.start()

    def band_of(o, p):
        first = p < 8 - o
        return jnp.where(first, o, 7 - o), jnp.where(first, o + p, p - 1)

    def s1(t):
        slot = t % 2
        return (remote(part.at[slot, :, 1 - x, lo, :], r1x.at[t], ssem.at[0, 0, t], rsem.at[0, 0, t], nx),
                remote(part.at[slot, 1 - y, :, hi, :], r1y.at[t], ssem.at[0, 1, t], rsem.at[0, 1, t], ny))

    def s2(t):
        slot = t % 2
        return (remote(s2x.at[slot], r2x.at[t], ssem.at[1, 0, t], rsem.at[1, 0, t], ny),
                remote(s2y.at[slot], r2y.at[t], ssem.at[1, 1, t], rsem.at[1, 1, t], nx))

    def a1(t):
        bx, by = gb.at[t, y, x, lo, :], gb.at[t, y, x, hi, :]
        return (remote(bx, bx, ssem.at[2, 0, t], rsem.at[2, 0, t], ny),
                remote(by, by, ssem.at[2, 1, t], rsem.at[2, 1, t], nx))

    def a2(t):
        bx, by = gb.at[t, :, x, lo, :], gb.at[t, y, :, hi, :]
        return (remote(bx, bx, ssem.at[3, 0, t], rsem.at[3, 0, t], nx),
                remote(by, by, ssem.at[3, 1, t], rsem.at[3, 1, t], ny))

    def band_copies(n):
        m = n % 2
        sets = ((n < 8, x2_hbm, x2t_hbm, n), (jnp.logical_and(n >= 8, n < 16), x1_hbm, x1t_hbm, n - 8),
                (jnp.logical_and(n >= 16, n < 18), h_hbm, ht_hbm, n - 16))
        return [(cond, pltpu.make_async_copy(src.at[:, blk_ds(b)], tin.at[m], tsem.at[0, m]),
                 pltpu.make_async_copy(tout.at[m], dst.at[blk_ds(b), :], tsem.at[1, m]))
                for cond, src, dst, b in sets]

    def band_do(n, what):
        for cond, load, store in band_copies(n):
            @pl.when(cond)
            def _():
                if what == 'load':
                    load.start()
                elif what == 'turn':
                    load.wait()
                else:
                    store.wait()
            if what == 'turn':
                @pl.when(cond)
                def _():
                    tout[n % 2] = tin[n % 2].T
                    store.start()

    mp_ref[...] = jnp.zeros_like(mp_ref)
    loss_ref[...] = jnp.zeros_like(loss_ref)
    for o in range(4):
        zt[o] = z_ref[:, o * BLK:(o + 1) * BLK].T

    def body(t, carry):
        slot = t % 2
        old = (t + 1) % 2
        band = 2 * (t - 1)

        @pl.when(jnp.logical_and(t >= 1, t < 10))
        def _():
            band_do(band, 'load')
            band_do(band + 1, 'load')

        @pl.when(t < 9)
        def _():
            @pl.when(t >= 5)
            def _():
                zt[t - 1] = z_ref[:, blk_ds(t - 1)].T

            for o in range(4):
                i, j = band_of(o, t)
                part[slot, o // 2, o % 2] = jnp.dot(zt[i], z_ref[:, blk_ds(j)], preferred_element_type=F32)
            for cp in s1(t):
                cp.start()

        @pl.when(jnp.logical_and(t >= 1, t < 10))
        def _():
            g = t - 1
            for cp in s1(g):
                cp.wait()
            s2x[old] = part[old, 1 - y, x, lo, :] + r1x[g, 1 - y]
            s2y[old] = part[old, y, 1 - x, hi, :] + r1y[g, 1 - x]
            for cp in s2(g):
                cp.start()
            kx[old] = part[old, y, x, lo, :] + r1x[g, y]
            ky[old] = part[old, y, x, hi, :] + r1y[g, x]

        @pl.when(jnp.logical_and(t >= 2, t < 11))
        def _():
            g = t - 2
            for cp in s2(g):
                cp.wait()
            i, j = band_of(q, g)
            mu_j = mu_ref[:, blk_ds(j)]
            on_diag = i == j
            r_i = lax.broadcasted_iota(jnp.int32, (half, BLK), 0)
            k_i = lax.broadcasted_iota(jnp.int32, (half, BLK), 1)
            for off, k_ref, r_ref in ((0, kx, r2x), (half, ky, r2y)):
                mu_i = muc_ref[pl.ds(pl.multiple_of(i * BLK + off, half), half), :]
                cov = (k_ref[slot] + r_ref[g] - all_rows * (mu_i * mu_j)) / (all_rows - 1)
                diag = jnp.logical_and(r_i + off == k_i, on_diag)
                std = jnp.sqrt(jnp.where(diag, cov, 1.0) + STD_EPS)
                g_diag = jnp.where(std < 1.0, -VAR_WEIGHT, 0.0) / (2.0 * std)
                g_val = jnp.where(diag, g_diag, (2.0 * COV_WEIGHT) * cov)
                gb[g, y, x, pl.ds(off, half), :] = g_val.astype(BF16)
                weight = jnp.where(on_diag, COV_WEIGHT, 2.0 * COV_WEIGHT)
                terms = jnp.where(diag, VAR_WEIGHT * jnp.maximum(1.0 - std, 0.0), weight * cov * cov)
                loss_ref[...] += jnp.sum(terms, axis=0, keepdims=True)
            for cp in a1(g):
                cp.start()

        @pl.when(jnp.logical_and(t >= 3, t < 12))
        def _():
            for cp in a1(t - 3):
                cp.wait()
            for cp in a2(t - 3):
                cp.start()

        @pl.when(jnp.logical_and(t >= 2, t < 11))
        def _():
            band_do(band - 2, 'stored')
            band_do(band - 1, 'stored')

        @pl.when(jnp.logical_and(t >= 1, t < 10))
        def _():
            band_do(band, 'turn')
            band_do(band + 1, 'turn')

        @pl.when(t >= 4)
        def _():
            g = t - 4
            for cp in a2(g):
                cp.wait()
            for o in range(4):
                i, j = band_of(o, g)
                blk = gb[g, o // 2, o % 2]
                gh_ref[blk_ds(i), blk_ds(j)] = blk
                mp_ref[:, blk_ds(j)] += jnp.sum(muc_ref[blk_ds(i), :] * blk.astype(F32), axis=0, keepdims=True)

                @pl.when(i != j)
                def _():
                    blk_t = gb[g, o // 2, o % 2].T
                    gh_ref[blk_ds(j), blk_ds(i)] = blk_t
                    mp_ref[:, blk_ds(i)] += jnp.sum(muc_ref[blk_ds(j), :] * blk_t.astype(F32), axis=0, keepdims=True)

        return carry

    lax.fori_loop(0, 13, body, 0)
    for cp in z_out:
        cp.wait()


def gram_exchange(z, mu, x2, x1, h, all_rows):
    rows, dim = z.shape
    vmem = pl.BlockSpec(memory_space=pltpu.VMEM)
    half = BLK // 2
    hbm = pl.BlockSpec(memory_space=pl.ANY)
    return pl.pallas_call(
        functools.partial(gram_kernel, all_rows),
        out_shape=(jax.ShapeDtypeStruct((dim, dim), BF16), jax.ShapeDtypeStruct((1, dim), F32),
                   jax.ShapeDtypeStruct((1, BLK), F32), jax.ShapeDtypeStruct((rows, dim), BF16),
                   jax.ShapeDtypeStruct((dim, rows), BF16), jax.ShapeDtypeStruct((dim, rows), BF16),
                   jax.ShapeDtypeStruct((h.shape[1], rows), BF16)),
        in_specs=[vmem, vmem, vmem, hbm, hbm, hbm],
        out_specs=(vmem, vmem, vmem, hbm, hbm, hbm, hbm),
        scratch_shapes=[
            pltpu.VMEM((2, rows, BLK), BF16),
            pltpu.VMEM((2, BLK, rows), BF16),
            pltpu.SemaphoreType.DMA((2, 2)),
            pltpu.VMEM((8, BLK, rows), BF16),
            pltpu.VMEM((2, 2, 2, BLK, BLK), F32),
            pltpu.VMEM((9, 2, half, BLK), F32),
            pltpu.VMEM((9, 2, half, BLK), F32),
            pltpu.VMEM((9, half, BLK), F32),
            pltpu.VMEM((9, half, BLK), F32),
            pltpu.VMEM((2, half, BLK), F32),
            pltpu.VMEM((2, half, BLK), F32),
            pltpu.VMEM((2, half, BLK), F32),
            pltpu.VMEM((2, half, BLK), F32),
            pltpu.VMEM((9, 2, 2, BLK, BLK), BF16),
            pltpu.SemaphoreType.DMA((4, 2, 9)),
            pltpu.SemaphoreType.DMA((4, 2, 9)),
            pltpu.SemaphoreType.DMA((4,)),
        ],
        compiler_params=pltpu.CompilerParams(collective_id=1, has_side_effects=True, vmem_limit_bytes=60 << 20),
        cost_estimate=pl.CostEstimate(flops=36 * 2 * BLK * BLK * rows, bytes_accessed=30 << 20, transcendentals=0),
    )(z, mu.reshape(1, dim), mu.reshape(dim, 1), x2, x1, h)


LAG = 2
SLOTS = 6 * LAG
LANE = 128
GROUPS = 36
TILE = 512


def backward_kernel(all_rows, z_hbm, zo_hbm, gh_hbm, x2t_hbm, x1t_hbm, ht_hbm, w3_hbm, w2_hbm, u2_hbm, u1_hbm,
                    mp_ref, vec2_ref, vec1_ref, lossv_ref,
                    out_hbm, part_hbm, grads_ref, loss_ref,
                    buf_a, buf_b, buf_c, ht, sb, wb, zb, ub, ps, own, r0, r1, r2, st, sr, tot, lacc,
                    ssem, rsem, lsem, dsem, psem, bsem, tsend, trecv):
    idx = lax.axis_index('data')
    c, x, y = idx % 2, (idx // 2) % 2, idx // 4
    bits = (c, x, y)

    def peer(d):
        dev = idx
        for b in range(3):
            if (d >> b) & 1:
                dev = dev + (1 << b) - (2 << b) * bits[b]
        return dev

    nc, nx, ny = peer(1), peer(2), peer(4)
    dim = buf_a.shape[1]
    rows = buf_a.shape[0]

    def rds(start, size):
        return pl.ds(pl.multiple_of(start, size), size)

    row_x, row_y = x * 256 + y * 128, 512 + y * 256 + x * 128

    def s0(g):
        k = g % SLOTS
        return (remote(part_hbm.at[g, rds((1 - c) * 1024, 1024)], r0.at[k], ssem.at[0, k], rsem.at[0, k], nc),)

    def load_own(g):
        k = g % SLOTS
        return pltpu.make_async_copy(part_hbm.at[g, rds(c * 1024, 1024)], own.at[k], lsem.at[0, k])

    def s1(g):
        k = g % SLOTS
        return (remote(own.at[k, rds((1 - x) * 256, 256)], r1.at[0, k], ssem.at[1, k], rsem.at[1, k], nx),
                remote(own.at[k, rds(512 + (1 - y) * 256, 256)], r1.at[1, k], ssem.at[2, k], rsem.at[2, k], ny))

    def s2(g):
        k = g % SLOTS
        return (remote(own.at[k, rds(x * 256 + (1 - y) * 128, 128)], r2.at[0, k], ssem.at[3, k], rsem.at[3, k], ny),
                remote(own.at[k, rds(512 + y * 256 + (1 - x) * 128, 128)], r2.at[1, k], ssem.at[4, k], rsem.at[4, k],
                       nx))

    def a1(g):
        k = g % SLOTS
        ox, oy = out_hbm.at[g, rds(c * 1024 + row_x, 128)], out_hbm.at[g, rds(c * 1024 + row_y, 128)]
        return (remote(own.at[k, rds(row_x, 128)], ox, ssem.at[5, k], rsem.at[5, k], ny),
                remote(own.at[k, rds(row_y, 128)], oy, ssem.at[6, k], rsem.at[6, k], nx),
                pltpu.make_async_copy(own.at[k, rds(row_x, 128)], ox, lsem.at[1, k]),
                pltpu.make_async_copy(own.at[k, rds(row_y, 128)], oy, lsem.at[2, k]))

    def a2(g):
        k = g % SLOTS
        bx, by = out_hbm.at[g, rds(c * 1024 + x * 256, 256)], out_hbm.at[g, rds(c * 1024 + 512 + y * 256, 256)]
        return (remote(bx, bx, ssem.at[7, k], rsem.at[7, k], nx), remote(by, by, ssem.at[8, k], rsem.at[8, k], ny))

    def a0(g):
        k = g % SLOTS
        b = out_hbm.at[g, rds(c * 1024, 1024)]
        return (remote(b, b, ssem.at[9, k], rsem.at[9, k], nc),)

    def stage(g, fn):
        @pl.when(jnp.logical_and(g >= 0, g < GROUPS))
        def _():
            fn(g)

    def wait_all(cps):
        for cp in cps:
            cp.wait()

    def start_all(cps):
        for cp in cps:
            cp.start()

    def to_a0(g):
        wait_all(a2(g))
        start_all(a0(g))

    def to_a2(g):
        wait_all(a1(g))
        start_all(a2(g))

    def to_a1(g):
        wait_all(s2(g))
        k = g % SLOTS
        own[k, rds(row_x, 128)] += r2[0, k]
        own[k, rds(row_y, 128)] += r2[1, k]
        start_all(a1(g))

    def to_s2(g):
        wait_all(s1(g))
        k = g % SLOTS
        own[k, rds(x * 256, 256)] += r1[0, k]
        own[k, rds(512 + y * 256, 256)] += r1[1, k]
        start_all(s2(g))

    def to_s1(g):
        wait_all(s0(g))
        load_own(g).wait()
        k = g % SLOTS
        own[k] += r0[k]
        start_all(s1(g))

    def to_s0(g):
        start_all(s0(g))
        load_own(g).start()

    def streams(n):
        slot = n % 2
        blk = n % 8
        return ((n < 8, (pltpu.make_async_copy(gh_hbm.at[:, blk_ds(blk)], sb.at[slot], dsem.at[0, slot]),
                         pltpu.make_async_copy(zo_hbm.at[:, blk_ds(blk)], zb.at[slot], dsem.at[1, slot]))),
                (jnp.logical_and(n >= 8, n < 24),
                 (pltpu.make_async_copy(w3_hbm.at[blk_ds(blk), :], wb.at[slot], dsem.at[0, slot]),
                  pltpu.make_async_copy(u2_hbm.at[:, blk_ds(blk)], ub.at[slot], dsem.at[1, slot]))),
                (jnp.logical_and(n >= 24, n < 40),
                 (pltpu.make_async_copy(w2_hbm.at[blk_ds(blk), :], wb.at[slot], dsem.at[0, slot]),
                  pltpu.make_async_copy(u1_hbm.at[:, blk_ds(blk)], ub.at[slot], dsem.at[1, slot]))))

    def start_streams(n):
        for cond, cps in streams(n):
            pl.when(cond)(functools.partial(start_all, cps))

    def wait_streams(n, which):
        wait_all(streams(n)[which][1])

    def part_writes(n):
        g = jnp.where(n < 8, 2 * n, 2 * n - 16)
        return tuple(pltpu.make_async_copy(ps.at[:, pl.ds(h * LANE, LANE)], part_hbm.at[g + h], psem.at[h])
                     for h in range(2))

    def part_writes_one(n):
        tile = 2 * (n - 32)
        return tuple(pltpu.make_async_copy(ps.at[pl.ds(0, 512), pl.ds(h * LANE, LANE)],
                                           part_hbm.at[32 + (tile + h) // 4, rds(((tile + h) % 4) * 512, 512)],
                                           psem.at[h]) for h in range(2))

    def loop_tiles(count, fn):
        def step(m, carry):
            fn(pl.ds(pl.multiple_of(m * TILE, TILE), TILE))
            return carry
        lax.fori_loop(0, count, step, 0)

    def nt(a, b):
        return lax.dot_general(a, b, (((1,), (1,)), ((), ())), preferred_element_type=F32)

    def piece_dz(n):
        slot, col = n % 2, blk_ds(n % 8)
        wait_streams(n, 0)
        start_streams(n + 1)

        def tile(r):
            rp = jnp.dot(buf_a[r, :], sb[slot], preferred_element_type=F32)
            zd = buf_a[r, col].astype(F32) - zb[slot, r, :].astype(F32)
            dz = (2.0 / (all_rows - 1)) * (rp - mp_ref[:, col]) + (2.0 * INV_WEIGHT / all_rows) * zd
            buf_c[r, col] = dz.astype(BF16)
            lacc[...] += jnp.sum(zd * zd, axis=0, keepdims=True)
        loop_tiles(rows // TILE, tile)

        @pl.when(n == 0)
        def _():
            big(1).wait()

        def grad(r):
            ps[r, :] = jnp.dot(buf_b[r, :], buf_c[:, col], preferred_element_type=F32)
        loop_tiles(dim // TILE, grad)
        start_all(part_writes(n))

    def d_act(d_ref, u_slot, r, vec_ref, col, slot):
        dx = nt(d_ref[r, :], wb[slot])
        nrm = (ub[slot, r, :] - vec_ref[0:1, col]) * vec_ref[1:2, col]
        act = vec_ref[2:3, col] * nrm + vec_ref[3:4, col]
        return jnp.where(act > 0.0, dx, 0.0), nrm

    def piece_stats(n, d_ref, vec_ref, layer, which):
        slot, col = n % 2, blk_ds(n % 8)
        wait_streams(n, which)
        start_streams(n + 1)
        st[layer, 0:2, col] = jnp.zeros((2, BLK), F32)

        def tile(r):
            da, nrm = d_act(d_ref, slot, r, vec_ref, col, slot)
            st[layer, 0:1, col] += jnp.sum(da, axis=0, keepdims=True)
            st[layer, 1:2, col] += jnp.sum(da * nrm, axis=0, keepdims=True)
        loop_tiles(rows // TILE, tile)

    def piece_du(n, d_ref, vec_ref, layer, which, du_ref):
        slot, col = n % 2, blk_ds(n % 8)
        wait_streams(n, which)
        start_streams(n + 1)

        def tile(r):
            da, nrm = d_act(d_ref, slot, r, vec_ref, col, slot)
            du = (vec_ref[1:2, col] * vec_ref[2:3, col]) * (
                da - tot[layer, 0:1, col] / all_rows - nrm * (tot[layer, 1:2, col] / all_rows))
            du_ref[r, col] = du.astype(BF16)
        loop_tiles(rows // TILE, tile)
        return col

    def stat_copies(layer):
        return tuple(remote(st.at[layer], sr.at[layer, idx], tsend.at[layer, d - 1], trecv.at[layer, d - 1], peer(d))
                     for d in range(1, 8))

    def send_stats(layer):
        start_all(stat_copies(layer))

    def finish_stats(layer):
        wait_all(stat_copies(layer))
        sr[layer, idx] = st[layer]
        va = (sr[layer, 0] + sr[layer, 2]) + (sr[layer, 4] + sr[layer, 6])
        vb = (sr[layer, 1] + sr[layer, 3]) + (sr[layer, 5] + sr[layer, 7])
        tot[layer] = jnp.where(c == 0, va, vb)
        grads_ref[layer] = va + vb

    def big(i):
        src = (z_hbm, x2t_hbm, x1t_hbm)[i]
        return pltpu.make_async_copy(src, (buf_a, buf_b, buf_a)[i], bsem.at[i])

    big(0).start()
    start_streams(0)
    big(1).start()
    ht_copy = pltpu.make_async_copy(ht_hbm, ht, bsem.at[3])
    ht_copy.start()
    lacc[...] = jnp.zeros_like(lacc)
    st[...] = jnp.zeros_like(st)
    meet([peer(d) for d in range(1, 8)])
    big(0).wait()

    def tick(it, carry):
        k = it - 1
        stage(k - 6 * LAG, lambda g: wait_all(a0(g)))
        stage(k - 5 * LAG, to_a0)
        stage(k - 4 * LAG, to_a2)
        stage(k - 3 * LAG, to_a1)
        stage(k - 2 * LAG, to_s2)
        stage(k - LAG, to_s1)

        @pl.when(jnp.logical_or(jnp.logical_and(it >= 1, it <= 8), jnp.logical_and(it >= 17, it <= 24)))
        def _():
            wait_all(part_writes(it - 1))

        @pl.when(jnp.logical_and(it >= 29, it <= 36))
        def _():
            wait_all(part_writes_one(it + 3))

        stage(k, to_s0)

        @pl.when(it < 8)
        def _():
            piece_dz(it)

        @pl.when(jnp.logical_and(it >= 8, it < 16))
        def _():
            @pl.when(it == 8)
            def _():
                big(2).start()

            piece_stats(it, buf_c, vec2_ref, 0, 1)

            @pl.when(it == 15)
            def _():
                st[0, 2:3, 0:BLK] = lossv_ref[...] + lacc[...] * (0.5 * INV_WEIGHT / all_rows)
                send_stats(0)

        @pl.when(jnp.logical_and(it >= 16, it < 24))
        def _():
            @pl.when(it == 16)
            def _():
                finish_stats(0)
                loss_ref[...] = jnp.broadcast_to(jnp.sum(grads_ref[0, 2:3, 0:BLK], axis=1, keepdims=True),
                                                 loss_ref.shape)
                big(2).wait()
                ht_copy.wait()

            col = piece_du(it, buf_c, vec2_ref, 0, 1, buf_b)

            def grad(r):
                ps[r, :] = jnp.dot(buf_a[r, :], buf_b[:, col], preferred_element_type=F32)
            loop_tiles(dim // TILE, grad)
            start_all(part_writes(it))

        @pl.when(jnp.logical_and(it >= 24, it < 28))
        def _():
            def two(m, carry):
                piece_stats(24 + 2 * (it - 24) + m, buf_b, vec1_ref, 1, 2)
                return carry
            lax.fori_loop(0, 2, two, 0)

            @pl.when(it == 27)
            def _():
                send_stats(1)

        @pl.when(jnp.logical_and(it >= 28, it < 36))
        def _():
            @pl.when(it == 28)
            def _():
                finish_stats(1)

            n = it + 4
            col = piece_du(n, buf_b, vec1_ref, 1, 2, buf_c)
            ps[0:512, :] = jnp.dot(ht[...], buf_c[:, col], preferred_element_type=F32)
            start_all(part_writes_one(n))

        return carry

    lax.fori_loop(0, GROUPS + 1 + 6 * LAG, tick, 0)


def backward(z, zo, gh, x2t, x1t, ht, w3, w2, u2, u1, mp, vec2, vec1, lossv, all_rows):
    rows, dim = z.shape
    feat = ht.shape[0]
    hbm = pl.BlockSpec(memory_space=pl.ANY)
    vmem = pl.BlockSpec(memory_space=pltpu.VMEM)
    dma = pltpu.SemaphoreType.DMA
    return pl.pallas_call(
        functools.partial(backward_kernel, all_rows),
        out_shape=(jax.ShapeDtypeStruct((GROUPS, dim, LANE), F32), jax.ShapeDtypeStruct((GROUPS, dim, LANE), F32),
                   jax.ShapeDtypeStruct((2, 4, dim), F32), jax.ShapeDtypeStruct((1, LANE), F32)),
        in_specs=[hbm] * 10 + [vmem] * 4,
        out_specs=(hbm, hbm, vmem, vmem),
        scratch_shapes=[
            pltpu.VMEM((rows, dim), BF16), pltpu.VMEM((rows, dim), BF16), pltpu.VMEM((rows, dim), BF16),
            pltpu.VMEM((feat, rows), BF16),
            pltpu.VMEM((2, dim, BLK), BF16), pltpu.VMEM((2, BLK, dim), BF16), pltpu.VMEM((2, rows, BLK), BF16),
            pltpu.VMEM((2, rows, BLK), F32), pltpu.VMEM((dim, BLK), F32),
            pltpu.VMEM((SLOTS, 1024, LANE), F32), pltpu.VMEM((SLOTS, 1024, LANE), F32),
            pltpu.VMEM((2, SLOTS, 256, LANE), F32), pltpu.VMEM((2, SLOTS, 128, LANE), F32),
            pltpu.VMEM((2, 4, dim), F32), pltpu.VMEM((2, 8, 4, dim), F32), pltpu.VMEM((2, 4, dim), F32),
            pltpu.VMEM((1, BLK), F32),
            dma((10, SLOTS)), dma((10, SLOTS)), dma((3, SLOTS)), dma((2, 2)), dma((2,)), dma((4,)),
            dma((2, 7)), dma((2, 7)),
        ],
        compiler_params=pltpu.CompilerParams(collective_id=2, has_side_effects=True, vmem_limit_bytes=67043328),
        cost_estimate=pl.CostEstimate(flops=150 * 10 ** 9, bytes_accessed=200 << 20, transcendentals=0),
    )(z, zo, gh, x2t, x1t, ht, w3, w2, u2, u1, mp, vec2, vec1, lossv)


def pairs_kernel(i_ref, o_ref):
    o_ref[:, :LANE] = i_ref[0]
    o_ref[:, LANE:] = i_ref[1]


def join_pairs(groups, first, dim):
    return pl.pallas_call(
        pairs_kernel,
        grid=(8,),
        out_shape=jax.ShapeDtypeStruct((dim, dim), F32),
        in_specs=[pl.BlockSpec((2, dim, LANE), lambda e: (first + e, 0, 0))],
        out_specs=pl.BlockSpec((dim, BLK), lambda e: (0, e)),
        compiler_params=pltpu.CompilerParams(dimension_semantics=("arbitrary",), vmem_limit_bytes=32 << 20),
        cost_estimate=pl.CostEstimate(flops=0, bytes_accessed=8 * dim * dim, transcendentals=0),
    )(groups)


def quads_kernel(i_ref, o_ref):
    for k in range(4):
        o_ref[:, k * LANE:(k + 1) * LANE] = i_ref[0, k * 512:(k + 1) * 512]


def join_quads(groups, first, dim):
    return pl.pallas_call(
        quads_kernel,
        grid=(4,),
        out_shape=jax.ShapeDtypeStruct((512, dim), F32),
        in_specs=[pl.BlockSpec((1, dim, LANE), lambda e: (first + e, 0, 0))],
        out_specs=pl.BlockSpec((512, 512), lambda e: (0, e)),
        compiler_params=pltpu.CompilerParams(dimension_semantics=("arbitrary",), vmem_limit_bytes=32 << 20),
        cost_estimate=pl.CostEstimate(flops=0, bytes_accessed=2 * dim * dim, transcendentals=0),
    )(groups)


def layer_forward(x_in, weight, gain, bias, all_rows):
    u = mm(x_in, weight, ((1,), (0,)))
    sums = chip_sum(jnp.stack([jnp.sum(u, axis=0), jnp.sum(u * u, axis=0)]))
    mean = sums[0] / all_rows
    var = sums[1] / all_rows - mean * mean
    inv = lax.rsqrt(var + BN_EPS)
    return u, mean, inv


def normed_of(u, mean, inv):
    return (u - mean) * inv


def act_of(u, mean, inv, gain, bias):
    return gain * normed_of(u, mean, inv) + bias


def solution(mesh):
    group_devs = mesh.shape['data']

    def local_step(h_a, h_b, w_one, w_two, w_three, gain_one, bias_one, gain_two, bias_two):
        t = Topo()
        all_rows = h_a.shape[0] * group_devs
        rows = h_a.shape[0]
        dim = w_two.shape[0]
        is_a = t.c == 0
        keep = jnp.where(is_a, h_a, h_b)
        got = swap(jnp.where(is_a, h_b, h_a), 1)
        h = jnp.concatenate([keep, got])

        u1, m1, r1 = layer_forward(h, w_one, gain_one, bias_one, all_rows)
        x1 = jnp.maximum(act_of(u1, m1, r1, gain_one, bias_one), 0.0).astype(BF16)
        u2, m2, r2 = layer_forward(x1, w_two, gain_two, bias_two, all_rows)
        x2 = jnp.maximum(act_of(u2, m2, r2, gain_two, bias_two), 0.0).astype(BF16)
        z = mm(x2, w_three, ((1,), (0,))).astype(BF16)
        z = lax.optimization_barrier(z)
        col_sum = chip_sum(jnp.sum(z.astype(F32), axis=0)[None])[0]
        mu = col_sum / all_rows
        g_hat, mean_part, loss_vec, z_other, x2t, x1t, ht = gram_exchange(z, mu, x2, x1, h, all_rows)
        stat2 = jnp.stack([m2, r2, gain_two, bias_two])
        stat1 = jnp.stack([m1, r1, gain_one, bias_one])
        groups, _, grads, loss = backward(z, z_other, g_hat, x2t, x1t, ht, w_three, w_two, u2, u1, mean_part, stat2,
                                          stat1, loss_vec, all_rows)
        return (loss[0, 0], join_quads(groups, 32, dim), join_pairs(groups, 8, dim), join_pairs(groups, 0, dim),
                grads[1, 1], grads[1, 0], grads[0, 1], grads[0, 0])

    row_spec = P('data', None)
    return jax.shard_map(local_step, mesh=mesh,
                         in_specs=(row_spec, row_spec, P(), P(), P(), P(), P(), P(), P()),
                         out_specs=(P(), P(), P(), P(), P(), P(), P(), P()),
                         check_vma=False)
```

```python
import functools

import jax
import jax.numpy as jnp
from jax import lax
from jax.experimental import pallas as pl
from jax.experimental.pallas import tpu as pltpu
from jax.sharding import PartitionSpec as P

BN_EPS = 1e-5
STD_EPS = 1e-4
INV_WEIGHT = 2.0
VAR_WEIGHT = 1.0
COV_WEIGHT = 2.0
BLK = 256

F32 = jnp.float32
BF16 = jnp.bfloat16


MESH_ID = pl.DeviceIdType.MESH


def remote(src, dst, send_sem, recv_sem, dev):
    return pltpu.make_async_remote_copy(src_ref=src, dst_ref=dst, send_sem=send_sem, recv_sem=recv_sem,
                                        device_id=(dev,), device_id_type=MESH_ID)


def meet(devs):
    barrier = pltpu.get_barrier_semaphore()
    for dev in devs:
        pl.semaphore_signal(barrier, inc=1, device_id=(dev,), device_id_type=MESH_ID)
    pl.semaphore_wait(barrier, len(devs))


def blk_ds(i):
    return pl.ds(pl.multiple_of(i * BLK, BLK), BLK)


def peer_of(idx, bits, d):
    dev = idx
    for b in range(3):
        if (d >> b) & 1:
            dev = dev + (1 << b) - (2 << b) * bits[b]
    return dev


def forward_kernel(all_rows, ha_hbm, hb_hbm, w1_ref, w2_hbm, w3_hbm, vec_ref,
                   h_hbm, u1_hbm, x1_hbm, u2_hbm, x2_hbm, z_hbm, stat1_ref, stat2_ref, zsum_ref,
                   hbuf, w2, w3, u, xb, zb, st, sr, hsem, wsem, usem, xsem, zsem, tsend, trecv):
    idx = lax.axis_index('data')
    c, x, y, q = idx % 2, (idx // 2) % 2, idx // 4, idx // 2
    bits = (c, x, y)
    nc = peer_of(idx, bits, 1)
    half = hbuf.shape[0] // 2
    dim = u.shape[1]
    tiles = [slice(0, half), slice(half, 2 * half)]

    def load_w(i):
        return pltpu.make_async_copy((w2_hbm, w3_hbm)[i], (w2, w3)[i], wsem.at[i])

    def views(what):
        for core, mine, other in ((0, ha_hbm, hb_hbm), (1, hb_hbm, ha_hbm)):
            @pl.when(c == core)
            def _():
                own = pltpu.make_async_copy(mine, hbuf.at[pl.ds(0, half)], hsem.at[0])
                sent = remote(other, hbuf.at[pl.ds(half, half)], hsem.at[1], hsem.at[2], nc)
                if what == 'own':
                    own.start()
                elif what == 'send':
                    sent.start()
                    own.wait()
                else:
                    sent.wait()

    views('own')
    load_w(0).start()
    meet([nc] + [peer_of(idx, bits, d) for d in (2, 4, 6)])
    views('send')
    load_w(1).start()

    def columns(fn):
        def step(nb, carry):
            fn(nb, blk_ds(nb))
            return carry
        lax.fori_loop(0, dim // BLK, step, 0)

    def add_sums(layer, m, col, val):
        sums = jnp.concatenate([jnp.sum(val, axis=0, keepdims=True), jnp.sum(val * val, axis=0, keepdims=True)])
        st[layer, :, col] = sums if m == 0 else st[layer, :, col] + sums

    def exchange(layer):
        return [remote(st.at[layer], sr.at[layer, q], tsend.at[layer, i], trecv.at[layer, i], peer_of(idx, bits, d))
                for i, d in enumerate((2, 4, 6))]

    def statistics(layer, stat_ref):
        cps = exchange(layer)
        for cp in cps:
            cp.start()
        sr[layer, q] = st[layer]
        for cp in cps:
            cp.wait()
        total = (sr[layer, 0] + sr[layer, 1]) + (sr[layer, 2] + sr[layer, 3])
        mean = total[0:1] / all_rows
        var = total[1:2] / all_rows - mean * mean
        stat_ref[0:1, :] = mean
        stat_ref[1:2, :] = lax.rsqrt(var + BN_EPS)
        stat_ref[2:4, :] = vec_ref[2 * layer:2 * layer + 2, :]

    def activate(stat_ref, m, col):
        nrm = (u[tiles[m], col] - stat_ref[0:1, col]) * stat_ref[1:2, col]
        xb[m, :, col] = jnp.maximum(stat_ref[2:3, col] * nrm + stat_ref[3:4, col], 0.0).astype(BF16)

    def u_out(layer, m):
        rows = pl.ds(m * half, half)
        return pltpu.make_async_copy(u.at[rows], (u1_hbm, u2_hbm)[layer].at[rows], usem.at[m])

    def x_out(layer, m):
        return pltpu.make_async_copy(xb.at[m], (x1_hbm, x2_hbm)[layer].at[pl.ds(m * half, half)], xsem.at[m])

    for m in range(2):
        if m == 1:
            views('got')

        def first(nb, col):
            val = jnp.dot(hbuf[tiles[m], :], w1_ref[:, col], preferred_element_type=F32)
            u[tiles[m], col] = val
            add_sums(0, m, col, val)
        columns(first)
        u_out(0, m).start()
    h_out = pltpu.make_async_copy(hbuf, h_hbm, hsem.at[3])
    h_out.start()
    statistics(0, stat1_ref)

    columns(lambda nb, col: activate(stat1_ref, 0, col))
    load_w(0).wait()
    for m in range(2):
        x_out(0, m).start()
        u_out(0, m).wait()

        def second(nb, col):
            val = jnp.dot(xb[m], w2[:, col], preferred_element_type=F32)
            if m == 0:
                activate(stat1_ref, 1, col)
            u[tiles[m], col] = val
            add_sums(1, m, col, val)
        columns(second)
        u_out(1, m).start()
    statistics(1, stat2_ref)

    x_out(0, 0).wait()
    x_out(0, 1).wait()
    columns(lambda nb, col: activate(stat2_ref, 0, col))
    load_w(1).wait()

    def z_out(m, nb):
        return pltpu.make_async_copy(zb.at[nb % 2], z_hbm.at[pl.ds(m * half, half), blk_ds(nb)], zsem.at[nb % 2])

    for m in range(2):
        x_out(1, m).start()

        def third(nb, col):
            val = jnp.dot(xb[m], w3[:, col], preferred_element_type=F32).astype(BF16)
            if m == 0:
                activate(stat2_ref, 1, col)

            @pl.when(nb >= 2)
            def _():
                z_out(m, nb - 2).wait()
            zb[nb % 2] = val
            sums = jnp.sum(val.astype(F32), axis=0, keepdims=True)
            zsum_ref[0:1, col] = sums if m == 0 else zsum_ref[0:1, col] + sums
            z_out(m, nb).start()
        columns(third)
        z_out(m, 6).wait()
        z_out(m, 7).wait()
    zsum_ref[1:2, :] = jnp.zeros((1, dim), F32)
    for m in range(2):
        u_out(1, m).wait()
        x_out(1, m).wait()
    h_out.wait()


def forward(h_a, h_b, w1, w2, w3, vec, all_rows):
    rows, feat = 2 * h_a.shape[0], h_a.shape[1]
    dim = w2.shape[0]
    hbm = pl.BlockSpec(memory_space=pl.ANY)
    vmem = pl.BlockSpec(memory_space=pltpu.VMEM)
    dma = pltpu.SemaphoreType.DMA
    shape = jax.ShapeDtypeStruct
    return pl.pallas_call(
        functools.partial(forward_kernel, all_rows),
        out_shape=(shape((rows, feat), BF16), shape((rows, dim), F32), shape((rows, dim), BF16),
                   shape((rows, dim), F32), shape((rows, dim), BF16), shape((rows, dim), BF16),
                   shape((4, dim), F32), shape((4, dim), F32), shape((2, dim), F32)),
        in_specs=[hbm, hbm, vmem, hbm, hbm, vmem],
        out_specs=(hbm,) * 6 + (vmem,) * 3,
        scratch_shapes=[
            pltpu.VMEM((rows, feat), BF16), pltpu.VMEM((dim, dim), BF16), pltpu.VMEM((dim, dim), BF16),
            pltpu.VMEM((rows, dim), F32), pltpu.VMEM((2, rows // 2, dim), BF16),
            pltpu.VMEM((2, rows // 2, BLK), BF16),
            pltpu.VMEM((2, 2, dim), F32), pltpu.VMEM((2, 4, 2, dim), F32),
            dma((4,)), dma((2,)), dma((2,)), dma((2,)), dma((2,)), dma((2, 3)), dma((2, 3)),
        ],
        compiler_params=pltpu.CompilerParams(collective_id=3, has_side_effects=True, vmem_limit_bytes=67043328),
        cost_estimate=pl.CostEstimate(flops=40 * 10 ** 9, bytes_accessed=90 << 20, transcendentals=0),
    )(h_a, h_b, w1, w2, w3, vec)


def gram_kernel(all_rows, z_ref, zsum_ref, x2_hbm, x1_hbm, h_hbm, gh_ref, mp_ref, loss_ref, zo_ref,
                x2t_hbm, x1t_hbm, ht_hbm, tin, tout, tsem, mu_ref, muc_ref, zsum_all, msend, mrecv, zt, part, r1x, r1y, r2x, r2y, s2x, s2y, kx, ky, gb, ssem, rsem, zsem):
    idx = lax.axis_index('data')
    c, x, y, q = idx % 2, (idx // 2) % 2, idx // 4, idx // 2
    flip = lambda b: idx + b - 2 * b * ((idx // b) % 2)
    nc, nx, ny = flip(1), flip(2), flip(4)
    half = BLK // 2
    rows = z_ref.shape[0]
    lo, hi = pl.ds(0, half), pl.ds(half, half)

    nd = flip(2) + 4 - 8 * y
    meet((nc, nx, ny, nd))
    sums_out = [remote(zsum_ref, zsum_all.at[q], msend.at[i], mrecv.at[i], dev) for i, dev in enumerate((nx, ny, nd))]
    for cp in sums_out:
        cp.start()
    zsum_all[q] = zsum_ref[...]
    z_out = [remote(z_ref.at[pl.ds(rows // 2, rows // 2)], zo_ref.at[pl.ds(0, rows // 2)], zsem.at[0], zsem.at[1], nc),
             remote(z_ref.at[pl.ds(0, rows // 2)], zo_ref.at[pl.ds(rows // 2, rows // 2)], zsem.at[2], zsem.at[3], nc)]
    for cp in z_out:
        cp.start()

    def band_of(o, p):
        first = p < 8 - o
        return jnp.where(first, o, 7 - o), jnp.where(first, o + p, p - 1)

    def s1(t):
        slot = t % 2
        return (remote(part.at[slot, :, 1 - x, lo, :], r1x.at[t], ssem.at[0, 0, t], rsem.at[0, 0, t], nx),
                remote(part.at[slot, 1 - y, :, hi, :], r1y.at[t], ssem.at[0, 1, t], rsem.at[0, 1, t], ny))

    def s2(t):
        slot = t % 2
        return (remote(s2x.at[slot], r2x.at[t], ssem.at[1, 0, t], rsem.at[1, 0, t], ny),
                remote(s2y.at[slot], r2y.at[t], ssem.at[1, 1, t], rsem.at[1, 1, t], nx))

    def a1(t):
        bx, by = gb.at[t, y, x, lo, :], gb.at[t, y, x, hi, :]
        return (remote(bx, bx, ssem.at[2, 0, t], rsem.at[2, 0, t], ny),
                remote(by, by, ssem.at[2, 1, t], rsem.at[2, 1, t], nx))

    def a2(t):
        bx, by = gb.at[t, :, x, lo, :], gb.at[t, y, :, hi, :]
        return (remote(bx, bx, ssem.at[3, 0, t], rsem.at[3, 0, t], nx),
                remote(by, by, ssem.at[3, 1, t], rsem.at[3, 1, t], ny))

    def band_copies(n):
        m = n % 2
        sets = ((n < 8, x2_hbm, x2t_hbm, n), (jnp.logical_and(n >= 8, n < 16), x1_hbm, x1t_hbm, n - 8),
                (jnp.logical_and(n >= 16, n < 18), h_hbm, ht_hbm, n - 16))
        return [(cond, pltpu.make_async_copy(src.at[:, blk_ds(b)], tin.at[m], tsem.at[0, m]),
                 pltpu.make_async_copy(tout.at[m], dst.at[blk_ds(b), :], tsem.at[1, m]))
                for cond, src, dst, b in sets]

    def band_do(n, what):
        for cond, load, store in band_copies(n):
            @pl.when(cond)
            def _():
                if what == 'load':
                    load.start()
                elif what == 'turn':
                    load.wait()
                else:
                    store.wait()
            if what == 'turn':
                @pl.when(cond)
                def _():
                    tout[n % 2] = tin[n % 2].T
                    store.start()

    mp_ref[...] = jnp.zeros_like(mp_ref)
    loss_ref[...] = jnp.zeros_like(loss_ref)
    for o in range(4):
        zt[o] = z_ref[:, o * BLK:(o + 1) * BLK].T

    def body(t, carry):
        slot = t % 2
        old = (t + 1) % 2
        band = 2 * (t - 1)

        @pl.when(jnp.logical_and(t >= 1, t < 10))
        def _():
            band_do(band, 'load')
            band_do(band + 1, 'load')

        @pl.when(t < 9)
        def _():
            @pl.when(t >= 5)
            def _():
                zt[t - 1] = z_ref[:, blk_ds(t - 1)].T

            for o in range(4):
                i, j = band_of(o, t)
                part[slot, o // 2, o % 2] = jnp.dot(zt[i], z_ref[:, blk_ds(j)], preferred_element_type=F32)
            for cp in s1(t):
                cp.start()

        @pl.when(jnp.logical_and(t >= 1, t < 10))
        def _():
            g = t - 1
            for cp in s1(g):
                cp.wait()
            s2x[old] = part[old, 1 - y, x, lo, :] + r1x[g, 1 - y]
            s2y[old] = part[old, y, 1 - x, hi, :] + r1y[g, 1 - x]
            for cp in s2(g):
                cp.start()
            kx[old] = part[old, y, x, lo, :] + r1x[g, y]
            ky[old] = part[old, y, x, hi, :] + r1y[g, x]

        @pl.when(jnp.logical_and(t >= 2, t < 11))
        def _():
            g = t - 2

            @pl.when(g == 0)
            def _():
                for cp in sums_out:
                    cp.wait()
                total = (zsum_all[0] + zsum_all[1]) + (zsum_all[2] + zsum_all[3])
                mu = total[0:1] / all_rows
                mu_ref[...] = mu
                for b in range(mu.shape[1] // BLK):
                    s = slice(b * BLK, (b + 1) * BLK)
                    muc_ref[s, :] = jnp.broadcast_to(mu[:, s], (BLK, BLK)).T

            for cp in s2(g):
                cp.wait()
            i, j = band_of(q, g)
            mu_j = mu_ref[:, blk_ds(j)]
            on_diag = i == j
            r_i = lax.broadcasted_iota(jnp.int32, (half, BLK), 0)
            k_i = lax.broadcasted_iota(jnp.int32, (half, BLK), 1)
            for off, k_ref, r_ref in ((0, kx, r2x), (half, ky, r2y)):
                mu_i = muc_ref[pl.ds(pl.multiple_of(i * BLK + off, half), half), :]
                cov = (k_ref[slot] + r_ref[g] - all_rows * (mu_i * mu_j)) / (all_rows - 1)
                diag = jnp.logical_and(r_i + off == k_i, on_diag)
                std = jnp.sqrt(jnp.where(diag, cov, 1.0) + STD_EPS)
                g_diag = jnp.where(std < 1.0, -VAR_WEIGHT, 0.0) / (2.0 * std)
                g_val = jnp.where(diag, g_diag, (2.0 * COV_WEIGHT) * cov)
                gb[g, y, x, pl.ds(off, half), :] = g_val.astype(BF16)
                weight = jnp.where(on_diag, COV_WEIGHT, 2.0 * COV_WEIGHT)
                terms = jnp.where(diag, VAR_WEIGHT * jnp.maximum(1.0 - std, 0.0), weight * cov * cov)
                loss_ref[...] += jnp.sum(terms, axis=0, keepdims=True)
            for cp in a1(g):
                cp.start()

        @pl.when(jnp.logical_and(t >= 3, t < 12))
        def _():
            for cp in a1(t - 3):
                cp.wait()
            for cp in a2(t - 3):
                cp.start()

        @pl.when(jnp.logical_and(t >= 2, t < 11))
        def _():
            band_do(band - 2, 'stored')
            band_do(band - 1, 'stored')

        @pl.when(jnp.logical_and(t >= 1, t < 10))
        def _():
            band_do(band, 'turn')
            band_do(band + 1, 'turn')

        @pl.when(t >= 4)
        def _():
            g = t - 4
            for cp in a2(g):
                cp.wait()
            for o in range(4):
                i, j = band_of(o, g)
                blk = gb[g, o // 2, o % 2]
                gh_ref[blk_ds(i), blk_ds(j)] = blk
                mp_ref[:, blk_ds(j)] += jnp.sum(muc_ref[blk_ds(i), :] * blk.astype(F32), axis=0, keepdims=True)

                @pl.when(i != j)
                def _():
                    blk_t = gb[g, o // 2, o % 2].T
                    gh_ref[blk_ds(j), blk_ds(i)] = blk_t
                    mp_ref[:, blk_ds(i)] += jnp.sum(muc_ref[blk_ds(j), :] * blk_t.astype(F32), axis=0, keepdims=True)

        return carry

    lax.fori_loop(0, 13, body, 0)
    for cp in z_out:
        cp.wait()


def gram_exchange(z, zsum, x2, x1, h, all_rows):
    rows, dim = z.shape
    vmem = pl.BlockSpec(memory_space=pltpu.VMEM)
    half = BLK // 2
    hbm = pl.BlockSpec(memory_space=pl.ANY)
    return pl.pallas_call(
        functools.partial(gram_kernel, all_rows),
        out_shape=(jax.ShapeDtypeStruct((dim, dim), BF16), jax.ShapeDtypeStruct((1, dim), F32),
                   jax.ShapeDtypeStruct((1, BLK), F32), jax.ShapeDtypeStruct((rows, dim), BF16),
                   jax.ShapeDtypeStruct((dim, rows), BF16), jax.ShapeDtypeStruct((dim, rows), BF16),
                   jax.ShapeDtypeStruct((h.shape[1], rows), BF16)),
        in_specs=[vmem, vmem, hbm, hbm, hbm],
        out_specs=(vmem, vmem, vmem, hbm, hbm, hbm, hbm),
        scratch_shapes=[
            pltpu.VMEM((2, rows, BLK), BF16),
            pltpu.VMEM((2, BLK, rows), BF16),
            pltpu.SemaphoreType.DMA((2, 2)),
            pltpu.VMEM((1, dim), F32),
            pltpu.VMEM((dim, BLK), F32),
            pltpu.VMEM((4, 2, dim), F32),
            pltpu.SemaphoreType.DMA((3,)),
            pltpu.SemaphoreType.DMA((3,)),
            pltpu.VMEM((8, BLK, rows), BF16),
            pltpu.VMEM((2, 2, 2, BLK, BLK), F32),
            pltpu.VMEM((9, 2, half, BLK), F32),
            pltpu.VMEM((9, 2, half, BLK), F32),
            pltpu.VMEM((9, half, BLK), F32),
            pltpu.VMEM((9, half, BLK), F32),
            pltpu.VMEM((2, half, BLK), F32),
            pltpu.VMEM((2, half, BLK), F32),
            pltpu.VMEM((2, half, BLK), F32),
            pltpu.VMEM((2, half, BLK), F32),
            pltpu.VMEM((9, 2, 2, BLK, BLK), BF16),
            pltpu.SemaphoreType.DMA((4, 2, 9)),
            pltpu.SemaphoreType.DMA((4, 2, 9)),
            pltpu.SemaphoreType.DMA((4,)),
        ],
        compiler_params=pltpu.CompilerParams(collective_id=1, has_side_effects=True, vmem_limit_bytes=60 << 20),
        cost_estimate=pl.CostEstimate(flops=36 * 2 * BLK * BLK * rows, bytes_accessed=30 << 20, transcendentals=0),
    )(z, zsum, x2, x1, h)


LAG = 2
SLOTS = 6 * LAG
LANE = 128
GROUPS = 36
TILE = 1024


def backward_kernel(all_rows, z_hbm, zo_hbm, gh_hbm, x2t_hbm, x1t_hbm, ht_hbm, w3_hbm, w2_hbm, u2_hbm, u1_hbm,
                    mp_ref, vec2_ref, vec1_ref, lossv_ref,
                    out_hbm, part_hbm, grads_ref, loss_ref,
                    buf_a, buf_b, buf_c, ht, sb, wb, zb, ub, ps, own, r0, r1, r2, st, sr, tot, lacc,
                    ssem, rsem, lsem, dsem, psem, bsem, tsend, trecv):
    idx = lax.axis_index('data')
    c, x, y = idx % 2, (idx // 2) % 2, idx // 4
    bits = (c, x, y)

    def peer(d):
        dev = idx
        for b in range(3):
            if (d >> b) & 1:
                dev = dev + (1 << b) - (2 << b) * bits[b]
        return dev

    nc, nx, ny = peer(1), peer(2), peer(4)
    dim = buf_a.shape[1]
    rows = buf_a.shape[0]

    def rds(start, size):
        return pl.ds(pl.multiple_of(start, size), size)

    row_x, row_y = x * 256 + y * 128, 512 + y * 256 + x * 128

    def s0(g):
        k = g % SLOTS
        return (remote(part_hbm.at[g, rds((1 - c) * 1024, 1024)], r0.at[k], ssem.at[0, k], rsem.at[0, k], nc),)

    def load_own(g):
        k = g % SLOTS
        return pltpu.make_async_copy(part_hbm.at[g, rds(c * 1024, 1024)], own.at[k], lsem.at[0, k])

    def s1(g):
        k = g % SLOTS
        return (remote(own.at[k, rds((1 - x) * 256, 256)], r1.at[0, k], ssem.at[1, k], rsem.at[1, k], nx),
                remote(own.at[k, rds(512 + (1 - y) * 256, 256)], r1.at[1, k], ssem.at[2, k], rsem.at[2, k], ny))

    def s2(g):
        k = g % SLOTS
        return (remote(own.at[k, rds(x * 256 + (1 - y) * 128, 128)], r2.at[0, k], ssem.at[3, k], rsem.at[3, k], ny),
                remote(own.at[k, rds(512 + y * 256 + (1 - x) * 128, 128)], r2.at[1, k], ssem.at[4, k], rsem.at[4, k],
                       nx))

    def a1(g):
        k = g % SLOTS
        ox, oy = out_hbm.at[g, rds(c * 1024 + row_x, 128)], out_hbm.at[g, rds(c * 1024 + row_y, 128)]
        return (remote(own.at[k, rds(row_x, 128)], ox, ssem.at[5, k], rsem.at[5, k], ny),
                remote(own.at[k, rds(row_y, 128)], oy, ssem.at[6, k], rsem.at[6, k], nx),
                pltpu.make_async_copy(own.at[k, rds(row_x, 128)], ox, lsem.at[1, k]),
                pltpu.make_async_copy(own.at[k, rds(row_y, 128)], oy, lsem.at[2, k]))

    def a2(g):
        k = g % SLOTS
        bx, by = out_hbm.at[g, rds(c * 1024 + x * 256, 256)], out_hbm.at[g, rds(c * 1024 + 512 + y * 256, 256)]
        return (remote(bx, bx, ssem.at[7, k], rsem.at[7, k], nx), remote(by, by, ssem.at[8, k], rsem.at[8, k], ny))

    def a0(g):
        k = g % SLOTS
        b = out_hbm.at[g, rds(c * 1024, 1024)]
        return (remote(b, b, ssem.at[9, k], rsem.at[9, k], nc),)

    def stage(g, fn):
        @pl.when(jnp.logical_and(g >= 0, g < GROUPS))
        def _():
            fn(g)

    def wait_all(cps):
        for cp in cps:
            cp.wait()

    def start_all(cps):
        for cp in cps:
            cp.start()

    def to_a0(g):
        wait_all(a2(g))
        start_all(a0(g))

    def to_a2(g):
        wait_all(a1(g))
        start_all(a2(g))

    def to_a1(g):
        wait_all(s2(g))
        k = g % SLOTS
        own[k, rds(row_x, 128)] += r2[0, k]
        own[k, rds(row_y, 128)] += r2[1, k]
        start_all(a1(g))

    def to_s2(g):
        wait_all(s1(g))
        k = g % SLOTS
        own[k, rds(x * 256, 256)] += r1[0, k]
        own[k, rds(512 + y * 256, 256)] += r1[1, k]
        start_all(s2(g))

    def to_s1(g):
        wait_all(s0(g))
        load_own(g).wait()
        k = g % SLOTS
        own[k] += r0[k]
        start_all(s1(g))

    def to_s0(g):
        start_all(s0(g))
        load_own(g).start()

    def streams(n):
        slot = n % 2
        blk = n % 8
        return ((n < 8, (pltpu.make_async_copy(gh_hbm.at[:, blk_ds(blk)], sb.at[slot], dsem.at[0, slot]),
                         pltpu.make_async_copy(zo_hbm.at[:, blk_ds(blk)], zb.at[slot], dsem.at[1, slot]))),
                (jnp.logical_and(n >= 8, n < 24),
                 (pltpu.make_async_copy(w3_hbm.at[blk_ds(blk), :], wb.at[slot], dsem.at[0, slot]),
                  pltpu.make_async_copy(u2_hbm.at[:, blk_ds(blk)], ub.at[slot], dsem.at[1, slot]))),
                (jnp.logical_and(n >= 24, n < 40),
                 (pltpu.make_async_copy(w2_hbm.at[blk_ds(blk), :], wb.at[slot], dsem.at[0, slot]),
                  pltpu.make_async_copy(u1_hbm.at[:, blk_ds(blk)], ub.at[slot], dsem.at[1, slot]))))

    def start_streams(n):
        for cond, cps in streams(n):
            pl.when(cond)(functools.partial(start_all, cps))

    def wait_streams(n, which):
        wait_all(streams(n)[which][1])

    def part_writes(n):
        g = jnp.where(n < 8, 2 * n, 2 * n - 16)
        return tuple(pltpu.make_async_copy(ps.at[:, pl.ds(h * LANE, LANE)], part_hbm.at[g + h], psem.at[h])
                     for h in range(2))

    def part_writes_one(n):
        tile = 2 * (n - 32)
        return tuple(pltpu.make_async_copy(ps.at[pl.ds(0, 512), pl.ds(h * LANE, LANE)],
                                           part_hbm.at[32 + (tile + h) // 4, rds(((tile + h) % 4) * 512, 512)],
                                           psem.at[h]) for h in range(2))

    def loop_tiles(count, fn):
        def step(m, carry):
            fn(pl.ds(pl.multiple_of(m * TILE, TILE), TILE))
            return carry
        lax.fori_loop(0, count, step, 0)

    def nt(a, b):
        return lax.dot_general(a, b, (((1,), (1,)), ((), ())), preferred_element_type=F32)

    def piece_dz(n):
        slot, col = n % 2, blk_ds(n % 8)
        wait_streams(n, 0)
        start_streams(n + 1)

        def tile(r):
            rp = jnp.dot(buf_a[r, :], sb[slot], preferred_element_type=F32)
            zd = buf_a[r, col].astype(F32) - zb[slot, r, :].astype(F32)
            dz = (2.0 / (all_rows - 1)) * (rp - mp_ref[:, col]) + (2.0 * INV_WEIGHT / all_rows) * zd
            buf_c[r, col] = dz.astype(BF16)
            lacc[...] += jnp.sum(zd * zd, axis=0, keepdims=True)
        loop_tiles(rows // TILE, tile)

        @pl.when(n == 0)
        def _():
            big(1).wait()

        def grad(r):
            ps[r, :] = jnp.dot(buf_b[r, :], buf_c[:, col], preferred_element_type=F32)
        loop_tiles(dim // TILE, grad)
        start_all(part_writes(n))

    def d_act(d_ref, u_slot, r, vec_ref, col, slot):
        dx = nt(d_ref[r, :], wb[slot])
        nrm = (ub[slot, r, :] - vec_ref[0:1, col]) * vec_ref[1:2, col]
        act = vec_ref[2:3, col] * nrm + vec_ref[3:4, col]
        return jnp.where(act > 0.0, dx, 0.0), nrm

    def piece_stats(n, d_ref, vec_ref, layer, which):
        slot, col = n % 2, blk_ds(n % 8)
        wait_streams(n, which)
        start_streams(n + 1)
        st[layer, 0:2, col] = jnp.zeros((2, BLK), F32)

        def tile(r):
            da, nrm = d_act(d_ref, slot, r, vec_ref, col, slot)
            st[layer, 0:1, col] += jnp.sum(da, axis=0, keepdims=True)
            st[layer, 1:2, col] += jnp.sum(da * nrm, axis=0, keepdims=True)
        loop_tiles(rows // TILE, tile)

    def piece_du(n, d_ref, vec_ref, layer, which, du_ref):
        slot, col = n % 2, blk_ds(n % 8)
        wait_streams(n, which)
        start_streams(n + 1)

        def tile(r):
            da, nrm = d_act(d_ref, slot, r, vec_ref, col, slot)
            du = (vec_ref[1:2, col] * vec_ref[2:3, col]) * (
                da - tot[layer, 0:1, col] / all_rows - nrm * (tot[layer, 1:2, col] / all_rows))
            du_ref[r, col] = du.astype(BF16)
        loop_tiles(rows // TILE, tile)
        return col

    def stat_copies(layer):
        return tuple(remote(st.at[layer], sr.at[layer, idx], tsend.at[layer, d - 1], trecv.at[layer, d - 1], peer(d))
                     for d in range(1, 8))

    def send_stats(layer):
        start_all(stat_copies(layer))

    def finish_stats(layer):
        wait_all(stat_copies(layer))
        sr[layer, idx] = st[layer]
        va = (sr[layer, 0] + sr[layer, 2]) + (sr[layer, 4] + sr[layer, 6])
        vb = (sr[layer, 1] + sr[layer, 3]) + (sr[layer, 5] + sr[layer, 7])
        tot[layer] = jnp.where(c == 0, va, vb)
        grads_ref[layer] = va + vb

    def big(i):
        src = (z_hbm, x2t_hbm, x1t_hbm)[i]
        return pltpu.make_async_copy(src, (buf_a, buf_b, buf_a)[i], bsem.at[i])

    big(0).start()
    start_streams(0)
    big(1).start()
    ht_copy = pltpu.make_async_copy(ht_hbm, ht, bsem.at[3])
    ht_copy.start()
    lacc[...] = jnp.zeros_like(lacc)
    st[...] = jnp.zeros_like(st)
    meet([peer(d) for d in range(1, 8)])
    big(0).wait()

    def tick(it, carry):
        k = it - 1
        stage(k - 6 * LAG, lambda g: wait_all(a0(g)))
        stage(k - 5 * LAG, to_a0)
        stage(k - 4 * LAG, to_a2)
        stage(k - 3 * LAG, to_a1)
        stage(k - 2 * LAG, to_s2)
        stage(k - LAG, to_s1)

        @pl.when(jnp.logical_or(jnp.logical_and(it >= 1, it <= 8), jnp.logical_and(it >= 17, it <= 24)))
        def _():
            wait_all(part_writes(it - 1))

        @pl.when(jnp.logical_and(it >= 29, it <= 36))
        def _():
            wait_all(part_writes_one(it + 3))

        stage(k, to_s0)

        @pl.when(it < 8)
        def _():
            piece_dz(it)

        @pl.when(jnp.logical_and(it >= 8, it < 16))
        def _():
            @pl.when(it == 8)
            def _():
                big(2).start()

            piece_stats(it, buf_c, vec2_ref, 0, 1)

            @pl.when(it == 15)
            def _():
                st[0, 2:3, 0:BLK] = lossv_ref[...] + lacc[...] * (0.5 * INV_WEIGHT / all_rows)
                send_stats(0)

        @pl.when(jnp.logical_and(it >= 16, it < 24))
        def _():
            @pl.when(it == 16)
            def _():
                finish_stats(0)
                loss_ref[...] = jnp.broadcast_to(jnp.sum(grads_ref[0, 2:3, 0:BLK], axis=1, keepdims=True),
                                                 loss_ref.shape)
                big(2).wait()
                ht_copy.wait()

            col = piece_du(it, buf_c, vec2_ref, 0, 1, buf_b)

            def grad(r):
                ps[r, :] = jnp.dot(buf_a[r, :], buf_b[:, col], preferred_element_type=F32)
            loop_tiles(dim // TILE, grad)
            start_all(part_writes(it))

        @pl.when(jnp.logical_and(it >= 24, it < 28))
        def _():
            def two(m, carry):
                piece_stats(24 + 2 * (it - 24) + m, buf_b, vec1_ref, 1, 2)
                return carry
            lax.fori_loop(0, 2, two, 0)

            @pl.when(it == 27)
            def _():
                send_stats(1)

        @pl.when(jnp.logical_and(it >= 28, it < 36))
        def _():
            @pl.when(it == 28)
            def _():
                finish_stats(1)

            n = it + 4
            col = piece_du(n, buf_b, vec1_ref, 1, 2, buf_c)
            ps[0:512, :] = jnp.dot(ht[...], buf_c[:, col], preferred_element_type=F32)
            start_all(part_writes_one(n))

        return carry

    lax.fori_loop(0, GROUPS + 1 + 6 * LAG, tick, 0)


def backward(z, zo, gh, x2t, x1t, ht, w3, w2, u2, u1, mp, vec2, vec1, lossv, all_rows):
    rows, dim = z.shape
    feat = ht.shape[0]
    hbm = pl.BlockSpec(memory_space=pl.ANY)
    vmem = pl.BlockSpec(memory_space=pltpu.VMEM)
    dma = pltpu.SemaphoreType.DMA
    return pl.pallas_call(
        functools.partial(backward_kernel, all_rows),
        out_shape=(jax.ShapeDtypeStruct((GROUPS, dim, LANE), F32), jax.ShapeDtypeStruct((GROUPS, dim, LANE), F32),
                   jax.ShapeDtypeStruct((2, 4, dim), F32), jax.ShapeDtypeStruct((1, LANE), F32)),
        in_specs=[hbm] * 10 + [vmem] * 4,
        out_specs=(hbm, hbm, vmem, vmem),
        scratch_shapes=[
            pltpu.VMEM((rows, dim), BF16), pltpu.VMEM((rows, dim), BF16), pltpu.VMEM((rows, dim), BF16),
            pltpu.VMEM((feat, rows), BF16),
            pltpu.VMEM((2, dim, BLK), BF16), pltpu.VMEM((2, BLK, dim), BF16), pltpu.VMEM((2, rows, BLK), BF16),
            pltpu.VMEM((2, rows, BLK), F32), pltpu.VMEM((dim, BLK), F32),
            pltpu.VMEM((SLOTS, 1024, LANE), F32), pltpu.VMEM((SLOTS, 1024, LANE), F32),
            pltpu.VMEM((2, SLOTS, 256, LANE), F32), pltpu.VMEM((2, SLOTS, 128, LANE), F32),
            pltpu.VMEM((2, 4, dim), F32), pltpu.VMEM((2, 8, 4, dim), F32), pltpu.VMEM((2, 4, dim), F32),
            pltpu.VMEM((1, BLK), F32),
            dma((10, SLOTS)), dma((10, SLOTS)), dma((3, SLOTS)), dma((2, 2)), dma((2,)), dma((4,)),
            dma((2, 7)), dma((2, 7)),
        ],
        compiler_params=pltpu.CompilerParams(collective_id=2, has_side_effects=True, vmem_limit_bytes=67043328),
        cost_estimate=pl.CostEstimate(flops=150 * 10 ** 9, bytes_accessed=200 << 20, transcendentals=0),
    )(z, zo, gh, x2t, x1t, ht, w3, w2, u2, u1, mp, vec2, vec1, lossv)


def pairs_kernel(i_ref, o_ref):
    o_ref[:, :LANE] = i_ref[0]
    o_ref[:, LANE:] = i_ref[1]


def join_pairs(groups, first, dim):
    return pl.pallas_call(
        pairs_kernel,
        grid=(8,),
        out_shape=jax.ShapeDtypeStruct((dim, dim), F32),
        in_specs=[pl.BlockSpec((2, dim, LANE), lambda e: (first + e, 0, 0))],
        out_specs=pl.BlockSpec((dim, BLK), lambda e: (0, e)),
        compiler_params=pltpu.CompilerParams(dimension_semantics=("arbitrary",), vmem_limit_bytes=32 << 20),
        cost_estimate=pl.CostEstimate(flops=0, bytes_accessed=8 * dim * dim, transcendentals=0),
    )(groups)


def quads_kernel(i_ref, o_ref):
    for k in range(4):
        o_ref[:, k * LANE:(k + 1) * LANE] = i_ref[0, k * 512:(k + 1) * 512]


def join_quads(groups, first, dim):
    return pl.pallas_call(
        quads_kernel,
        grid=(4,),
        out_shape=jax.ShapeDtypeStruct((512, dim), F32),
        in_specs=[pl.BlockSpec((1, dim, LANE), lambda e: (first + e, 0, 0))],
        out_specs=pl.BlockSpec((512, 512), lambda e: (0, e)),
        compiler_params=pltpu.CompilerParams(dimension_semantics=("arbitrary",), vmem_limit_bytes=32 << 20),
        cost_estimate=pl.CostEstimate(flops=0, bytes_accessed=2 * dim * dim, transcendentals=0),
    )(groups)


def solution(mesh):
    group_devs = mesh.shape['data']

    def local_step(h_a, h_b, w_one, w_two, w_three, gain_one, bias_one, gain_two, bias_two):
        all_rows = h_a.shape[0] * group_devs
        dim = w_two.shape[0]
        vec = jnp.stack([gain_one, bias_one, gain_two, bias_two])
        h, u1, x1, u2, x2, z, stat1, stat2, zsum = forward(h_a, h_b, w_one, w_two, w_three, vec, all_rows)
        g_hat, mean_part, loss_vec, z_other, x2t, x1t, ht = gram_exchange(z, zsum, x2, x1, h, all_rows)
        groups, _, grads, loss = backward(z, z_other, g_hat, x2t, x1t, ht, w_three, w_two, u2, u1, mean_part, stat2,
                                          stat1, loss_vec, all_rows)
        return (loss[0, 0], join_quads(groups, 32, dim), join_pairs(groups, 8, dim), join_pairs(groups, 0, dim),
                grads[1, 1], grads[1, 0], grads[0, 1], grads[0, 0])

    row_spec = P('data', None)
    return jax.shard_map(local_step, mesh=mesh,
                         in_specs=(row_spec, row_spec, P(), P(), P(), P(), P(), P(), P()),
                         out_specs=(P(), P(), P(), P(), P(), P(), P(), P()),
                         check_vma=False)
```

```python
import functools

import jax
import jax.numpy as jnp
from jax import lax
from jax.experimental import pallas as pl
from jax.experimental.pallas import tpu as pltpu
from jax.sharding import PartitionSpec as P

BN_EPS = 1e-5
STD_EPS = 1e-4
INV_WEIGHT = 2.0
VAR_WEIGHT = 1.0
COV_WEIGHT = 2.0
BLK = 256

F32 = jnp.float32
BF16 = jnp.bfloat16


MESH_ID = pl.DeviceIdType.MESH


def remote(src, dst, send_sem, recv_sem, dev):
    return pltpu.make_async_remote_copy(src_ref=src, dst_ref=dst, send_sem=send_sem, recv_sem=recv_sem,
                                        device_id=(dev,), device_id_type=MESH_ID)


def meet(devs):
    barrier = pltpu.get_barrier_semaphore()
    for dev in devs:
        pl.semaphore_signal(barrier, inc=1, device_id=(dev,), device_id_type=MESH_ID)
    pl.semaphore_wait(barrier, len(devs))


def blk_ds(i):
    return pl.ds(pl.multiple_of(i * BLK, BLK), BLK)


def peer_of(idx, bits, d):
    dev = idx
    for b in range(3):
        if (d >> b) & 1:
            dev = dev + (1 << b) - (2 << b) * bits[b]
    return dev


def front_kernel(all_rows, ha_hbm, hb_hbm, w1_ref, w2_hbm, w3_hbm, vec_ref,
                 u1_hbm, x1_hbm, u2_hbm, z_hbm, zo_hbm, gh_hbm, x2t_hbm, x1t_hbm, ht_hbm,
                 stat1_ref, stat2_ref, mp_ref, loss_ref,
                 hbuf, wblk, xb, z, st, sr, zs, zs_all, mu_ref,
                 part, r1x, r1y, r2x, r2y, s2x, s2y, kx, ky, gb,
                 hsem, wsem, usem, xsem, osem, bsem, tsend, trecv, zsend, zrecv, osend, orecv, ssem, rsem):
    idx = lax.axis_index('data')
    c, x, y, q = idx % 2, (idx // 2) % 2, idx // 4, idx // 2
    bits = (c, x, y)
    nc, nx, ny = [peer_of(idx, bits, d) for d in (1, 2, 4)]
    chips = [peer_of(idx, bits, d) for d in (2, 4, 6)]
    rows, dim = z.shape
    half_rows = rows // 2
    half = BLK // 2
    lo, hi = pl.ds(0, half), pl.ds(half, half)
    tiles = [slice(0, half_rows), slice(half_rows, rows)]

    def start_all(cps):
        for cp in cps:
            cp.start()

    def wait_all(cps):
        for cp in cps:
            cp.wait()

    def views(what):
        for core, mine, other in ((0, ha_hbm, hb_hbm), (1, hb_hbm, ha_hbm)):
            @pl.when(c == core)
            def _():
                own = pltpu.make_async_copy(mine, hbuf.at[pl.ds(0, half_rows)], hsem.at[0])
                sent = remote(other, hbuf.at[pl.ds(half_rows, half_rows)], hsem.at[1], hsem.at[2], nc)
                if what == 'own':
                    own.start()
                elif what == 'send':
                    sent.start()
                    own.wait()
                else:
                    sent.wait()

    def w_copies(s):
        col = blk_ds(s % 8)
        return ((s < 16, pltpu.make_async_copy(w2_hbm.at[:, col], wblk.at[s % 2], wsem.at[s % 2])),
                (jnp.logical_and(s >= 16, s < 24),
                 pltpu.make_async_copy(w3_hbm.at[:, col], wblk.at[s % 2], wsem.at[s % 2])))

    def w_start(s):
        for cond, cp in w_copies(s):
            pl.when(cond)(cp.start)

    def columns(fn):
        def step(nb, carry):
            fn(nb, blk_ds(nb))
            return carry
        lax.fori_loop(0, dim // BLK, step, 0)

    def layers(u):
        def add_sums(layer, m, col, val):
            sums = jnp.concatenate([jnp.sum(val, axis=0, keepdims=True), jnp.sum(val * val, axis=0, keepdims=True)])
            st[layer, :, col] = sums if m == 0 else st[layer, :, col] + sums

        def statistics(layer, stat_ref):
            cps = [remote(st.at[layer], sr.at[layer, q], tsend.at[layer, i], trecv.at[layer, i], dev)
                   for i, dev in enumerate(chips)]
            start_all(cps)
            sr[layer, q] = st[layer]
            wait_all(cps)
            total = (sr[layer, 0] + sr[layer, 1]) + (sr[layer, 2] + sr[layer, 3])
            mean = total[0:1] / all_rows
            var = total[1:2] / all_rows - mean * mean
            stat_ref[0:1, :] = mean
            stat_ref[1:2, :] = lax.rsqrt(var + BN_EPS)
            stat_ref[2:4, :] = vec_ref[2 * layer:2 * layer + 2, :]

        def activate(stat_ref, m, col):
            nrm = (u[tiles[m], col] - stat_ref[0:1, col]) * stat_ref[1:2, col]
            xb[m, :, col] = jnp.maximum(stat_ref[2:3, col] * nrm + stat_ref[3:4, col], 0.0).astype(BF16)

        def u_out(layer, m):
            r = pl.ds(m * half_rows, half_rows)
            return pltpu.make_async_copy(u.at[r], (u1_hbm, u2_hbm)[layer].at[r], usem.at[m])

        def x_out(m):
            return pltpu.make_async_copy(xb.at[m], x1_hbm.at[pl.ds(m * half_rows, half_rows)], xsem.at[m])

        for m in range(2):
            if m == 1:
                views('got')

            def first(nb, col):
                val = jnp.dot(hbuf[tiles[m], :], w1_ref[:, col], preferred_element_type=F32)
                u[tiles[m], col] = val
                add_sums(0, m, col, val)
            columns(first)
            u_out(0, m).start()
        statistics(0, stat1_ref)

        columns(lambda nb, col: activate(stat1_ref, 0, col))
        for m in range(2):
            x_out(m).start()
            u_out(0, m).wait()

            def second(nb, col):
                s = 8 * m + nb
                w_copies(s)[0][1].wait()
                w_start(s + 1)
                val = jnp.dot(xb[m], wblk[s % 2], preferred_element_type=F32)
                if m == 0:
                    activate(stat1_ref, 1, col)
                u[tiles[m], col] = val
                add_sums(1, m, col, val)
            columns(second)
            u_out(1, m).start()
        statistics(1, stat2_ref)
        for m in range(2):
            x_out(m).wait()
            columns(lambda nb, col: activate(stat2_ref, m, col))
        for m in range(2):
            u_out(1, m).wait()

    views('own')
    w_start(0)
    meet([nc] + chips)
    views('send')
    pl.run_scoped(layers, pltpu.VMEM((rows, dim), F32))

    def block_of(o, g):
        b = 4 * g + o
        j = jnp.int32(0)
        for k in range(1, 8):
            j = j + jnp.where(b >= k * (k + 1) // 2, 1, 0)
        return b - j * (j + 1) // 2, j

    def s1(t):
        slot = t % 2
        return (remote(part.at[slot, :, 1 - x, lo, :], r1x.at[t], ssem.at[0, 0, t], rsem.at[0, 0, t], nx),
                remote(part.at[slot, 1 - y, :, hi, :], r1y.at[t], ssem.at[0, 1, t], rsem.at[0, 1, t], ny))

    def s2(t):
        slot = t % 2
        return (remote(s2x.at[slot], r2x.at[t], ssem.at[1, 0, t], rsem.at[1, 0, t], ny),
                remote(s2y.at[slot], r2y.at[t], ssem.at[1, 1, t], rsem.at[1, 1, t], nx))

    def a1(t):
        bx, by = gb.at[t, y, x, lo, :], gb.at[t, y, x, hi, :]
        return (remote(bx, bx, ssem.at[2, 0, t], rsem.at[2, 0, t], ny),
                remote(by, by, ssem.at[2, 1, t], rsem.at[2, 1, t], nx))

    def a2(t):
        bx, by = gb.at[t, :, x, lo, :], gb.at[t, y, :, hi, :]
        return (remote(bx, bx, ssem.at[3, 0, t], rsem.at[3, 0, t], nx),
                remote(by, by, ssem.at[3, 1, t], rsem.at[3, 1, t], ny))

    def z_sums(nb):
        return [remote(zs.at[nb], zs_all.at[q, nb], zsend.at[nb, i], zrecv.at[nb, i], dev)
                for i, dev in enumerate(chips)]

    def other_copies():
        first, second = pl.ds(0, half_rows), pl.ds(half_rows, half_rows)
        return [remote(z.at[second], zo_hbm.at[first], osend.at[0], orecv.at[0], nc),
                remote(z.at[first], zo_hbm.at[second], osend.at[1], orecv.at[1], nc),
                pltpu.make_async_copy(z, z_hbm, osem.at[0])]

    def gram(zt, gh, tin, tout, muc):
        mp_ref[...] = jnp.zeros_like(mp_ref)
        loss_ref[...] = jnp.zeros_like(loss_ref)

        def third(nb):
            col = blk_ds(nb)
            s = 16 + nb
            w_copies(s)[1][1].wait()
            w_start(s + 1)
            sums = jnp.zeros((1, BLK), F32)
            for m in range(2):
                val = jnp.dot(xb[m], wblk[s % 2], preferred_element_type=F32).astype(BF16)
                z[tiles[m], col] = val
                sums = sums + jnp.sum(val.astype(F32), axis=0, keepdims=True)
            zs[nb] = jnp.broadcast_to(sums, (8, BLK))
            start_all(z_sums(nb))
            zt[nb] = z[:, col].T

        def means(nb):
            wait_all(z_sums(nb))
            zs_all[q, nb] = zs[nb]
            total = (zs_all[0, nb] + zs_all[1, nb]) + (zs_all[2, nb] + zs_all[3, nb])
            mu = total[0:1] / all_rows
            mu_ref[:, blk_ds(nb)] = mu
            muc[blk_ds(nb), :] = jnp.broadcast_to(mu, (BLK, BLK)).T

        def each(lo_nb, hi_nb, fn):
            def step(nb, carry):
                fn(nb)
                return carry
            lax.fori_loop(lo_nb, hi_nb, step, 0)

        def new_col(t):
            return (jnp.logical_or(t < 4, jnp.logical_or(t == 5, t == 7)),
                    jnp.where(t < 4, t + 2, (t + 7) // 2))

        def x1_load(n):
            return pltpu.make_async_copy(x1_hbm.at[:, blk_ds(n)], tin, bsem.at[0])

        def store2(n):
            return pltpu.make_async_copy(tout.at[0], x2t_hbm.at[blk_ds(n), :], bsem.at[1])

        def store1(n):
            return pltpu.make_async_copy(tout.at[1], x1t_hbm.at[blk_ds(n), :], bsem.at[2])

        def store_h(n):
            return pltpu.make_async_copy(tout.at[n], ht_hbm.at[pl.ds(n * BLK, BLK), :], bsem.at[1 + n])

        each(0, 2, third)

        def body(t, carry):
            slot = t % 2
            old = (t + 1) % 2
            has_col, nb_new = new_col(t)

            @pl.when(jnp.logical_and(t >= 1, t < 9))
            def _():
                x1_load(t - 1).start()

            @pl.when(jnp.logical_and(t < 9, has_col))
            def _():
                third(nb_new)

            @pl.when(t == 7)
            def _():
                start_all(other_copies())

            @pl.when(t < 9)
            def _():
                for o in range(4):
                    i, j = block_of(o, t)
                    part[slot, o // 2, o % 2] = jnp.dot(zt[i], z[:, blk_ds(j)], preferred_element_type=F32)
                start_all(s1(t))

            @pl.when(jnp.logical_and(t >= 1, t < 10))
            def _():
                g = t - 1
                wait_all(s1(g))
                s2x[old] = part[old, 1 - y, x, lo, :] + r1x[g, 1 - y]
                s2y[old] = part[old, y, 1 - x, hi, :] + r1y[g, 1 - x]
                start_all(s2(g))
                kx[old] = part[old, y, x, lo, :] + r1x[g, y]
                ky[old] = part[old, y, x, hi, :] + r1y[g, x]

            @pl.when(jnp.logical_and(t >= 2, t < 11))
            def _():
                g = t - 2
                had_col, nb_old = new_col(g)

                @pl.when(g == 0)
                def _():
                    each(0, 2, means)

                @pl.when(had_col)
                def _():
                    means(nb_old)

                wait_all(s2(g))
                i, j = block_of(q, g)
                mu_j = mu_ref[:, blk_ds(j)]
                on_diag = i == j
                r_i = lax.broadcasted_iota(jnp.int32, (half, BLK), 0)
                k_i = lax.broadcasted_iota(jnp.int32, (half, BLK), 1)
                for off, k_ref, r_ref in ((0, kx, r2x), (half, ky, r2y)):
                    mu_i = muc[pl.ds(pl.multiple_of(i * BLK + off, half), half), :]
                    cov = (k_ref[slot] + r_ref[g] - all_rows * (mu_i * mu_j)) / (all_rows - 1)
                    diag = jnp.logical_and(r_i + off == k_i, on_diag)
                    std = jnp.sqrt(jnp.where(diag, cov, 1.0) + STD_EPS)
                    g_diag = jnp.where(std < 1.0, -VAR_WEIGHT, 0.0) / (2.0 * std)
                    g_val = jnp.where(diag, g_diag, (2.0 * COV_WEIGHT) * cov)
                    gb[g, y, x, pl.ds(off, half), :] = g_val.astype(BF16)
                    weight = jnp.where(on_diag, COV_WEIGHT, 2.0 * COV_WEIGHT)
                    terms = jnp.where(diag, VAR_WEIGHT * jnp.maximum(1.0 - std, 0.0), weight * cov * cov)
                    loss_ref[...] += jnp.sum(terms, axis=0, keepdims=True)
                start_all(a1(g))

            @pl.when(jnp.logical_and(t >= 3, t < 12))
            def _():
                wait_all(a1(t - 3))
                start_all(a2(t - 3))

            @pl.when(jnp.logical_and(t >= 2, t < 10))
            def _():
                store2(t - 2).wait()
                store1(t - 2).wait()

            @pl.when(jnp.logical_and(t >= 1, t < 9))
            def _():
                band = blk_ds(t - 1)
                for m in range(2):
                    tout[0, :, tiles[m]] = xb[m, :, band].T
                store2(t - 1).start()
                x1_load(t - 1).wait()
                tout[1] = tin[...].T
                store1(t - 1).start()

            @pl.when(t == 9)
            def _():
                for n in range(2):
                    tout[n] = hbuf[:, n * BLK:(n + 1) * BLK].T
                    store_h(n).start()

            @pl.when(t >= 4)
            def _():
                g = t - 4
                wait_all(a2(g))
                for o in range(4):
                    i, j = block_of(o, g)
                    blk = gb[g, o // 2, o % 2]
                    gh[blk_ds(i), blk_ds(j)] = blk
                    mp_ref[:, blk_ds(j)] += jnp.sum(muc[blk_ds(i), :] * blk.astype(F32), axis=0, keepdims=True)

                    @pl.when(i != j)
                    def _():
                        blk_t = gb[g, o // 2, o % 2].T
                        gh[blk_ds(j), blk_ds(i)] = blk_t
                        mp_ref[:, blk_ds(i)] += jnp.sum(muc[blk_ds(j), :] * blk_t.astype(F32), axis=0, keepdims=True)

            return carry

        lax.fori_loop(0, 13, body, 0)
        gh_out = pltpu.make_async_copy(gh, gh_hbm, osem.at[1])
        gh_out.start()
        for n in range(2):
            store_h(n).wait()
        wait_all(other_copies())
        gh_out.wait()

    pl.run_scoped(gram, pltpu.VMEM((8, BLK, rows), BF16), pltpu.VMEM((dim, dim), BF16), pltpu.VMEM((rows, BLK), BF16),
                  pltpu.VMEM((2, BLK, rows), BF16), pltpu.VMEM((dim, BLK), F32))


def front(h_a, h_b, w1, w2, w3, vec, all_rows):
    rows, feat = 2 * h_a.shape[0], h_a.shape[1]
    dim = w2.shape[0]
    half = BLK // 2
    hbm = pl.BlockSpec(memory_space=pl.ANY)
    vmem = pl.BlockSpec(memory_space=pltpu.VMEM)
    dma = pltpu.SemaphoreType.DMA
    shape = jax.ShapeDtypeStruct
    return pl.pallas_call(
        functools.partial(front_kernel, all_rows),
        out_shape=(shape((rows, dim), F32), shape((rows, dim), BF16), shape((rows, dim), F32),
                   shape((rows, dim), BF16), shape((rows, dim), BF16), shape((dim, dim), BF16),
                   shape((dim, rows), BF16), shape((dim, rows), BF16), shape((feat, rows), BF16),
                   shape((4, dim), F32), shape((4, dim), F32), shape((1, dim), F32), shape((1, BLK), F32)),
        in_specs=[hbm, hbm, vmem, hbm, hbm, vmem],
        out_specs=(hbm,) * 9 + (vmem,) * 4,
        scratch_shapes=[
            pltpu.VMEM((rows, feat), BF16), pltpu.VMEM((2, dim, BLK), BF16),
            pltpu.VMEM((2, rows // 2, dim), BF16), pltpu.VMEM((rows, dim), BF16),
            pltpu.VMEM((2, 2, dim), F32), pltpu.VMEM((2, 4, 2, dim), F32),
            pltpu.VMEM((8, 8, BLK), F32), pltpu.VMEM((4, 8, 8, BLK), F32), pltpu.VMEM((1, dim), F32),
            pltpu.VMEM((2, 2, 2, BLK, BLK), F32),
            pltpu.VMEM((9, 2, half, BLK), F32), pltpu.VMEM((9, 2, half, BLK), F32),
            pltpu.VMEM((9, half, BLK), F32), pltpu.VMEM((9, half, BLK), F32),
            pltpu.VMEM((2, half, BLK), F32), pltpu.VMEM((2, half, BLK), F32),
            pltpu.VMEM((2, half, BLK), F32), pltpu.VMEM((2, half, BLK), F32),
            pltpu.VMEM((9, 2, 2, BLK, BLK), BF16),
            dma((3,)), dma((2,)), dma((2,)), dma((2,)), dma((2,)), dma((3,)), dma((2, 3)), dma((2, 3)),
            dma((8, 3)), dma((8, 3)), dma((2,)), dma((2,)), dma((4, 2, 9)), dma((4, 2, 9)),
        ],
        compiler_params=pltpu.CompilerParams(collective_id=3, has_side_effects=True, vmem_limit_bytes=67043328),
        cost_estimate=pl.CostEstimate(flops=50 * 10 ** 9, bytes_accessed=120 << 20, transcendentals=0),
    )(h_a, h_b, w1, w2, w3, vec)


LAG = 2
SLOTS = 6 * LAG
LANE = 128
GROUPS = 36
TILE = 1024


def backward_kernel(all_rows, z_hbm, zo_hbm, gh_hbm, x2t_hbm, x1t_hbm, ht_hbm, w3_hbm, w2_hbm, u2_hbm, u1_hbm,
                    mp_ref, vec2_ref, vec1_ref, lossv_ref,
                    out_hbm, part_hbm, grads_ref, loss_ref,
                    buf_a, buf_b, buf_c, ht, sb, wb, zb, ub, ps, own, r0, r1, r2, st, sr, tot, lacc,
                    ssem, rsem, lsem, dsem, psem, bsem, tsend, trecv):
    idx = lax.axis_index('data')
    c, x, y = idx % 2, (idx // 2) % 2, idx // 4
    bits = (c, x, y)

    def peer(d):
        dev = idx
        for b in range(3):
            if (d >> b) & 1:
                dev = dev + (1 << b) - (2 << b) * bits[b]
        return dev

    nc, nx, ny = peer(1), peer(2), peer(4)
    dim = buf_a.shape[1]
    rows = buf_a.shape[0]

    def rds(start, size):
        return pl.ds(pl.multiple_of(start, size), size)

    row_x, row_y = x * 256 + y * 128, 512 + y * 256 + x * 128

    def s0(g):
        k = g % SLOTS
        return (remote(part_hbm.at[g, rds((1 - c) * 1024, 1024)], r0.at[k], ssem.at[0, k], rsem.at[0, k], nc),)

    def load_own(g):
        k = g % SLOTS
        return pltpu.make_async_copy(part_hbm.at[g, rds(c * 1024, 1024)], own.at[k], lsem.at[0, k])

    def s1(g):
        k = g % SLOTS
        return (remote(own.at[k, rds((1 - x) * 256, 256)], r1.at[0, k], ssem.at[1, k], rsem.at[1, k], nx),
                remote(own.at[k, rds(512 + (1 - y) * 256, 256)], r1.at[1, k], ssem.at[2, k], rsem.at[2, k], ny))

    def s2(g):
        k = g % SLOTS
        return (remote(own.at[k, rds(x * 256 + (1 - y) * 128, 128)], r2.at[0, k], ssem.at[3, k], rsem.at[3, k], ny),
                remote(own.at[k, rds(512 + y * 256 + (1 - x) * 128, 128)], r2.at[1, k], ssem.at[4, k], rsem.at[4, k],
                       nx))

    def a1(g):
        k = g % SLOTS
        ox, oy = out_hbm.at[g, rds(c * 1024 + row_x, 128)], out_hbm.at[g, rds(c * 1024 + row_y, 128)]
        return (remote(own.at[k, rds(row_x, 128)], ox, ssem.at[5, k], rsem.at[5, k], ny),
                remote(own.at[k, rds(row_y, 128)], oy, ssem.at[6, k], rsem.at[6, k], nx),
                pltpu.make_async_copy(own.at[k, rds(row_x, 128)], ox, lsem.at[1, k]),
                pltpu.make_async_copy(own.at[k, rds(row_y, 128)], oy, lsem.at[2, k]))

    def a2(g):
        k = g % SLOTS
        bx, by = out_hbm.at[g, rds(c * 1024 + x * 256, 256)], out_hbm.at[g, rds(c * 1024 + 512 + y * 256, 256)]
        return (remote(bx, bx, ssem.at[7, k], rsem.at[7, k], nx), remote(by, by, ssem.at[8, k], rsem.at[8, k], ny))

    def a0(g):
        k = g % SLOTS
        b = out_hbm.at[g, rds(c * 1024, 1024)]
        return (remote(b, b, ssem.at[9, k], rsem.at[9, k], nc),)

    def stage(g, fn):
        @pl.when(jnp.logical_and(g >= 0, g < GROUPS))
        def _():
            fn(g)

    def wait_all(cps):
        for cp in cps:
            cp.wait()

    def start_all(cps):
        for cp in cps:
            cp.start()

    def to_a0(g):
        wait_all(a2(g))
        start_all(a0(g))

    def to_a2(g):
        wait_all(a1(g))
        start_all(a2(g))

    def to_a1(g):
        wait_all(s2(g))
        k = g % SLOTS
        own[k, rds(row_x, 128)] += r2[0, k]
        own[k, rds(row_y, 128)] += r2[1, k]
        start_all(a1(g))

    def to_s2(g):
        wait_all(s1(g))
        k = g % SLOTS
        own[k, rds(x * 256, 256)] += r1[0, k]
        own[k, rds(512 + y * 256, 256)] += r1[1, k]
        start_all(s2(g))

    def to_s1(g):
        wait_all(s0(g))
        load_own(g).wait()
        k = g % SLOTS
        own[k] += r0[k]
        start_all(s1(g))

    def to_s0(g):
        start_all(s0(g))
        load_own(g).start()

    def streams(n):
        slot = n % 2
        blk = n % 8
        return ((n < 8, (pltpu.make_async_copy(gh_hbm.at[:, blk_ds(blk)], sb.at[slot], dsem.at[0, slot]),
                         pltpu.make_async_copy(zo_hbm.at[:, blk_ds(blk)], zb.at[slot], dsem.at[1, slot]))),
                (jnp.logical_and(n >= 8, n < 24),
                 (pltpu.make_async_copy(w3_hbm.at[blk_ds(blk), :], wb.at[slot], dsem.at[0, slot]),
                  pltpu.make_async_copy(u2_hbm.at[:, blk_ds(blk)], ub.at[slot], dsem.at[1, slot]))),
                (jnp.logical_and(n >= 24, n < 40),
                 (pltpu.make_async_copy(w2_hbm.at[blk_ds(blk), :], wb.at[slot], dsem.at[0, slot]),
                  pltpu.make_async_copy(u1_hbm.at[:, blk_ds(blk)], ub.at[slot], dsem.at[1, slot]))))

    def start_streams(n):
        for cond, cps in streams(n):
            pl.when(cond)(functools.partial(start_all, cps))

    def wait_streams(n, which):
        wait_all(streams(n)[which][1])

    def part_writes(n):
        g = jnp.where(n < 8, 2 * n, 2 * n - 16)
        return tuple(pltpu.make_async_copy(ps.at[:, pl.ds(h * LANE, LANE)], part_hbm.at[g + h], psem.at[h])
                     for h in range(2))

    def part_writes_one(n):
        tile = 2 * (n - 32)
        return tuple(pltpu.make_async_copy(ps.at[pl.ds(0, 512), pl.ds(h * LANE, LANE)],
                                           part_hbm.at[32 + (tile + h) // 4, rds(((tile + h) % 4) * 512, 512)],
                                           psem.at[h]) for h in range(2))

    def loop_tiles(count, fn):
        def step(m, carry):
            fn(pl.ds(pl.multiple_of(m * TILE, TILE), TILE))
            return carry
        lax.fori_loop(0, count, step, 0)

    def nt(a, b):
        return lax.dot_general(a, b, (((1,), (1,)), ((), ())), preferred_element_type=F32)

    def piece_dz(n):
        slot, col = n % 2, blk_ds(n % 8)
        wait_streams(n, 0)
        start_streams(n + 1)

        def tile(r):
            rp = jnp.dot(buf_a[r, :], sb[slot], preferred_element_type=F32)
            zd = buf_a[r, col].astype(F32) - zb[slot, r, :].astype(F32)
            dz = (2.0 / (all_rows - 1)) * (rp - mp_ref[:, col]) + (2.0 * INV_WEIGHT / all_rows) * zd
            buf_c[r, col] = dz.astype(BF16)
            lacc[...] += jnp.sum(zd * zd, axis=0, keepdims=True)
        loop_tiles(rows // TILE, tile)

        @pl.when(n == 0)
        def _():
            big(1).wait()

        def grad(r):
            ps[r, :] = jnp.dot(buf_b[r, :], buf_c[:, col], preferred_element_type=F32)
        loop_tiles(dim // TILE, grad)
        start_all(part_writes(n))

    def d_act(d_ref, u_slot, r, vec_ref, col, slot):
        dx = nt(d_ref[r, :], wb[slot])
        nrm = (ub[slot, r, :] - vec_ref[0:1, col]) * vec_ref[1:2, col]
        act = vec_ref[2:3, col] * nrm + vec_ref[3:4, col]
        return jnp.where(act > 0.0, dx, 0.0), nrm

    def piece_stats(n, d_ref, vec_ref, layer, which):
        slot, col = n % 2, blk_ds(n % 8)
        wait_streams(n, which)
        start_streams(n + 1)
        st[layer, 0:2, col] = jnp.zeros((2, BLK), F32)

        def tile(r):
            da, nrm = d_act(d_ref, slot, r, vec_ref, col, slot)
            st[layer, 0:1, col] += jnp.sum(da, axis=0, keepdims=True)
            st[layer, 1:2, col] += jnp.sum(da * nrm, axis=0, keepdims=True)
        loop_tiles(rows // TILE, tile)

    def piece_du(n, d_ref, vec_ref, layer, which, du_ref):
        slot, col = n % 2, blk_ds(n % 8)
        wait_streams(n, which)
        start_streams(n + 1)

        def tile(r):
            da, nrm = d_act(d_ref, slot, r, vec_ref, col, slot)
            du = (vec_ref[1:2, col] * vec_ref[2:3, col]) * (
                da - tot[layer, 0:1, col] / all_rows - nrm * (tot[layer, 1:2, col] / all_rows))
            du_ref[r, col] = du.astype(BF16)
        loop_tiles(rows // TILE, tile)
        return col

    def stat_copies(layer):
        return tuple(remote(st.at[layer], sr.at[layer, idx], tsend.at[layer, d - 1], trecv.at[layer, d - 1], peer(d))
                     for d in range(1, 8))

    def send_stats(layer):
        start_all(stat_copies(layer))

    def finish_stats(layer):
        wait_all(stat_copies(layer))
        sr[layer, idx] = st[layer]
        va = (sr[layer, 0] + sr[layer, 2]) + (sr[layer, 4] + sr[layer, 6])
        vb = (sr[layer, 1] + sr[layer, 3]) + (sr[layer, 5] + sr[layer, 7])
        tot[layer] = jnp.where(c == 0, va, vb)
        grads_ref[layer] = va + vb

    def big(i):
        src = (z_hbm, x2t_hbm, x1t_hbm)[i]
        return pltpu.make_async_copy(src, (buf_a, buf_b, buf_a)[i], bsem.at[i])

    big(0).start()
    start_streams(0)
    big(1).start()
    ht_copy = pltpu.make_async_copy(ht_hbm, ht, bsem.at[3])
    ht_copy.start()
    lacc[...] = jnp.zeros_like(lacc)
    st[...] = jnp.zeros_like(st)
    meet([peer(d) for d in range(1, 8)])
    big(0).wait()

    def tick(it, carry):
        k = it - 1
        stage(k - 6 * LAG, lambda g: wait_all(a0(g)))
        stage(k - 5 * LAG, to_a0)
        stage(k - 4 * LAG, to_a2)
        stage(k - 3 * LAG, to_a1)
        stage(k - 2 * LAG, to_s2)
        stage(k - LAG, to_s1)

        @pl.when(jnp.logical_or(jnp.logical_and(it >= 1, it <= 8), jnp.logical_and(it >= 17, it <= 24)))
        def _():
            wait_all(part_writes(it - 1))

        @pl.when(jnp.logical_and(it >= 29, it <= 36))
        def _():
            wait_all(part_writes_one(it + 3))

        stage(k, to_s0)

        @pl.when(it < 8)
        def _():
            piece_dz(it)

        @pl.when(jnp.logical_and(it >= 8, it < 16))
        def _():
            @pl.when(it == 8)
            def _():
                big(2).start()

            piece_stats(it, buf_c, vec2_ref, 0, 1)

            @pl.when(it == 15)
            def _():
                st[0, 2:3, 0:BLK] = lossv_ref[...] + lacc[...] * (0.5 * INV_WEIGHT / all_rows)
                send_stats(0)

        @pl.when(jnp.logical_and(it >= 16, it < 24))
        def _():
            @pl.when(it == 16)
            def _():
                finish_stats(0)
                loss_ref[...] = jnp.broadcast_to(jnp.sum(grads_ref[0, 2:3, 0:BLK], axis=1, keepdims=True),
                                                 loss_ref.shape)
                big(2).wait()
                ht_copy.wait()

            col = piece_du(it, buf_c, vec2_ref, 0, 1, buf_b)

            def grad(r):
                ps[r, :] = jnp.dot(buf_a[r, :], buf_b[:, col], preferred_element_type=F32)
            loop_tiles(dim // TILE, grad)
            start_all(part_writes(it))

        @pl.when(jnp.logical_and(it >= 24, it < 28))
        def _():
            def two(m, carry):
                piece_stats(24 + 2 * (it - 24) + m, buf_b, vec1_ref, 1, 2)
                return carry
            lax.fori_loop(0, 2, two, 0)

            @pl.when(it == 27)
            def _():
                send_stats(1)

        @pl.when(jnp.logical_and(it >= 28, it < 36))
        def _():
            @pl.when(it == 28)
            def _():
                finish_stats(1)

            n = it + 4
            col = piece_du(n, buf_b, vec1_ref, 1, 2, buf_c)
            ps[0:512, :] = jnp.dot(ht[...], buf_c[:, col], preferred_element_type=F32)
            start_all(part_writes_one(n))

        return carry

    lax.fori_loop(0, GROUPS + 1 + 6 * LAG, tick, 0)


def backward(z, zo, gh, x2t, x1t, ht, w3, w2, u2, u1, mp, vec2, vec1, lossv, all_rows):
    rows, dim = z.shape
    feat = ht.shape[0]
    hbm = pl.BlockSpec(memory_space=pl.ANY)
    vmem = pl.BlockSpec(memory_space=pltpu.VMEM)
    dma = pltpu.SemaphoreType.DMA
    return pl.pallas_call(
        functools.partial(backward_kernel, all_rows),
        out_shape=(jax.ShapeDtypeStruct((GROUPS, dim, LANE), F32), jax.ShapeDtypeStruct((GROUPS, dim, LANE), F32),
                   jax.ShapeDtypeStruct((2, 4, dim), F32), jax.ShapeDtypeStruct((1, LANE), F32)),
        in_specs=[hbm] * 10 + [vmem] * 4,
        out_specs=(hbm, hbm, vmem, vmem),
        scratch_shapes=[
            pltpu.VMEM((rows, dim), BF16), pltpu.VMEM((rows, dim), BF16), pltpu.VMEM((rows, dim), BF16),
            pltpu.VMEM((feat, rows), BF16),
            pltpu.VMEM((2, dim, BLK), BF16), pltpu.VMEM((2, BLK, dim), BF16), pltpu.VMEM((2, rows, BLK), BF16),
            pltpu.VMEM((2, rows, BLK), F32), pltpu.VMEM((dim, BLK), F32),
            pltpu.VMEM((SLOTS, 1024, LANE), F32), pltpu.VMEM((SLOTS, 1024, LANE), F32),
            pltpu.VMEM((2, SLOTS, 256, LANE), F32), pltpu.VMEM((2, SLOTS, 128, LANE), F32),
            pltpu.VMEM((2, 4, dim), F32), pltpu.VMEM((2, 8, 4, dim), F32), pltpu.VMEM((2, 4, dim), F32),
            pltpu.VMEM((1, BLK), F32),
            dma((10, SLOTS)), dma((10, SLOTS)), dma((3, SLOTS)), dma((2, 2)), dma((2,)), dma((4,)),
            dma((2, 7)), dma((2, 7)),
        ],
        compiler_params=pltpu.CompilerParams(collective_id=2, has_side_effects=True, vmem_limit_bytes=67043328),
        cost_estimate=pl.CostEstimate(flops=150 * 10 ** 9, bytes_accessed=200 << 20, transcendentals=0),
    )(z, zo, gh, x2t, x1t, ht, w3, w2, u2, u1, mp, vec2, vec1, lossv)


RING = 16
AHEAD = 8


def join_kernel(groups, w1_out, w2_out, w3_out, buf, lsem, ssem):
    def load(g):
        return pltpu.make_async_copy(groups.at[g], buf.at[g % RING], lsem.at[g % RING])

    def stores(g):
        k = g % RING
        if g < 32:
            out = (w3_out, w2_out)[g // 16]
            return [pltpu.make_async_copy(buf.at[k], out.at[:, pl.ds((g % 16) * LANE, LANE)], ssem.at[k, 0])]
        return [pltpu.make_async_copy(buf.at[k, pl.ds(i * 512, 512)],
                                      w1_out.at[:, pl.ds(((g - 32) * 4 + i) * LANE, LANE)], ssem.at[k, i])
                for i in range(4)]

    for g in range(AHEAD):
        load(g).start()
    for g in range(GROUPS):
        load(g).wait()
        for cp in stores(g):
            cp.start()
        n = g + AHEAD
        if n < GROUPS:
            if n >= RING:
                for cp in stores(n - RING):
                    cp.wait()
            load(n).start()
    for g in range(GROUPS - RING, GROUPS):
        for cp in stores(g):
            cp.wait()


def join(groups, dim):
    hbm = pl.BlockSpec(memory_space=pl.ANY)
    return pl.pallas_call(
        join_kernel,
        out_shape=(jax.ShapeDtypeStruct((512, dim), F32), jax.ShapeDtypeStruct((dim, dim), F32),
                   jax.ShapeDtypeStruct((dim, dim), F32)),
        in_specs=[hbm],
        out_specs=(hbm, hbm, hbm),
        scratch_shapes=[pltpu.VMEM((RING, dim, LANE), F32), pltpu.SemaphoreType.DMA((RING,)),
                        pltpu.SemaphoreType.DMA((RING, 4))],
        compiler_params=pltpu.CompilerParams(vmem_limit_bytes=40 << 20),
        cost_estimate=pl.CostEstimate(flops=0, bytes_accessed=8 * GROUPS * dim * LANE, transcendentals=0),
    )(groups)


def solution(mesh):
    group_devs = mesh.shape['data']

    def local_step(h_a, h_b, w_one, w_two, w_three, gain_one, bias_one, gain_two, bias_two):
        all_rows = h_a.shape[0] * group_devs
        dim = w_two.shape[0]
        vec = jnp.stack([gain_one, bias_one, gain_two, bias_two])
        (u1, _, u2, z, z_other, g_hat, x2t, x1t, ht, stat1, stat2, mean_part, loss_vec) = front(
            h_a, h_b, w_one, w_two, w_three, vec, all_rows)
        groups, _, grads, loss = backward(z, z_other, g_hat, x2t, x1t, ht, w_three, w_two, u2, u1, mean_part, stat2,
                                          stat1, loss_vec, all_rows)
        d_w1, d_w2, d_w3 = join(groups, dim)
        return (loss[0, 0], d_w1, d_w2, d_w3,
                grads[1, 1], grads[1, 0], grads[0, 1], grads[0, 0])

    row_spec = P('data', None)
    return jax.shard_map(local_step, mesh=mesh,
                         in_specs=(row_spec, row_spec, P(), P(), P(), P(), P(), P(), P()),
                         out_specs=(P(), P(), P(), P(), P(), P(), P(), P()),
                         check_vma=False)
```

```python
import functools

import jax
import jax.numpy as jnp
from jax import lax
from jax.experimental import pallas as pl
from jax.experimental.pallas import tpu as pltpu
from jax.sharding import PartitionSpec as P

BN_EPS = 1e-5
STD_EPS = 1e-4
INV_WEIGHT = 2.0
VAR_WEIGHT = 1.0
COV_WEIGHT = 2.0
BLK = 256

F32 = jnp.float32
BF16 = jnp.bfloat16


MESH_ID = pl.DeviceIdType.MESH


def remote(src, dst, send_sem, recv_sem, dev):
    return pltpu.make_async_remote_copy(src_ref=src, dst_ref=dst, send_sem=send_sem, recv_sem=recv_sem,
                                        device_id=(dev,), device_id_type=MESH_ID)


def meet(devs):
    barrier = pltpu.get_barrier_semaphore()
    for dev in devs:
        pl.semaphore_signal(barrier, inc=1, device_id=(dev,), device_id_type=MESH_ID)
    pl.semaphore_wait(barrier, len(devs))


def blk_ds(i):
    return pl.ds(pl.multiple_of(i * BLK, BLK), BLK)


def peer_of(idx, bits, d):
    dev = idx
    for b in range(3):
        if (d >> b) & 1:
            dev = dev + (1 << b) - (2 << b) * bits[b]
    return dev


def front_kernel(all_rows, ha_hbm, hb_hbm, w1_ref, w2_hbm, w3_hbm, vec_ref,
                 u1_hbm, x1_hbm, u2_hbm, z_hbm, zo_hbm, gh_hbm, x2t_hbm, x1t_hbm, ht_hbm,
                 stat1_ref, stat2_ref, mp_ref, loss_ref,
                 hbuf, wblk, xb, z, st, sr, zs, zs_all, mu_ref,
                 part, r1x, r1y, r2x, r2y, s2x, s2y, kx, ky, gb,
                 hsem, wsem, usem, xsem, osem, bsem, tsend, trecv, zsend, zrecv, osend, orecv, ssem, rsem):
    idx = lax.axis_index('data')
    c, x, y, q = idx % 2, (idx // 2) % 2, idx // 4, idx // 2
    bits = (c, x, y)
    nc, nx, ny = [peer_of(idx, bits, d) for d in (1, 2, 4)]
    chips = [peer_of(idx, bits, d) for d in (2, 4, 6)]
    rows, dim = z.shape
    half_rows = rows // 2
    half = BLK // 2
    lo, hi = pl.ds(0, half), pl.ds(half, half)
    tiles = [slice(0, half_rows), slice(half_rows, rows)]

    def start_all(cps):
        for cp in cps:
            cp.start()

    def wait_all(cps):
        for cp in cps:
            cp.wait()

    def views(what):
        for core, mine, other in ((0, ha_hbm, hb_hbm), (1, hb_hbm, ha_hbm)):
            @pl.when(c == core)
            def _():
                own = pltpu.make_async_copy(mine, hbuf.at[pl.ds(0, half_rows)], hsem.at[0])
                sent = remote(other, hbuf.at[pl.ds(half_rows, half_rows)], hsem.at[1], hsem.at[2], nc)
                if what == 'own':
                    own.start()
                elif what == 'send':
                    sent.start()
                    own.wait()
                else:
                    sent.wait()

    def w_copies(s):
        col = blk_ds(s % 8)
        return ((s < 16, pltpu.make_async_copy(w2_hbm.at[:, col], wblk.at[s % 2], wsem.at[s % 2])),
                (jnp.logical_and(s >= 16, s < 24),
                 pltpu.make_async_copy(w3_hbm.at[:, col], wblk.at[s % 2], wsem.at[s % 2])))

    def w_start(s):
        for cond, cp in w_copies(s):
            pl.when(cond)(cp.start)

    def columns(fn):
        def step(nb, carry):
            fn(nb, blk_ds(nb))
            return carry
        lax.fori_loop(0, dim // BLK, step, 0)

    def layers(u):
        def add_sums(layer, m, col, val):
            sums = jnp.concatenate([jnp.sum(val, axis=0, keepdims=True), jnp.sum(val * val, axis=0, keepdims=True)])
            st[layer, :, col] = sums if m == 0 else st[layer, :, col] + sums

        def statistics(layer, stat_ref):
            cps = [remote(st.at[layer], sr.at[layer, q], tsend.at[layer, i], trecv.at[layer, i], dev)
                   for i, dev in enumerate(chips)]
            start_all(cps)
            sr[layer, q] = st[layer]
            wait_all(cps)
            total = (sr[layer, 0] + sr[layer, 1]) + (sr[layer, 2] + sr[layer, 3])
            mean = total[0:1] / all_rows
            var = total[1:2] / all_rows - mean * mean
            stat_ref[0:1, :] = mean
            stat_ref[1:2, :] = lax.rsqrt(var + BN_EPS)
            stat_ref[2:4, :] = vec_ref[2 * layer:2 * layer + 2, :]

        def activate(stat_ref, m, col):
            nrm = (u[tiles[m], col] - stat_ref[0:1, col]) * stat_ref[1:2, col]
            xb[m, :, col] = jnp.maximum(stat_ref[2:3, col] * nrm + stat_ref[3:4, col], 0.0).astype(BF16)

        def u_out(layer, m):
            r = pl.ds(m * half_rows, half_rows)
            return pltpu.make_async_copy(u.at[r], (u1_hbm, u2_hbm)[layer].at[r], usem.at[m])

        def x_out(m):
            return pltpu.make_async_copy(xb.at[m], x1_hbm.at[pl.ds(m * half_rows, half_rows)], xsem.at[m])

        for m in range(2):
            if m == 1:
                views('got')

            def first(nb, col):
                val = jnp.dot(hbuf[tiles[m], :], w1_ref[:, col], preferred_element_type=F32)
                u[tiles[m], col] = val
                add_sums(0, m, col, val)
            columns(first)
            u_out(0, m).start()
        statistics(0, stat1_ref)

        columns(lambda nb, col: activate(stat1_ref, 0, col))
        for m in range(2):
            x_out(m).start()
            u_out(0, m).wait()

            def second(nb, col):
                s = 8 * m + nb
                w_copies(s)[0][1].wait()
                w_start(s + 1)
                val = jnp.dot(xb[m], wblk[s % 2], preferred_element_type=F32)
                if m == 0:
                    activate(stat1_ref, 1, col)
                u[tiles[m], col] = val
                add_sums(1, m, col, val)
            columns(second)
            u_out(1, m).start()
        statistics(1, stat2_ref)
        for m in range(2):
            x_out(m).wait()
            columns(lambda nb, col: activate(stat2_ref, m, col))
        for m in range(2):
            u_out(1, m).wait()

    views('own')
    w_start(0)
    meet([nc] + chips)
    views('send')
    pl.run_scoped(layers, pltpu.VMEM((rows, dim), F32))

    def block_of(o, g):
        b = 4 * g + o
        j = jnp.int32(0)
        for k in range(1, 8):
            j = j + jnp.where(b >= k * (k + 1) // 2, 1, 0)
        return b - j * (j + 1) // 2, j

    def s1(t):
        slot = t % 2
        return (remote(part.at[slot, :, 1 - x, lo, :], r1x.at[t], ssem.at[0, 0, t], rsem.at[0, 0, t], nx),
                remote(part.at[slot, 1 - y, :, hi, :], r1y.at[t], ssem.at[0, 1, t], rsem.at[0, 1, t], ny))

    def s2(t):
        slot = t % 2
        return (remote(s2x.at[slot], r2x.at[t], ssem.at[1, 0, t], rsem.at[1, 0, t], ny),
                remote(s2y.at[slot], r2y.at[t], ssem.at[1, 1, t], rsem.at[1, 1, t], nx))

    def a1(t):
        bx, by = gb.at[t, y, x, lo, :], gb.at[t, y, x, hi, :]
        return (remote(bx, bx, ssem.at[2, 0, t], rsem.at[2, 0, t], ny),
                remote(by, by, ssem.at[2, 1, t], rsem.at[2, 1, t], nx))

    def a2(t):
        bx, by = gb.at[t, :, x, lo, :], gb.at[t, y, :, hi, :]
        return (remote(bx, bx, ssem.at[3, 0, t], rsem.at[3, 0, t], nx),
                remote(by, by, ssem.at[3, 1, t], rsem.at[3, 1, t], ny))

    def z_sums(nb):
        return [remote(zs.at[nb], zs_all.at[q, nb], zsend.at[nb, i], zrecv.at[nb, i], dev)
                for i, dev in enumerate(chips)]

    def other_copies():
        first, second = pl.ds(0, half_rows), pl.ds(half_rows, half_rows)
        return [remote(z.at[second], zo_hbm.at[first], osend.at[0], orecv.at[0], nc),
                remote(z.at[first], zo_hbm.at[second], osend.at[1], orecv.at[1], nc),
                pltpu.make_async_copy(z, z_hbm, osem.at[0])]

    def gram(zt, gh, tin, tout, muc):
        mp_ref[...] = jnp.zeros_like(mp_ref)
        loss_ref[...] = jnp.zeros_like(loss_ref)

        def third(nb):
            col = blk_ds(nb)
            s = 16 + nb
            w_copies(s)[1][1].wait()
            w_start(s + 1)
            sums = jnp.zeros((1, BLK), F32)
            for m in range(2):
                val = jnp.dot(xb[m], wblk[s % 2], preferred_element_type=F32).astype(BF16)
                z[tiles[m], col] = val
                sums = sums + jnp.sum(val.astype(F32), axis=0, keepdims=True)
            zs[nb] = jnp.broadcast_to(sums, (8, BLK))
            start_all(z_sums(nb))
            zt[nb] = z[:, col].T

        def means(nb):
            wait_all(z_sums(nb))
            zs_all[q, nb] = zs[nb]
            total = (zs_all[0, nb] + zs_all[1, nb]) + (zs_all[2, nb] + zs_all[3, nb])
            mu = total[0:1] / all_rows
            mu_ref[:, blk_ds(nb)] = mu
            muc[blk_ds(nb), :] = jnp.broadcast_to(mu, (BLK, BLK)).T

        def each(lo_nb, hi_nb, fn):
            def step(nb, carry):
                fn(nb)
                return carry
            lax.fori_loop(lo_nb, hi_nb, step, 0)

        def new_col(t):
            return (jnp.logical_or(t < 4, jnp.logical_or(t == 5, t == 7)),
                    jnp.where(t < 4, t + 2, (t + 7) // 2))

        def x1_load(n):
            return pltpu.make_async_copy(x1_hbm.at[:, blk_ds(n)], tin, bsem.at[0])

        def store2(n):
            return pltpu.make_async_copy(tout.at[0], x2t_hbm.at[blk_ds(n), :], bsem.at[1])

        def store1(n):
            return pltpu.make_async_copy(tout.at[1], x1t_hbm.at[blk_ds(n), :], bsem.at[2])

        def store_h(n):
            return pltpu.make_async_copy(tout.at[n], ht_hbm.at[pl.ds(n * BLK, BLK), :], bsem.at[1 + n])

        each(0, 2, third)

        def body(t, carry):
            slot = t % 2
            old = (t + 1) % 2
            has_col, nb_new = new_col(t)

            @pl.when(jnp.logical_and(t >= 1, t < 9))
            def _():
                x1_load(t - 1).start()

            @pl.when(jnp.logical_and(t < 9, has_col))
            def _():
                third(nb_new)

            @pl.when(t == 7)
            def _():
                start_all(other_copies())

            @pl.when(t < 9)
            def _():
                for o in range(4):
                    i, j = block_of(o, t)
                    part[slot, o // 2, o % 2] = jnp.dot(zt[i], z[:, blk_ds(j)], preferred_element_type=F32)
                start_all(s1(t))

            @pl.when(jnp.logical_and(t >= 1, t < 10))
            def _():
                g = t - 1
                wait_all(s1(g))
                s2x[old] = part[old, 1 - y, x, lo, :] + r1x[g, 1 - y]
                s2y[old] = part[old, y, 1 - x, hi, :] + r1y[g, 1 - x]
                start_all(s2(g))
                kx[old] = part[old, y, x, lo, :] + r1x[g, y]
                ky[old] = part[old, y, x, hi, :] + r1y[g, x]

            @pl.when(jnp.logical_and(t >= 2, t < 11))
            def _():
                g = t - 2
                had_col, nb_old = new_col(g)

                @pl.when(g == 0)
                def _():
                    each(0, 2, means)

                @pl.when(had_col)
                def _():
                    means(nb_old)

                wait_all(s2(g))
                i, j = block_of(q, g)
                mu_j = mu_ref[:, blk_ds(j)]
                on_diag = i == j
                r_i = lax.broadcasted_iota(jnp.int32, (half, BLK), 0)
                k_i = lax.broadcasted_iota(jnp.int32, (half, BLK), 1)
                for off, k_ref, r_ref in ((0, kx, r2x), (half, ky, r2y)):
                    mu_i = muc[pl.ds(pl.multiple_of(i * BLK + off, half), half), :]
                    cov = (k_ref[slot] + r_ref[g] - all_rows * (mu_i * mu_j)) / (all_rows - 1)
                    diag = jnp.logical_and(r_i + off == k_i, on_diag)
                    std = jnp.sqrt(jnp.where(diag, cov, 1.0) + STD_EPS)
                    g_diag = jnp.where(std < 1.0, -VAR_WEIGHT, 0.0) / (2.0 * std)
                    g_val = jnp.where(diag, g_diag, (2.0 * COV_WEIGHT) * cov)
                    gb[g, y, x, pl.ds(off, half), :] = g_val.astype(BF16)
                    weight = jnp.where(on_diag, COV_WEIGHT, 2.0 * COV_WEIGHT)
                    terms = jnp.where(diag, VAR_WEIGHT * jnp.maximum(1.0 - std, 0.0), weight * cov * cov)
                    loss_ref[...] += jnp.sum(terms, axis=0, keepdims=True)
                start_all(a1(g))

            @pl.when(jnp.logical_and(t >= 3, t < 12))
            def _():
                wait_all(a1(t - 3))
                start_all(a2(t - 3))

            @pl.when(jnp.logical_and(t >= 2, t < 10))
            def _():
                store2(t - 2).wait()
                store1(t - 2).wait()

            @pl.when(jnp.logical_and(t >= 1, t < 9))
            def _():
                band = blk_ds(t - 1)
                for m in range(2):
                    tout[0, :, tiles[m]] = xb[m, :, band].T
                store2(t - 1).start()
                x1_load(t - 1).wait()
                tout[1] = tin[...].T
                store1(t - 1).start()

            @pl.when(t == 9)
            def _():
                for n in range(2):
                    tout[n] = hbuf[:, n * BLK:(n + 1) * BLK].T
                    store_h(n).start()

            @pl.when(t >= 4)
            def _():
                g = t - 4
                wait_all(a2(g))
                for o in range(4):
                    i, j = block_of(o, g)
                    blk = gb[g, o // 2, o % 2]
                    gh[blk_ds(i), blk_ds(j)] = blk
                    mp_ref[:, blk_ds(j)] += jnp.sum(muc[blk_ds(i), :] * blk.astype(F32), axis=0, keepdims=True)

                    @pl.when(i != j)
                    def _():
                        blk_t = gb[g, o // 2, o % 2].T
                        gh[blk_ds(j), blk_ds(i)] = blk_t
                        mp_ref[:, blk_ds(i)] += jnp.sum(muc[blk_ds(j), :] * blk_t.astype(F32), axis=0, keepdims=True)

            return carry

        lax.fori_loop(0, 13, body, 0)
        gh_out = pltpu.make_async_copy(gh, gh_hbm, osem.at[1])
        gh_out.start()
        for n in range(2):
            store_h(n).wait()
        wait_all(other_copies())
        gh_out.wait()

    pl.run_scoped(gram, pltpu.VMEM((8, BLK, rows), BF16), pltpu.VMEM((dim, dim), BF16), pltpu.VMEM((rows, BLK), BF16),
                  pltpu.VMEM((2, BLK, rows), BF16), pltpu.VMEM((dim, BLK), F32))


def front(h_a, h_b, w1, w2, w3, vec, all_rows):
    rows, feat = 2 * h_a.shape[0], h_a.shape[1]
    dim = w2.shape[0]
    half = BLK // 2
    hbm = pl.BlockSpec(memory_space=pl.ANY)
    vmem = pl.BlockSpec(memory_space=pltpu.VMEM)
    dma = pltpu.SemaphoreType.DMA
    shape = jax.ShapeDtypeStruct
    return pl.pallas_call(
        functools.partial(front_kernel, all_rows),
        out_shape=(shape((rows, dim), F32), shape((rows, dim), BF16), shape((rows, dim), F32),
                   shape((rows, dim), BF16), shape((rows, dim), BF16), shape((dim, dim), BF16),
                   shape((dim, rows), BF16), shape((dim, rows), BF16), shape((feat, rows), BF16),
                   shape((4, dim), F32), shape((4, dim), F32), shape((1, dim), F32), shape((1, BLK), F32)),
        in_specs=[hbm, hbm, vmem, hbm, hbm, vmem],
        out_specs=(hbm,) * 9 + (vmem,) * 4,
        scratch_shapes=[
            pltpu.VMEM((rows, feat), BF16), pltpu.VMEM((2, dim, BLK), BF16),
            pltpu.VMEM((2, rows // 2, dim), BF16), pltpu.VMEM((rows, dim), BF16),
            pltpu.VMEM((2, 2, dim), F32), pltpu.VMEM((2, 4, 2, dim), F32),
            pltpu.VMEM((8, 8, BLK), F32), pltpu.VMEM((4, 8, 8, BLK), F32), pltpu.VMEM((1, dim), F32),
            pltpu.VMEM((2, 2, 2, BLK, BLK), F32),
            pltpu.VMEM((9, 2, half, BLK), F32), pltpu.VMEM((9, 2, half, BLK), F32),
            pltpu.VMEM((9, half, BLK), F32), pltpu.VMEM((9, half, BLK), F32),
            pltpu.VMEM((2, half, BLK), F32), pltpu.VMEM((2, half, BLK), F32),
            pltpu.VMEM((2, half, BLK), F32), pltpu.VMEM((2, half, BLK), F32),
            pltpu.VMEM((9, 2, 2, BLK, BLK), BF16),
            dma((3,)), dma((2,)), dma((2,)), dma((2,)), dma((2,)), dma((3,)), dma((2, 3)), dma((2, 3)),
            dma((8, 3)), dma((8, 3)), dma((2,)), dma((2,)), dma((4, 2, 9)), dma((4, 2, 9)),
        ],
        compiler_params=pltpu.CompilerParams(collective_id=3, has_side_effects=True, vmem_limit_bytes=67043328),
        cost_estimate=pl.CostEstimate(flops=50 * 10 ** 9, bytes_accessed=120 << 20, transcendentals=0),
    )(h_a, h_b, w1, w2, w3, vec)


LAG = 2
SLOTS = 6 * LAG
LANE = 128
GROUPS = 36
TILE = 1024


def backward_kernel(all_rows, z_hbm, zo_hbm, gh_hbm, x2t_hbm, x1t_hbm, ht_hbm, w3_hbm, w2_hbm, u2_hbm, u1_hbm,
                    mp_ref, vec2_ref, vec1_ref, lossv_ref,
                    out_hbm, part_hbm, da_hbm, grads_ref, loss_ref,
                    buf_a, buf_b, buf_c, ht, sb, wb, zb, ub, db, ps, own, r0, r1, r2, st, sr, tot, lacc,
                    ssem, rsem, lsem, dsem, psem, bsem, dasem, tsend, trecv):
    idx = lax.axis_index('data')
    c, x, y = idx % 2, (idx // 2) % 2, idx // 4
    bits = (c, x, y)

    def peer(d):
        dev = idx
        for b in range(3):
            if (d >> b) & 1:
                dev = dev + (1 << b) - (2 << b) * bits[b]
        return dev

    nc, nx, ny = peer(1), peer(2), peer(4)
    dim = buf_a.shape[1]
    rows = buf_a.shape[0]

    def rds(start, size):
        return pl.ds(pl.multiple_of(start, size), size)

    row_x, row_y = x * 256 + y * 128, 512 + y * 256 + x * 128

    def s0(g):
        k = g % SLOTS
        return (remote(part_hbm.at[g, rds((1 - c) * 1024, 1024)], r0.at[k], ssem.at[0, k], rsem.at[0, k], nc),)

    def load_own(g):
        k = g % SLOTS
        return pltpu.make_async_copy(part_hbm.at[g, rds(c * 1024, 1024)], own.at[k], lsem.at[0, k])

    def s1(g):
        k = g % SLOTS
        return (remote(own.at[k, rds((1 - x) * 256, 256)], r1.at[0, k], ssem.at[1, k], rsem.at[1, k], nx),
                remote(own.at[k, rds(512 + (1 - y) * 256, 256)], r1.at[1, k], ssem.at[2, k], rsem.at[2, k], ny))

    def s2(g):
        k = g % SLOTS
        return (remote(own.at[k, rds(x * 256 + (1 - y) * 128, 128)], r2.at[0, k], ssem.at[3, k], rsem.at[3, k], ny),
                remote(own.at[k, rds(512 + y * 256 + (1 - x) * 128, 128)], r2.at[1, k], ssem.at[4, k], rsem.at[4, k],
                       nx))

    def a1(g):
        k = g % SLOTS
        ox, oy = out_hbm.at[g, rds(c * 1024 + row_x, 128)], out_hbm.at[g, rds(c * 1024 + row_y, 128)]
        return (remote(own.at[k, rds(row_x, 128)], ox, ssem.at[5, k], rsem.at[5, k], ny),
                remote(own.at[k, rds(row_y, 128)], oy, ssem.at[6, k], rsem.at[6, k], nx),
                pltpu.make_async_copy(own.at[k, rds(row_x, 128)], ox, lsem.at[1, k]),
                pltpu.make_async_copy(own.at[k, rds(row_y, 128)], oy, lsem.at[2, k]))

    def a2(g):
        k = g % SLOTS
        bx, by = out_hbm.at[g, rds(c * 1024 + x * 256, 256)], out_hbm.at[g, rds(c * 1024 + 512 + y * 256, 256)]
        return (remote(bx, bx, ssem.at[7, k], rsem.at[7, k], nx), remote(by, by, ssem.at[8, k], rsem.at[8, k], ny))

    def a0(g):
        k = g % SLOTS
        b = out_hbm.at[g, rds(c * 1024, 1024)]
        return (remote(b, b, ssem.at[9, k], rsem.at[9, k], nc),)

    def stage(g, fn):
        @pl.when(jnp.logical_and(g >= 0, g < GROUPS))
        def _():
            fn(g)

    def wait_all(cps):
        for cp in cps:
            cp.wait()

    def start_all(cps):
        for cp in cps:
            cp.start()

    def to_a0(g):
        wait_all(a2(g))
        start_all(a0(g))

    def to_a2(g):
        wait_all(a1(g))
        start_all(a2(g))

    def to_a1(g):
        wait_all(s2(g))
        k = g % SLOTS
        own[k, rds(row_x, 128)] += r2[0, k]
        own[k, rds(row_y, 128)] += r2[1, k]
        start_all(a1(g))

    def to_s2(g):
        wait_all(s1(g))
        k = g % SLOTS
        own[k, rds(x * 256, 256)] += r1[0, k]
        own[k, rds(512 + y * 256, 256)] += r1[1, k]
        start_all(s2(g))

    def to_s1(g):
        wait_all(s0(g))
        load_own(g).wait()
        k = g % SLOTS
        own[k] += r0[k]
        start_all(s1(g))

    def to_s0(g):
        start_all(s0(g))
        load_own(g).start()

    def streams(n):
        slot = n % 2
        blk = n % 8
        return ((n < 8, (pltpu.make_async_copy(gh_hbm.at[:, blk_ds(blk)], sb.at[slot], dsem.at[0, slot]),
                         pltpu.make_async_copy(zo_hbm.at[:, blk_ds(blk)], zb.at[slot], dsem.at[1, slot]))),
                (jnp.logical_and(n >= 8, n < 16),
                 (pltpu.make_async_copy(w3_hbm.at[blk_ds(blk), :], wb.at[slot], dsem.at[0, slot]),
                  pltpu.make_async_copy(u2_hbm.at[:, blk_ds(blk)], ub.at[slot], dsem.at[1, slot]))),
                (jnp.logical_and(n >= 16, n < 24),
                 (pltpu.make_async_copy(da_hbm.at[blk], db.at[slot], dsem.at[0, slot]),
                  pltpu.make_async_copy(u2_hbm.at[:, blk_ds(blk)], ub.at[slot], dsem.at[1, slot]))),
                (jnp.logical_and(n >= 24, n < 32),
                 (pltpu.make_async_copy(w2_hbm.at[blk_ds(blk), :], wb.at[slot], dsem.at[0, slot]),
                  pltpu.make_async_copy(u1_hbm.at[:, blk_ds(blk)], ub.at[slot], dsem.at[1, slot]))),
                (jnp.logical_and(n >= 32, n < 40),
                 (pltpu.make_async_copy(da_hbm.at[blk], db.at[slot], dsem.at[0, slot]),
                  pltpu.make_async_copy(u1_hbm.at[:, blk_ds(blk)], ub.at[slot], dsem.at[1, slot]))))

    def da_write(n):
        return pltpu.make_async_copy(db.at[n % 2], da_hbm.at[n % 8], dasem.at[n % 2])

    def start_streams(n):
        for cond, cps in streams(n):
            pl.when(cond)(functools.partial(start_all, cps))

    def wait_streams(n, which):
        wait_all(streams(n)[which][1])

    def part_writes(n):
        g = jnp.where(n < 8, 2 * n, 2 * n - 16)
        return tuple(pltpu.make_async_copy(ps.at[:, pl.ds(h * LANE, LANE)], part_hbm.at[g + h], psem.at[h])
                     for h in range(2))

    def part_writes_one(n):
        tile = 2 * (n - 32)
        return tuple(pltpu.make_async_copy(ps.at[rds((n % 2) * 512, 512), pl.ds(h * LANE, LANE)],
                                           part_hbm.at[32 + (tile + h) // 4, rds(((tile + h) % 4) * 512, 512)],
                                           psem.at[2 * (n % 2) + h]) for h in range(2))

    def loop_tiles(count, fn):
        def step(m, carry):
            fn(pl.ds(pl.multiple_of(m * TILE, TILE), TILE))
            return carry
        lax.fori_loop(0, count, step, 0)

    def nt(a, b):
        return lax.dot_general(a, b, (((1,), (1,)), ((), ())), preferred_element_type=F32)

    def piece_dz(n):
        slot, col = n % 2, blk_ds(n % 8)
        wait_streams(n, 0)
        start_streams(n + 1)

        def tile(r):
            rp = jnp.dot(buf_a[r, :], sb[slot], preferred_element_type=F32)
            zd = buf_a[r, col].astype(F32) - zb[slot, r, :].astype(F32)
            dz = (2.0 / (all_rows - 1)) * (rp - mp_ref[:, col]) + (2.0 * INV_WEIGHT / all_rows) * zd
            buf_c[r, col] = dz.astype(BF16)
            lacc[...] += jnp.sum(zd * zd, axis=0, keepdims=True)
        loop_tiles(rows // TILE, tile)

        @pl.when(n == 0)
        def _():
            big(1).wait()

        def grad(r):
            ps[r, :] = jnp.dot(buf_b[r, :], buf_c[:, col], preferred_element_type=F32)
        loop_tiles(dim // TILE, grad)
        start_all(part_writes(n))

    def normed(r, vec_ref, col, slot):
        return (ub[slot, r, :] - vec_ref[0:1, col]) * vec_ref[1:2, col]

    def piece_stats(n, d_ref, vec_ref, layer, which):
        slot, col = n % 2, blk_ds(n % 8)
        wait_streams(n, which)

        @pl.when(n % 8 != 7)
        def _():
            start_streams(n + 1)

        @pl.when(n % 8 >= 2)
        def _():
            da_write(n - 2).wait()
        st[layer, 0:2, col] = jnp.zeros((2, BLK), F32)

        def tile(r):
            dx = nt(d_ref[r, :], wb[slot])
            nrm = normed(r, vec_ref, col, slot)
            da = jnp.where(vec_ref[2:3, col] * nrm + vec_ref[3:4, col] > 0.0, dx, 0.0)
            db[slot, r, :] = da
            st[layer, 0:1, col] += jnp.sum(da, axis=0, keepdims=True)
            st[layer, 1:2, col] += jnp.sum(da * nrm, axis=0, keepdims=True)
        loop_tiles(rows // TILE, tile)
        da_write(n).start()

        @pl.when(n % 8 == 7)
        def _():
            da_write(n - 1).wait()
            da_write(n).wait()
            start_streams(n + 1)

    def piece_du(n, vec_ref, layer, which, du_ref):
        slot, col = n % 2, blk_ds(n % 8)
        wait_streams(n, which)
        start_streams(n + 1)
        scale = vec_ref[1:2, col] * vec_ref[2:3, col]
        mean_da, mean_dan = tot[layer, 0:1, col] / all_rows, tot[layer, 1:2, col] / all_rows

        def tile(r):
            nrm = normed(r, vec_ref, col, slot)
            du_ref[r, col] = (scale * (db[slot, r, :] - mean_da - nrm * mean_dan)).astype(BF16)
        loop_tiles(rows // TILE, tile)
        return col

    def stat_copies(layer):
        return tuple(remote(st.at[layer], sr.at[layer, idx], tsend.at[layer, d - 1], trecv.at[layer, d - 1], peer(d))
                     for d in range(1, 8))

    def send_stats(layer):
        start_all(stat_copies(layer))

    def finish_stats(layer):
        wait_all(stat_copies(layer))
        sr[layer, idx] = st[layer]
        va = (sr[layer, 0] + sr[layer, 2]) + (sr[layer, 4] + sr[layer, 6])
        vb = (sr[layer, 1] + sr[layer, 3]) + (sr[layer, 5] + sr[layer, 7])
        tot[layer] = jnp.where(c == 0, va, vb)
        grads_ref[layer] = va + vb

    def big(i):
        src = (z_hbm, x2t_hbm, x1t_hbm)[i]
        return pltpu.make_async_copy(src, (buf_a, buf_b, buf_a)[i], bsem.at[i])

    big(0).start()
    start_streams(0)
    ht_copy = pltpu.make_async_copy(ht_hbm, ht, bsem.at[3])
    lacc[...] = jnp.zeros_like(lacc)
    st[...] = jnp.zeros_like(st)
    meet([peer(d) for d in range(1, 8)])
    big(0).wait()
    big(1).start()
    ht_copy.start()

    def dz_at(t):
        return (jnp.logical_or(t == 0, jnp.logical_or(t == 2, jnp.logical_and(t >= 4, t < 10))),
                jnp.where(t < 4, t // 2, t - 2))

    def tick(it, carry):
        k = it - 1
        stage(k - 6 * LAG, lambda g: wait_all(a0(g)))
        stage(k - 5 * LAG, to_a0)
        stage(k - 4 * LAG, to_a2)
        stage(k - 3 * LAG, to_a1)
        stage(k - 2 * LAG, to_s2)
        stage(k - LAG, to_s1)

        wrote_dz, dz_piece = dz_at(it - 1)

        @pl.when(wrote_dz)
        def _():
            wait_all(part_writes(dz_piece))

        @pl.when(jnp.logical_and(it >= 17, it <= 24))
        def _():
            wait_all(part_writes(it - 1))

        @pl.when(jnp.logical_and(it >= 33, it <= 36))
        def _():
            wait_all(part_writes_one(2 * it - 34))
            wait_all(part_writes_one(2 * it - 33))

        stage(k, to_s0)

        has_dz, dz_now = dz_at(it)

        @pl.when(has_dz)
        def _():
            piece_dz(dz_now)

        @pl.when(jnp.logical_and(it >= 10, it < 16))
        def _():
            @pl.when(it == 10)
            def _():
                big(2).start()

            twice = jnp.logical_or(it == 10, it == 12)
            first = jnp.where(it == 10, 8, jnp.where(it < 13, it - 1, it))

            def step(n, carry):
                piece_stats(n, buf_c, vec2_ref, 0, 1)
                return carry
            lax.fori_loop(first, first + jnp.where(twice, 2, 1), step, 0)

            @pl.when(it == 15)
            def _():
                st[0, 2:3, 0:BLK] = lossv_ref[...] + lacc[...] * (0.5 * INV_WEIGHT / all_rows)
                send_stats(0)

        @pl.when(jnp.logical_and(it >= 16, it < 24))
        def _():
            @pl.when(it == 16)
            def _():
                finish_stats(0)
                loss_ref[...] = jnp.broadcast_to(jnp.sum(grads_ref[0, 2:3, 0:BLK], axis=1, keepdims=True),
                                                 loss_ref.shape)
                big(2).wait()
                ht_copy.wait()

            col = piece_du(it, vec2_ref, 0, 2, buf_b)

            def grad(r):
                ps[r, :] = jnp.dot(buf_a[r, :], buf_b[:, col], preferred_element_type=F32)
            loop_tiles(dim // TILE, grad)
            start_all(part_writes(it))

        @pl.when(jnp.logical_and(it >= 24, it < 32))
        def _():
            piece_stats(it, buf_b, vec1_ref, 1, 3)

            @pl.when(it == 31)
            def _():
                send_stats(1)

        @pl.when(jnp.logical_and(it >= 32, it < 36))
        def _():
            @pl.when(it == 32)
            def _():
                finish_stats(1)

            def two(m, carry):
                n = 2 * it - 32 + m
                col = piece_du(n, vec1_ref, 1, 4, buf_c)
                ps[rds((n % 2) * 512, 512), :] = jnp.dot(ht[...], buf_c[:, col], preferred_element_type=F32)
                start_all(part_writes_one(n))
                return carry
            lax.fori_loop(0, 2, two, 0)

        return carry

    lax.fori_loop(0, GROUPS + 1 + 6 * LAG, tick, 0)


def backward(z, zo, gh, x2t, x1t, ht, w3, w2, u2, u1, mp, vec2, vec1, lossv, all_rows):
    rows, dim = z.shape
    feat = ht.shape[0]
    hbm = pl.BlockSpec(memory_space=pl.ANY)
    vmem = pl.BlockSpec(memory_space=pltpu.VMEM)
    dma = pltpu.SemaphoreType.DMA
    return pl.pallas_call(
        functools.partial(backward_kernel, all_rows),
        out_shape=(jax.ShapeDtypeStruct((GROUPS, dim, LANE), F32), jax.ShapeDtypeStruct((GROUPS, dim, LANE), F32),
                   jax.ShapeDtypeStruct((8, rows, BLK), F32),
                   jax.ShapeDtypeStruct((2, 4, dim), F32), jax.ShapeDtypeStruct((1, LANE), F32)),
        in_specs=[hbm] * 10 + [vmem] * 4,
        out_specs=(hbm, hbm, hbm, vmem, vmem),
        scratch_shapes=[
            pltpu.VMEM((rows, dim), BF16), pltpu.VMEM((rows, dim), BF16), pltpu.VMEM((rows, dim), BF16),
            pltpu.VMEM((feat, rows), BF16),
            pltpu.VMEM((2, dim, BLK), BF16), pltpu.VMEM((2, BLK, dim), BF16), pltpu.VMEM((2, rows, BLK), BF16),
            pltpu.VMEM((2, rows, BLK), F32), pltpu.VMEM((2, rows, BLK), F32), pltpu.VMEM((dim, BLK), F32),
            pltpu.VMEM((SLOTS, 1024, LANE), F32), pltpu.VMEM((SLOTS, 1024, LANE), F32),
            pltpu.VMEM((2, SLOTS, 256, LANE), F32), pltpu.VMEM((2, SLOTS, 128, LANE), F32),
            pltpu.VMEM((2, 4, dim), F32), pltpu.VMEM((2, 8, 4, dim), F32), pltpu.VMEM((2, 4, dim), F32),
            pltpu.VMEM((1, BLK), F32),
            dma((10, SLOTS)), dma((10, SLOTS)), dma((3, SLOTS)), dma((2, 2)), dma((4,)), dma((4,)), dma((2,)),
            dma((2, 7)), dma((2, 7)),
        ],
        compiler_params=pltpu.CompilerParams(collective_id=2, has_side_effects=True, vmem_limit_bytes=67043328),
        cost_estimate=pl.CostEstimate(flops=150 * 10 ** 9, bytes_accessed=200 << 20, transcendentals=0),
    )(z, zo, gh, x2t, x1t, ht, w3, w2, u2, u1, mp, vec2, vec1, lossv)


RING = 16
AHEAD = 8


def join_kernel(groups, w1_out, w2_out, w3_out, buf, lsem, ssem):
    def load(g):
        return pltpu.make_async_copy(groups.at[g], buf.at[g % RING], lsem.at[g % RING])

    def stores(g):
        k = g % RING
        if g < 32:
            out = (w3_out, w2_out)[g // 16]
            return [pltpu.make_async_copy(buf.at[k], out.at[:, pl.ds((g % 16) * LANE, LANE)], ssem.at[k, 0])]
        return [pltpu.make_async_copy(buf.at[k, pl.ds(i * 512, 512)],
                                      w1_out.at[:, pl.ds(((g - 32) * 4 + i) * LANE, LANE)], ssem.at[k, i])
                for i in range(4)]

    for g in range(AHEAD):
        load(g).start()
    for g in range(GROUPS):
        load(g).wait()
        for cp in stores(g):
            cp.start()
        n = g + AHEAD
        if n < GROUPS:
            if n >= RING:
                for cp in stores(n - RING):
                    cp.wait()
            load(n).start()
    for g in range(GROUPS - RING, GROUPS):
        for cp in stores(g):
            cp.wait()


def join(groups, dim):
    hbm = pl.BlockSpec(memory_space=pl.ANY)
    return pl.pallas_call(
        join_kernel,
        out_shape=(jax.ShapeDtypeStruct((512, dim), F32), jax.ShapeDtypeStruct((dim, dim), F32),
                   jax.ShapeDtypeStruct((dim, dim), F32)),
        in_specs=[hbm],
        out_specs=(hbm, hbm, hbm),
        scratch_shapes=[pltpu.VMEM((RING, dim, LANE), F32), pltpu.SemaphoreType.DMA((RING,)),
                        pltpu.SemaphoreType.DMA((RING, 4))],
        compiler_params=pltpu.CompilerParams(vmem_limit_bytes=40 << 20),
        cost_estimate=pl.CostEstimate(flops=0, bytes_accessed=8 * GROUPS * dim * LANE, transcendentals=0),
    )(groups)


def solution(mesh):
    group_devs = mesh.shape['data']

    def local_step(h_a, h_b, w_one, w_two, w_three, gain_one, bias_one, gain_two, bias_two):
        all_rows = h_a.shape[0] * group_devs
        dim = w_two.shape[0]
        vec = jnp.stack([gain_one, bias_one, gain_two, bias_two])
        (u1, _, u2, z, z_other, g_hat, x2t, x1t, ht, stat1, stat2, mean_part, loss_vec) = front(
            h_a, h_b, w_one, w_two, w_three, vec, all_rows)
        groups, _, _, grads, loss = backward(z, z_other, g_hat, x2t, x1t, ht, w_three, w_two, u2, u1, mean_part, stat2,
                                          stat1, loss_vec, all_rows)
        d_w1, d_w2, d_w3 = join(groups, dim)
        return (loss[0, 0], d_w1, d_w2, d_w3,
                grads[1, 1], grads[1, 0], grads[0, 1], grads[0, 0])

    row_spec = P('data', None)
    return jax.shard_map(local_step, mesh=mesh,
                         in_specs=(row_spec, row_spec, P(), P(), P(), P(), P(), P(), P()),
                         out_specs=(P(), P(), P(), P(), P(), P(), P(), P()),
                         check_vma=False)
```

```python
import functools

import jax
import jax.numpy as jnp
from jax import lax
from jax.experimental import pallas as pl
from jax.experimental.pallas import tpu as pltpu
from jax.sharding import PartitionSpec as P

BN_EPS = 1e-5
STD_EPS = 1e-4
INV_WEIGHT = 2.0
VAR_WEIGHT = 1.0
COV_WEIGHT = 2.0
BLK = 256

F32 = jnp.float32
BF16 = jnp.bfloat16


MESH_ID = pl.DeviceIdType.MESH


def remote(src, dst, send_sem, recv_sem, dev):
    return pltpu.make_async_remote_copy(src_ref=src, dst_ref=dst, send_sem=send_sem, recv_sem=recv_sem,
                                        device_id=(dev,), device_id_type=MESH_ID)


def meet(devs):
    barrier = pltpu.get_barrier_semaphore()
    for dev in devs:
        pl.semaphore_signal(barrier, inc=1, device_id=(dev,), device_id_type=MESH_ID)
    pl.semaphore_wait(barrier, len(devs))


def blk_ds(i):
    return pl.ds(pl.multiple_of(i * BLK, BLK), BLK)


def peer_of(idx, bits, d):
    dev = idx
    for b in range(3):
        if (d >> b) & 1:
            dev = dev + (1 << b) - (2 << b) * bits[b]
    return dev


def front_kernel(all_rows, ha_hbm, hb_hbm, w1_ref, w2_hbm, w3_hbm, vec_ref,
                 u1_hbm, x1_hbm, u2_hbm, z_hbm, zo_hbm, gh_hbm, x2t_hbm, x1t_hbm, ht_hbm,
                 stat1_ref, stat2_ref, mp_ref, loss_ref,
                 hbuf, wblk, xb, z, st, sr, zs, zs_all, mu_ref,
                 part, r1x, r1y, r2x, r2y, s2x, s2y, kx, ky, gb,
                 hsem, wsem, usem, xsem, osem, bsem, tsend, trecv, zsend, zrecv, osend, orecv, ssem, rsem):
    idx = lax.axis_index('data')
    c, x, y, q = idx % 2, (idx // 2) % 2, idx // 4, idx // 2
    bits = (c, x, y)
    nc, nx, ny = [peer_of(idx, bits, d) for d in (1, 2, 4)]
    chips = [peer_of(idx, bits, d) for d in (2, 4, 6)]
    rows, dim = z.shape
    half_rows = rows // 2
    half = BLK // 2
    lo, hi = pl.ds(0, half), pl.ds(half, half)
    tiles = [slice(0, half_rows), slice(half_rows, rows)]

    def start_all(cps):
        for cp in cps:
            cp.start()

    def wait_all(cps):
        for cp in cps:
            cp.wait()

    def views(what):
        for core, mine, other in ((0, ha_hbm, hb_hbm), (1, hb_hbm, ha_hbm)):
            @pl.when(c == core)
            def _():
                own = pltpu.make_async_copy(mine, hbuf.at[pl.ds(0, half_rows)], hsem.at[0])
                sent = remote(other, hbuf.at[pl.ds(half_rows, half_rows)], hsem.at[1], hsem.at[2], nc)
                if what == 'own':
                    own.start()
                elif what == 'send':
                    sent.start()
                    own.wait()
                else:
                    sent.wait()

    def w_copies(s):
        col = blk_ds(s % 8)
        return ((s < 16, pltpu.make_async_copy(w2_hbm.at[:, col], wblk.at[s % 2], wsem.at[s % 2])),
                (jnp.logical_and(s >= 16, s < 24),
                 pltpu.make_async_copy(w3_hbm.at[:, col], wblk.at[s % 2], wsem.at[s % 2])))

    def w_start(s):
        for cond, cp in w_copies(s):
            pl.when(cond)(cp.start)

    def columns(fn):
        def step(nb, carry):
            fn(nb, blk_ds(nb))
            return carry
        lax.fori_loop(0, dim // BLK, step, 0)

    def layers(u):
        def add_sums(layer, m, col, val):
            sums = jnp.concatenate([jnp.sum(val, axis=0, keepdims=True), jnp.sum(val * val, axis=0, keepdims=True)])
            st[layer, :, col] = sums if m == 0 else st[layer, :, col] + sums

        def statistics(layer, stat_ref):
            cps = [remote(st.at[layer], sr.at[layer, q], tsend.at[layer, i], trecv.at[layer, i], dev)
                   for i, dev in enumerate(chips)]
            start_all(cps)
            sr[layer, q] = st[layer]
            wait_all(cps)
            total = (sr[layer, 0] + sr[layer, 1]) + (sr[layer, 2] + sr[layer, 3])
            mean = total[0:1] / all_rows
            var = total[1:2] / all_rows - mean * mean
            stat_ref[0:1, :] = mean
            stat_ref[1:2, :] = lax.rsqrt(var + BN_EPS)
            stat_ref[2:4, :] = vec_ref[2 * layer:2 * layer + 2, :]

        def activate(stat_ref, m, col):
            nrm = (u[tiles[m], col] - stat_ref[0:1, col]) * stat_ref[1:2, col]
            xb[m, :, col] = jnp.maximum(stat_ref[2:3, col] * nrm + stat_ref[3:4, col], 0.0).astype(BF16)

        def u_out(layer, m):
            r = pl.ds(m * half_rows, half_rows)
            return pltpu.make_async_copy(u.at[r], (u1_hbm, u2_hbm)[layer].at[r], usem.at[m])

        def x_out(m):
            return pltpu.make_async_copy(xb.at[m], x1_hbm.at[pl.ds(m * half_rows, half_rows)], xsem.at[m])

        for m in range(2):
            if m == 1:
                views('got')

            def first(nb, col):
                val = jnp.dot(hbuf[tiles[m], :], w1_ref[:, col], preferred_element_type=F32)
                u[tiles[m], col] = val
                add_sums(0, m, col, val)
            columns(first)
            u_out(0, m).start()
        statistics(0, stat1_ref)

        columns(lambda nb, col: activate(stat1_ref, 0, col))
        for m in range(2):
            x_out(m).start()
            u_out(0, m).wait()

            def second(nb, col):
                s = 8 * m + nb
                w_copies(s)[0][1].wait()
                w_start(s + 1)
                val = jnp.dot(xb[m], wblk[s % 2], preferred_element_type=F32)
                if m == 0:
                    activate(stat1_ref, 1, col)
                u[tiles[m], col] = val
                add_sums(1, m, col, val)
            columns(second)
            u_out(1, m).start()
        statistics(1, stat2_ref)
        for m in range(2):
            x_out(m).wait()
            columns(lambda nb, col: activate(stat2_ref, m, col))
        for m in range(2):
            u_out(1, m).wait()

    views('own')
    w_start(0)
    meet([nc] + chips)
    views('send')
    pl.run_scoped(layers, pltpu.VMEM((rows, dim), F32))

    def block_of(o, g):
        b = 4 * g + o
        j = jnp.int32(0)
        for k in range(1, 8):
            j = j + jnp.where(b >= k * (k + 1) // 2, 1, 0)
        return b - j * (j + 1) // 2, j

    def s1(t):
        slot = t % 2
        return (remote(part.at[slot, :, 1 - x, lo, :], r1x.at[t], ssem.at[0, 0, t], rsem.at[0, 0, t], nx),
                remote(part.at[slot, 1 - y, :, hi, :], r1y.at[t], ssem.at[0, 1, t], rsem.at[0, 1, t], ny))

    def s2(t):
        slot = t % 2
        return (remote(s2x.at[slot], r2x.at[t], ssem.at[1, 0, t], rsem.at[1, 0, t], ny),
                remote(s2y.at[slot], r2y.at[t], ssem.at[1, 1, t], rsem.at[1, 1, t], nx))

    def a1(t):
        bx, by = gb.at[t, y, x, lo, :], gb.at[t, y, x, hi, :]
        return (remote(bx, bx, ssem.at[2, 0, t], rsem.at[2, 0, t], ny),
                remote(by, by, ssem.at[2, 1, t], rsem.at[2, 1, t], nx))

    def a2(t):
        bx, by = gb.at[t, :, x, lo, :], gb.at[t, y, :, hi, :]
        return (remote(bx, bx, ssem.at[3, 0, t], rsem.at[3, 0, t], nx),
                remote(by, by, ssem.at[3, 1, t], rsem.at[3, 1, t], ny))

    def z_sums(nb):
        return [remote(zs.at[nb], zs_all.at[q, nb], zsend.at[nb, i], zrecv.at[nb, i], dev)
                for i, dev in enumerate(chips)]

    def other_copies():
        first, second = pl.ds(0, half_rows), pl.ds(half_rows, half_rows)
        return [remote(z.at[second], zo_hbm.at[first], osend.at[0], orecv.at[0], nc),
                remote(z.at[first], zo_hbm.at[second], osend.at[1], orecv.at[1], nc),
                pltpu.make_async_copy(z, z_hbm, osem.at[0])]

    def gram(zt, gh, tin, tout, muc):
        mp_ref[...] = jnp.zeros_like(mp_ref)
        loss_ref[...] = jnp.zeros_like(loss_ref)

        def third(nb):
            col = blk_ds(nb)
            s = 16 + nb
            w_copies(s)[1][1].wait()
            w_start(s + 1)
            sums = jnp.zeros((1, BLK), F32)
            for m in range(2):
                val = jnp.dot(xb[m], wblk[s % 2], preferred_element_type=F32).astype(BF16)
                z[tiles[m], col] = val
                sums = sums + jnp.sum(val.astype(F32), axis=0, keepdims=True)
            zs[nb] = jnp.broadcast_to(sums, (8, BLK))
            start_all(z_sums(nb))
            zt[nb] = z[:, col].T

        def means(nb):
            wait_all(z_sums(nb))
            zs_all[q, nb] = zs[nb]
            total = (zs_all[0, nb] + zs_all[1, nb]) + (zs_all[2, nb] + zs_all[3, nb])
            mu = total[0:1] / all_rows
            mu_ref[:, blk_ds(nb)] = mu
            muc[blk_ds(nb), :] = jnp.broadcast_to(mu, (BLK, BLK)).T

        def each(lo_nb, hi_nb, fn):
            def step(nb, carry):
                fn(nb)
                return carry
            lax.fori_loop(lo_nb, hi_nb, step, 0)

        def new_col(t):
            return (jnp.logical_or(t < 4, jnp.logical_or(t == 5, t == 7)),
                    jnp.where(t < 4, t + 2, (t + 7) // 2))

        def x1_load(n):
            return pltpu.make_async_copy(x1_hbm.at[:, blk_ds(n)], tin, bsem.at[0])

        def store2(n):
            return pltpu.make_async_copy(tout.at[0], x2t_hbm.at[blk_ds(n), :], bsem.at[1])

        def store1(n):
            return pltpu.make_async_copy(tout.at[1], x1t_hbm.at[blk_ds(n), :], bsem.at[2])

        def store_h(n):
            return pltpu.make_async_copy(tout.at[n], ht_hbm.at[pl.ds(n * BLK, BLK), :], bsem.at[1 + n])

        each(0, 2, third)

        def body(t, carry):
            slot = t % 2
            old = (t + 1) % 2
            has_col, nb_new = new_col(t)

            @pl.when(jnp.logical_and(t >= 1, t < 9))
            def _():
                x1_load(t - 1).start()

            @pl.when(jnp.logical_and(t < 9, has_col))
            def _():
                third(nb_new)

            @pl.when(t == 7)
            def _():
                start_all(other_copies())

            @pl.when(t < 9)
            def _():
                for o in range(4):
                    i, j = block_of(o, t)
                    part[slot, o // 2, o % 2] = jnp.dot(zt[i], z[:, blk_ds(j)], preferred_element_type=F32)
                start_all(s1(t))

            @pl.when(jnp.logical_and(t >= 1, t < 10))
            def _():
                g = t - 1
                wait_all(s1(g))
                s2x[old] = part[old, 1 - y, x, lo, :] + r1x[g, 1 - y]
                s2y[old] = part[old, y, 1 - x, hi, :] + r1y[g, 1 - x]
                start_all(s2(g))
                kx[old] = part[old, y, x, lo, :] + r1x[g, y]
                ky[old] = part[old, y, x, hi, :] + r1y[g, x]

            @pl.when(jnp.logical_and(t >= 2, t < 11))
            def _():
                g = t - 2
                had_col, nb_old = new_col(g)

                @pl.when(g == 0)
                def _():
                    each(0, 2, means)

                @pl.when(had_col)
                def _():
                    means(nb_old)

                wait_all(s2(g))
                i, j = block_of(q, g)
                mu_j = mu_ref[:, blk_ds(j)]
                on_diag = i == j
                r_i = lax.broadcasted_iota(jnp.int32, (half, BLK), 0)
                k_i = lax.broadcasted_iota(jnp.int32, (half, BLK), 1)
                for off, k_ref, r_ref in ((0, kx, r2x), (half, ky, r2y)):
                    mu_i = muc[pl.ds(pl.multiple_of(i * BLK + off, half), half), :]
                    cov = (k_ref[slot] + r_ref[g] - all_rows * (mu_i * mu_j)) / (all_rows - 1)
                    diag = jnp.logical_and(r_i + off == k_i, on_diag)
                    std = jnp.sqrt(jnp.where(diag, cov, 1.0) + STD_EPS)
                    g_diag = jnp.where(std < 1.0, -VAR_WEIGHT, 0.0) / (2.0 * std)
                    g_val = jnp.where(diag, g_diag, (2.0 * COV_WEIGHT) * cov)
                    gb[g, y, x, pl.ds(off, half), :] = g_val.astype(BF16)
                    weight = jnp.where(on_diag, COV_WEIGHT, 2.0 * COV_WEIGHT)
                    terms = jnp.where(diag, VAR_WEIGHT * jnp.maximum(1.0 - std, 0.0), weight * cov * cov)
                    loss_ref[...] += jnp.sum(terms, axis=0, keepdims=True)
                start_all(a1(g))

            @pl.when(jnp.logical_and(t >= 3, t < 12))
            def _():
                wait_all(a1(t - 3))
                start_all(a2(t - 3))

            @pl.when(jnp.logical_and(t >= 2, t < 10))
            def _():
                store2(t - 2).wait()
                store1(t - 2).wait()

            @pl.when(jnp.logical_and(t >= 1, t < 9))
            def _():
                band = blk_ds(t - 1)
                for m in range(2):
                    tout[0, :, tiles[m]] = xb[m, :, band].T
                store2(t - 1).start()
                x1_load(t - 1).wait()
                tout[1] = tin[...].T
                store1(t - 1).start()

            @pl.when(t == 9)
            def _():
                for n in range(2):
                    tout[n] = hbuf[:, n * BLK:(n + 1) * BLK].T
                    store_h(n).start()

            @pl.when(t >= 4)
            def _():
                g = t - 4
                wait_all(a2(g))
                for o in range(4):
                    i, j = block_of(o, g)
                    blk = gb[g, o // 2, o % 2]
                    gh[blk_ds(i), blk_ds(j)] = blk
                    mp_ref[:, blk_ds(j)] += jnp.sum(muc[blk_ds(i), :] * blk.astype(F32), axis=0, keepdims=True)

                    @pl.when(i != j)
                    def _():
                        blk_t = gb[g, o // 2, o % 2].T
                        gh[blk_ds(j), blk_ds(i)] = blk_t
                        mp_ref[:, blk_ds(i)] += jnp.sum(muc[blk_ds(j), :] * blk_t.astype(F32), axis=0, keepdims=True)

            return carry

        lax.fori_loop(0, 13, body, 0)
        gh_out = pltpu.make_async_copy(gh, gh_hbm, osem.at[1])
        gh_out.start()
        for n in range(2):
            store_h(n).wait()
        wait_all(other_copies())
        gh_out.wait()

    pl.run_scoped(gram, pltpu.VMEM((8, BLK, rows), BF16), pltpu.VMEM((dim, dim), BF16), pltpu.VMEM((rows, BLK), BF16),
                  pltpu.VMEM((2, BLK, rows), BF16), pltpu.VMEM((dim, BLK), F32))


def front(h_a, h_b, w1, w2, w3, vec, all_rows):
    rows, feat = 2 * h_a.shape[0], h_a.shape[1]
    dim = w2.shape[0]
    half = BLK // 2
    hbm = pl.BlockSpec(memory_space=pl.ANY)
    vmem = pl.BlockSpec(memory_space=pltpu.VMEM)
    dma = pltpu.SemaphoreType.DMA
    shape = jax.ShapeDtypeStruct
    return pl.pallas_call(
        functools.partial(front_kernel, all_rows),
        out_shape=(shape((rows, dim), F32), shape((rows, dim), BF16), shape((rows, dim), F32),
                   shape((rows, dim), BF16), shape((rows, dim), BF16), shape((dim, dim), BF16),
                   shape((dim, rows), BF16), shape((dim, rows), BF16), shape((feat, rows), BF16),
                   shape((4, dim), F32), shape((4, dim), F32), shape((1, dim), F32), shape((1, BLK), F32)),
        in_specs=[hbm, hbm, vmem, hbm, hbm, vmem],
        out_specs=(hbm,) * 9 + (vmem,) * 4,
        scratch_shapes=[
            pltpu.VMEM((rows, feat), BF16), pltpu.VMEM((2, dim, BLK), BF16),
            pltpu.VMEM((2, rows // 2, dim), BF16), pltpu.VMEM((rows, dim), BF16),
            pltpu.VMEM((2, 2, dim), F32), pltpu.VMEM((2, 4, 2, dim), F32),
            pltpu.VMEM((8, 8, BLK), F32), pltpu.VMEM((4, 8, 8, BLK), F32), pltpu.VMEM((1, dim), F32),
            pltpu.VMEM((2, 2, 2, BLK, BLK), F32),
            pltpu.VMEM((9, 2, half, BLK), F32), pltpu.VMEM((9, 2, half, BLK), F32),
            pltpu.VMEM((9, half, BLK), F32), pltpu.VMEM((9, half, BLK), F32),
            pltpu.VMEM((2, half, BLK), F32), pltpu.VMEM((2, half, BLK), F32),
            pltpu.VMEM((2, half, BLK), F32), pltpu.VMEM((2, half, BLK), F32),
            pltpu.VMEM((9, 2, 2, BLK, BLK), BF16),
            dma((3,)), dma((2,)), dma((2,)), dma((2,)), dma((2,)), dma((3,)), dma((2, 3)), dma((2, 3)),
            dma((8, 3)), dma((8, 3)), dma((2,)), dma((2,)), dma((4, 2, 9)), dma((4, 2, 9)),
        ],
        compiler_params=pltpu.CompilerParams(collective_id=3, has_side_effects=True, vmem_limit_bytes=67043328),
        cost_estimate=pl.CostEstimate(flops=50 * 10 ** 9, bytes_accessed=120 << 20, transcendentals=0),
    )(h_a, h_b, w1, w2, w3, vec)


LAG = 2
SLOTS = 6 * LAG
LANE = 128
GROUPS = 36
TILE = 1024


def backward_kernel(all_rows, z_hbm, zo_hbm, gh_hbm, x2t_hbm, x1t_hbm, ht_hbm, w3_hbm, w2_hbm, u2_hbm, u1_hbm,
                    mp_ref, vec2_ref, vec1_ref, lossv_ref,
                    out_hbm, part_hbm, da_hbm, grads_ref, loss_ref,
                    buf_a, buf_b, buf_c, ht, sb, wb, zb, ub, db, ps, own, r0, r1, r2, st, sr, tot, lacc,
                    ssem, rsem, lsem, dsem, psem, bsem, dasem, tsend, trecv):
    idx = lax.axis_index('data')
    c, x, y = idx % 2, (idx // 2) % 2, idx // 4
    bits = (c, x, y)

    def peer(d):
        dev = idx
        for b in range(3):
            if (d >> b) & 1:
                dev = dev + (1 << b) - (2 << b) * bits[b]
        return dev

    nc, nx, ny = peer(1), peer(2), peer(4)
    dim = buf_a.shape[1]
    rows = buf_a.shape[0]

    def rds(start, size):
        return pl.ds(pl.multiple_of(start, size), size)

    row_x, row_y = x * 256 + y * 128, 512 + y * 256 + x * 128

    def s0(g):
        k = g % SLOTS
        return (remote(part_hbm.at[g, rds((1 - c) * 1024, 1024)], r0.at[k], ssem.at[0, k], rsem.at[0, k], nc),)

    def load_own(g):
        k = g % SLOTS
        return pltpu.make_async_copy(part_hbm.at[g, rds(c * 1024, 1024)], own.at[k], lsem.at[0, k])

    def s1(g):
        k = g % SLOTS
        return (remote(own.at[k, rds((1 - x) * 256, 256)], r1.at[0, k], ssem.at[1, k], rsem.at[1, k], nx),
                remote(own.at[k, rds(512 + (1 - y) * 256, 256)], r1.at[1, k], ssem.at[2, k], rsem.at[2, k], ny))

    def s2(g):
        k = g % SLOTS
        return (remote(own.at[k, rds(x * 256 + (1 - y) * 128, 128)], r2.at[0, k], ssem.at[3, k], rsem.at[3, k], ny),
                remote(own.at[k, rds(512 + y * 256 + (1 - x) * 128, 128)], r2.at[1, k], ssem.at[4, k], rsem.at[4, k],
                       nx))

    def a1(g):
        k = g % SLOTS
        ox, oy = out_hbm.at[g, rds(c * 1024 + row_x, 128)], out_hbm.at[g, rds(c * 1024 + row_y, 128)]
        return (remote(own.at[k, rds(row_x, 128)], ox, ssem.at[5, k], rsem.at[5, k], ny),
                remote(own.at[k, rds(row_y, 128)], oy, ssem.at[6, k], rsem.at[6, k], nx),
                pltpu.make_async_copy(own.at[k, rds(row_x, 128)], ox, lsem.at[1, k]),
                pltpu.make_async_copy(own.at[k, rds(row_y, 128)], oy, lsem.at[2, k]))

    def a2(g):
        k = g % SLOTS
        bx, by = out_hbm.at[g, rds(c * 1024 + x * 256, 256)], out_hbm.at[g, rds(c * 1024 + 512 + y * 256, 256)]
        return (remote(bx, bx, ssem.at[7, k], rsem.at[7, k], nx), remote(by, by, ssem.at[8, k], rsem.at[8, k], ny))

    def a0(g):
        k = g % SLOTS
        b = out_hbm.at[g, rds(c * 1024, 1024)]
        return (remote(b, b, ssem.at[9, k], rsem.at[9, k], nc),)

    def stage(g, fn):
        @pl.when(jnp.logical_and(g >= 0, g < GROUPS))
        def _():
            fn(g)

    def wait_all(cps):
        for cp in cps:
            cp.wait()

    def start_all(cps):
        for cp in cps:
            cp.start()

    def to_a0(g):
        wait_all(a2(g))
        start_all(a0(g))

    def to_a2(g):
        wait_all(a1(g))
        start_all(a2(g))

    def to_a1(g):
        wait_all(s2(g))
        k = g % SLOTS
        own[k, rds(row_x, 128)] += r2[0, k]
        own[k, rds(row_y, 128)] += r2[1, k]
        start_all(a1(g))

    def to_s2(g):
        wait_all(s1(g))
        k = g % SLOTS
        own[k, rds(x * 256, 256)] += r1[0, k]
        own[k, rds(512 + y * 256, 256)] += r1[1, k]
        start_all(s2(g))

    def to_s1(g):
        wait_all(s0(g))
        load_own(g).wait()
        k = g % SLOTS
        own[k] += r0[k]
        start_all(s1(g))

    def to_s0(g):
        start_all(s0(g))
        load_own(g).start()

    def streams(n):
        slot = n % 2
        blk = n % 8
        return ((n < 8, (pltpu.make_async_copy(gh_hbm.at[:, blk_ds(blk)], sb.at[slot], dsem.at[0, slot]),
                         pltpu.make_async_copy(zo_hbm.at[:, blk_ds(blk)], zb.at[slot], dsem.at[1, slot]))),
                (jnp.logical_and(n >= 8, n < 16),
                 (pltpu.make_async_copy(w3_hbm.at[blk_ds(blk), :], wb.at[slot], dsem.at[0, slot]),
                  pltpu.make_async_copy(u2_hbm.at[:, blk_ds(blk)], ub.at[slot], dsem.at[1, slot]))),
                (jnp.logical_and(n >= 16, n < 24),
                 (pltpu.make_async_copy(da_hbm.at[blk], db.at[slot], dsem.at[0, slot]),
                  pltpu.make_async_copy(u2_hbm.at[:, blk_ds(blk)], ub.at[slot], dsem.at[1, slot]))),
                (jnp.logical_and(n >= 24, n < 32),
                 (pltpu.make_async_copy(w2_hbm.at[blk_ds(blk), :], wb.at[slot], dsem.at[0, slot]),
                  pltpu.make_async_copy(u1_hbm.at[:, blk_ds(blk)], ub.at[slot], dsem.at[1, slot]))),
                (jnp.logical_and(n >= 32, n < 40),
                 (pltpu.make_async_copy(da_hbm.at[blk], db.at[slot], dsem.at[0, slot]),
                  pltpu.make_async_copy(u1_hbm.at[:, blk_ds(blk)], ub.at[slot], dsem.at[1, slot]))))

    def da_write(n):
        return pltpu.make_async_copy(db.at[n % 2], da_hbm.at[n % 8], dasem.at[n % 2])

    def start_streams(n):
        for cond, cps in streams(n):
            pl.when(cond)(functools.partial(start_all, cps))

    def wait_streams(n, which):
        wait_all(streams(n)[which][1])

    def part_writes(n):
        g = jnp.where(n < 8, 2 * n, 2 * n - 16)
        return tuple(pltpu.make_async_copy(ps.at[:, pl.ds(h * LANE, LANE)], part_hbm.at[g + h], psem.at[h])
                     for h in range(2))

    def part_writes_one(n):
        tile = 2 * (n - 32)
        return tuple(pltpu.make_async_copy(ps.at[rds((n % 2) * 512, 512), pl.ds(h * LANE, LANE)],
                                           part_hbm.at[32 + (tile + h) // 4, rds(((tile + h) % 4) * 512, 512)],
                                           psem.at[2 * (n % 2) + h]) for h in range(2))

    def loop_tiles(count, fn):
        def step(m, carry):
            fn(pl.ds(pl.multiple_of(m * TILE, TILE), TILE))
            return carry
        lax.fori_loop(0, count, step, 0)

    def nt(a, b):
        return lax.dot_general(a, b, (((1,), (1,)), ((), ())), preferred_element_type=F32)

    def piece_dz(n):
        slot, col = n % 2, blk_ds(n % 8)
        wait_streams(n, 0)
        start_streams(n + 1)

        def tile(r):
            rp = jnp.dot(buf_a[r, :], sb[slot], preferred_element_type=F32)
            zd = buf_a[r, col].astype(F32) - zb[slot, r, :].astype(F32)
            dz = (2.0 / (all_rows - 1)) * (rp - mp_ref[:, col]) + (2.0 * INV_WEIGHT / all_rows) * zd
            buf_c[r, col] = dz.astype(BF16)
            lacc[...] += jnp.sum(zd * zd, axis=0, keepdims=True)
        loop_tiles(rows // TILE, tile)

        @pl.when(n == 0)
        def _():
            big(1).wait()

        def grad(r):
            ps[r, :] = jnp.dot(buf_b[r, :], buf_c[:, col], preferred_element_type=F32)
        loop_tiles(dim // TILE, grad)
        start_all(part_writes(n))

    def normed(r, vec_ref, col, slot):
        return (ub[slot, r, :] - vec_ref[0:1, col]) * vec_ref[1:2, col]

    def piece_stats(n, d_ref, vec_ref, layer, which):
        slot, col = n % 2, blk_ds(n % 8)
        wait_streams(n, which)

        @pl.when(n % 8 != 7)
        def _():
            start_streams(n + 1)

        @pl.when(n % 8 >= 2)
        def _():
            da_write(n - 2).wait()
        st[layer, 0:2, col] = jnp.zeros((2, BLK), F32)

        def tile(r):
            dx = nt(d_ref[r, :], wb[slot])
            nrm = normed(r, vec_ref, col, slot)
            da = jnp.where(vec_ref[2:3, col] * nrm + vec_ref[3:4, col] > 0.0, dx, 0.0)
            db[slot, r, :] = da
            st[layer, 0:1, col] += jnp.sum(da, axis=0, keepdims=True)
            st[layer, 1:2, col] += jnp.sum(da * nrm, axis=0, keepdims=True)
        loop_tiles(rows // TILE, tile)
        da_write(n).start()

        @pl.when(n % 8 == 7)
        def _():
            da_write(n - 1).wait()
            da_write(n).wait()
            start_streams(n + 1)

    def piece_du(n, vec_ref, layer, which, du_ref):
        slot, col = n % 2, blk_ds(n % 8)
        wait_streams(n, which)
        start_streams(n + 1)
        scale = vec_ref[1:2, col] * vec_ref[2:3, col]
        mean_da, mean_dan = tot[layer, 0:1, col] / all_rows, tot[layer, 1:2, col] / all_rows

        def tile(r):
            nrm = normed(r, vec_ref, col, slot)
            du_ref[r, col] = (scale * (db[slot, r, :] - mean_da - nrm * mean_dan)).astype(BF16)
        loop_tiles(rows // TILE, tile)
        return col

    def stat_copies(layer):
        return tuple(remote(st.at[layer], sr.at[layer, idx], tsend.at[layer, d - 1], trecv.at[layer, d - 1], peer(d))
                     for d in range(1, 8))

    def send_stats(layer):
        start_all(stat_copies(layer))

    def finish_stats(layer):
        wait_all(stat_copies(layer))
        sr[layer, idx] = st[layer]
        va = (sr[layer, 0] + sr[layer, 2]) + (sr[layer, 4] + sr[layer, 6])
        vb = (sr[layer, 1] + sr[layer, 3]) + (sr[layer, 5] + sr[layer, 7])
        tot[layer] = jnp.where(c == 0, va, vb)
        grads_ref[layer] = va + vb

    def big(i):
        src = (z_hbm, x2t_hbm, x1t_hbm)[i]
        return pltpu.make_async_copy(src, (buf_a, buf_b, buf_a)[i], bsem.at[i])

    big(0).start()
    start_streams(0)
    ht_copy = pltpu.make_async_copy(ht_hbm, ht, bsem.at[3])
    lacc[...] = jnp.zeros_like(lacc)
    st[...] = jnp.zeros_like(st)
    meet([peer(d) for d in range(1, 8)])
    big(0).wait()
    big(1).start()
    ht_copy.start()

    def dz_at(t):
        return (jnp.logical_or(jnp.logical_or(t == 0, t == 2), jnp.logical_or(t == 4, jnp.logical_and(t >= 6, t < 11))),
                jnp.where(t < 6, t // 2, t - 3))

    def tick(it, carry):
        k = it - 1
        stage(k - 6 * LAG, lambda g: wait_all(a0(g)))
        stage(k - 5 * LAG, to_a0)
        stage(k - 4 * LAG, to_a2)
        stage(k - 3 * LAG, to_a1)
        stage(k - 2 * LAG, to_s2)
        stage(k - LAG, to_s1)

        wrote_dz, dz_piece = dz_at(it - 1)

        @pl.when(wrote_dz)
        def _():
            wait_all(part_writes(dz_piece))

        @pl.when(jnp.logical_and(it >= 17, it <= 24))
        def _():
            wait_all(part_writes(it - 1))

        @pl.when(jnp.logical_and(it >= 33, it <= 36))
        def _():
            wait_all(part_writes_one(2 * it - 34))
            wait_all(part_writes_one(2 * it - 33))

        stage(k, to_s0)

        has_dz, dz_now = dz_at(it)

        @pl.when(has_dz)
        def _():
            piece_dz(dz_now)

        @pl.when(jnp.logical_and(it >= 11, it < 16))
        def _():
            @pl.when(it == 11)
            def _():
                big(2).start()

            twice = it < 14
            first = jnp.where(it < 14, 2 * it - 14, it)

            def step(n, carry):
                piece_stats(n, buf_c, vec2_ref, 0, 1)
                return carry
            lax.fori_loop(first, first + jnp.where(twice, 2, 1), step, 0)

            @pl.when(it == 15)
            def _():
                st[0, 2:3, 0:BLK] = lossv_ref[...] + lacc[...] * (0.5 * INV_WEIGHT / all_rows)
                send_stats(0)

        @pl.when(jnp.logical_and(it >= 16, it < 24))
        def _():
            @pl.when(it == 16)
            def _():
                finish_stats(0)
                loss_ref[...] = jnp.broadcast_to(jnp.sum(grads_ref[0, 2:3, 0:BLK], axis=1, keepdims=True),
                                                 loss_ref.shape)
                big(2).wait()
                ht_copy.wait()

            col = piece_du(it, vec2_ref, 0, 2, buf_b)

            def grad(r):
                ps[r, :] = jnp.dot(buf_a[r, :], buf_b[:, col], preferred_element_type=F32)
            loop_tiles(dim // TILE, grad)
            start_all(part_writes(it))

        @pl.when(jnp.logical_and(it >= 24, it < 32))
        def _():
            piece_stats(it, buf_b, vec1_ref, 1, 3)

            @pl.when(it == 31)
            def _():
                send_stats(1)

        @pl.when(jnp.logical_and(it >= 32, it < 36))
        def _():
            @pl.when(it == 32)
            def _():
                finish_stats(1)

            def two(m, carry):
                n = 2 * it - 32 + m
                col = piece_du(n, vec1_ref, 1, 4, buf_c)
                ps[rds((n % 2) * 512, 512), :] = jnp.dot(ht[...], buf_c[:, col], preferred_element_type=F32)
                start_all(part_writes_one(n))
                return carry
            lax.fori_loop(0, 2, two, 0)

        return carry

    lax.fori_loop(0, GROUPS + 1 + 6 * LAG, tick, 0)


def backward(z, zo, gh, x2t, x1t, ht, w3, w2, u2, u1, mp, vec2, vec1, lossv, all_rows):
    rows, dim = z.shape
    feat = ht.shape[0]
    hbm = pl.BlockSpec(memory_space=pl.ANY)
    vmem = pl.BlockSpec(memory_space=pltpu.VMEM)
    dma = pltpu.SemaphoreType.DMA
    return pl.pallas_call(
        functools.partial(backward_kernel, all_rows),
        out_shape=(jax.ShapeDtypeStruct((GROUPS, dim, LANE), F32), jax.ShapeDtypeStruct((GROUPS, dim, LANE), F32),
                   jax.ShapeDtypeStruct((8, rows, BLK), F32),
                   jax.ShapeDtypeStruct((2, 4, dim), F32), jax.ShapeDtypeStruct((1, LANE), F32)),
        in_specs=[hbm] * 10 + [vmem] * 4,
        out_specs=(hbm, hbm, hbm, vmem, vmem),
        scratch_shapes=[
            pltpu.VMEM((rows, dim), BF16), pltpu.VMEM((rows, dim), BF16), pltpu.VMEM((rows, dim), BF16),
            pltpu.VMEM((feat, rows), BF16),
            pltpu.VMEM((2, dim, BLK), BF16), pltpu.VMEM((2, BLK, dim), BF16), pltpu.VMEM((2, rows, BLK), BF16),
            pltpu.VMEM((2, rows, BLK), F32), pltpu.VMEM((2, rows, BLK), F32), pltpu.VMEM((dim, BLK), F32),
            pltpu.VMEM((SLOTS, 1024, LANE), F32), pltpu.VMEM((SLOTS, 1024, LANE), F32),
            pltpu.VMEM((2, SLOTS, 256, LANE), F32), pltpu.VMEM((2, SLOTS, 128, LANE), F32),
            pltpu.VMEM((2, 4, dim), F32), pltpu.VMEM((2, 8, 4, dim), F32), pltpu.VMEM((2, 4, dim), F32),
            pltpu.VMEM((1, BLK), F32),
            dma((10, SLOTS)), dma((10, SLOTS)), dma((3, SLOTS)), dma((2, 2)), dma((4,)), dma((4,)), dma((2,)),
            dma((2, 7)), dma((2, 7)),
        ],
        compiler_params=pltpu.CompilerParams(collective_id=2, has_side_effects=True, vmem_limit_bytes=67043328),
        cost_estimate=pl.CostEstimate(flops=150 * 10 ** 9, bytes_accessed=200 << 20, transcendentals=0),
    )(z, zo, gh, x2t, x1t, ht, w3, w2, u2, u1, mp, vec2, vec1, lossv)


RING = 16
AHEAD = 8


def join_kernel(groups, w1_out, w2_out, w3_out, buf, lsem, ssem):
    def load(g):
        return pltpu.make_async_copy(groups.at[g], buf.at[g % RING], lsem.at[g % RING])

    def stores(g):
        k = g % RING
        if g < 32:
            out = (w3_out, w2_out)[g // 16]
            return [pltpu.make_async_copy(buf.at[k], out.at[:, pl.ds((g % 16) * LANE, LANE)], ssem.at[k, 0])]
        return [pltpu.make_async_copy(buf.at[k, pl.ds(i * 512, 512)],
                                      w1_out.at[:, pl.ds(((g - 32) * 4 + i) * LANE, LANE)], ssem.at[k, i])
                for i in range(4)]

    for g in range(AHEAD):
        load(g).start()
    for g in range(GROUPS):
        load(g).wait()
        for cp in stores(g):
            cp.start()
        n = g + AHEAD
        if n < GROUPS:
            if n >= RING:
                for cp in stores(n - RING):
                    cp.wait()
            load(n).start()
    for g in range(GROUPS - RING, GROUPS):
        for cp in stores(g):
            cp.wait()


def join(groups, dim):
    hbm = pl.BlockSpec(memory_space=pl.ANY)
    return pl.pallas_call(
        join_kernel,
        out_shape=(jax.ShapeDtypeStruct((512, dim), F32), jax.ShapeDtypeStruct((dim, dim), F32),
                   jax.ShapeDtypeStruct((dim, dim), F32)),
        in_specs=[hbm],
        out_specs=(hbm, hbm, hbm),
        scratch_shapes=[pltpu.VMEM((RING, dim, LANE), F32), pltpu.SemaphoreType.DMA((RING,)),
                        pltpu.SemaphoreType.DMA((RING, 4))],
        compiler_params=pltpu.CompilerParams(vmem_limit_bytes=40 << 20),
        cost_estimate=pl.CostEstimate(flops=0, bytes_accessed=8 * GROUPS * dim * LANE, transcendentals=0),
    )(groups)


def solution(mesh):
    group_devs = mesh.shape['data']

    def local_step(h_a, h_b, w_one, w_two, w_three, gain_one, bias_one, gain_two, bias_two):
        all_rows = h_a.shape[0] * group_devs
        dim = w_two.shape[0]
        vec = jnp.stack([gain_one, bias_one, gain_two, bias_two])
        (u1, _, u2, z, z_other, g_hat, x2t, x1t, ht, stat1, stat2, mean_part, loss_vec) = front(
            h_a, h_b, w_one, w_two, w_three, vec, all_rows)
        groups, _, _, grads, loss = backward(z, z_other, g_hat, x2t, x1t, ht, w_three, w_two, u2, u1, mean_part, stat2,
                                          stat1, loss_vec, all_rows)
        d_w1, d_w2, d_w3 = join(groups, dim)
        return (loss[0, 0], d_w1, d_w2, d_w3,
                grads[1, 1], grads[1, 0], grads[0, 1], grads[0, 0])

    row_spec = P('data', None)
    return jax.shard_map(local_step, mesh=mesh,
                         in_specs=(row_spec, row_spec, P(), P(), P(), P(), P(), P(), P()),
                         out_specs=(P(), P(), P(), P(), P(), P(), P(), P()),
                         check_vma=False)
```

```python
import functools

import jax
import jax.numpy as jnp
from jax import lax
from jax.experimental import pallas as pl
from jax.experimental.pallas import tpu as pltpu
from jax.sharding import PartitionSpec as P

BN_EPS = 1e-5
STD_EPS = 1e-4
INV_WEIGHT = 2.0
VAR_WEIGHT = 1.0
COV_WEIGHT = 2.0
BLK = 256

F32 = jnp.float32
BF16 = jnp.bfloat16


MESH_ID = pl.DeviceIdType.MESH


def remote(src, dst, send_sem, recv_sem, dev):
    return pltpu.make_async_remote_copy(src_ref=src, dst_ref=dst, send_sem=send_sem, recv_sem=recv_sem,
                                        device_id=(dev,), device_id_type=MESH_ID)


def meet(devs):
    barrier = pltpu.get_barrier_semaphore()
    for dev in devs:
        pl.semaphore_signal(barrier, inc=1, device_id=(dev,), device_id_type=MESH_ID)
    pl.semaphore_wait(barrier, len(devs))


def blk_ds(i):
    return pl.ds(pl.multiple_of(i * BLK, BLK), BLK)


def peer_of(idx, bits, d):
    dev = idx
    for b in range(3):
        if (d >> b) & 1:
            dev = dev + (1 << b) - (2 << b) * bits[b]
    return dev


def front_kernel(all_rows, ha_hbm, hb_hbm, w1_ref, w2_hbm, w3_hbm, vec_ref,
                 u1_hbm, x1_hbm, u2_hbm, z_hbm, zo_hbm, gh_hbm, x2t_hbm, x1t_hbm, ht_hbm,
                 stat1_ref, stat2_ref, mp_ref, loss_ref,
                 hbuf, wblk, xb, z, st, sr, zs, zs_all, mu_ref,
                 part, r1x, r1y, r2x, r2y, s2x, s2y, kx, ky, gb,
                 hsem, wsem, usem, xsem, osem, bsem, tsend, trecv, zsend, zrecv, osend, orecv, ssem, rsem):
    idx = lax.axis_index('data')
    c, x, y, q = idx % 2, (idx // 2) % 2, idx // 4, idx // 2
    bits = (c, x, y)
    nc, nx, ny = [peer_of(idx, bits, d) for d in (1, 2, 4)]
    chips = [peer_of(idx, bits, d) for d in (2, 4, 6)]
    rows, dim = z.shape
    half_rows = rows // 2
    half = BLK // 2
    lo, hi = pl.ds(0, half), pl.ds(half, half)
    tiles = [slice(0, half_rows), slice(half_rows, rows)]

    def start_all(cps):
        for cp in cps:
            cp.start()

    def wait_all(cps):
        for cp in cps:
            cp.wait()

    def views(what):
        for core, mine, other in ((0, ha_hbm, hb_hbm), (1, hb_hbm, ha_hbm)):
            @pl.when(c == core)
            def _():
                own = pltpu.make_async_copy(mine, hbuf.at[pl.ds(0, half_rows)], hsem.at[0])
                sent = remote(other, hbuf.at[pl.ds(half_rows, half_rows)], hsem.at[1], hsem.at[2], nc)
                if what == 'own':
                    own.start()
                elif what == 'send':
                    sent.start()
                    own.wait()
                else:
                    sent.wait()

    def w_copies(s):
        col = blk_ds(s % 8)
        return ((s < 16, pltpu.make_async_copy(w2_hbm.at[:, col], wblk.at[s % 2], wsem.at[s % 2])),
                (jnp.logical_and(s >= 16, s < 24),
                 pltpu.make_async_copy(w3_hbm.at[:, col], wblk.at[s % 2], wsem.at[s % 2])))

    def w_start(s):
        for cond, cp in w_copies(s):
            pl.when(cond)(cp.start)

    def columns(fn):
        def step(nb, carry):
            fn(nb, blk_ds(nb))
            return carry
        lax.fori_loop(0, dim // BLK, step, 0)

    def layers(u):
        def add_sums(layer, m, col, val):
            sums = jnp.concatenate([jnp.sum(val, axis=0, keepdims=True), jnp.sum(val * val, axis=0, keepdims=True)])
            st[layer, :, col] = sums if m == 0 else st[layer, :, col] + sums

        def statistics(layer, stat_ref):
            cps = [remote(st.at[layer], sr.at[layer, q], tsend.at[layer, i], trecv.at[layer, i], dev)
                   for i, dev in enumerate(chips)]
            start_all(cps)
            sr[layer, q] = st[layer]
            wait_all(cps)
            total = (sr[layer, 0] + sr[layer, 1]) + (sr[layer, 2] + sr[layer, 3])
            mean = total[0:1] / all_rows
            var = total[1:2] / all_rows - mean * mean
            stat_ref[0:1, :] = mean
            stat_ref[1:2, :] = lax.rsqrt(var + BN_EPS)
            stat_ref[2:4, :] = vec_ref[2 * layer:2 * layer + 2, :]

        def activate(stat_ref, m, col):
            nrm = (u[tiles[m], col] - stat_ref[0:1, col]) * stat_ref[1:2, col]
            xb[m, :, col] = jnp.maximum(stat_ref[2:3, col] * nrm + stat_ref[3:4, col], 0.0).astype(BF16)

        def u_out(layer, m):
            r = pl.ds(m * half_rows, half_rows)
            return pltpu.make_async_copy(u.at[r], (u1_hbm, u2_hbm)[layer].at[r], usem.at[m])

        def x_out(m):
            return pltpu.make_async_copy(xb.at[m], x1_hbm.at[pl.ds(m * half_rows, half_rows)], xsem.at[m])

        for m in range(2):
            if m == 1:
                views('got')

            def first(nb, col):
                val = jnp.dot(hbuf[tiles[m], :], w1_ref[:, col], preferred_element_type=F32)
                u[tiles[m], col] = val
                add_sums(0, m, col, val)
            columns(first)
            u_out(0, m).start()
        statistics(0, stat1_ref)

        columns(lambda nb, col: activate(stat1_ref, 0, col))
        for m in range(2):
            x_out(m).start()
            u_out(0, m).wait()

            def second(nb, col):
                s = 8 * m + nb
                w_copies(s)[0][1].wait()
                w_start(s + 1)
                val = jnp.dot(xb[m], wblk[s % 2], preferred_element_type=F32)
                if m == 0:
                    activate(stat1_ref, 1, col)
                u[tiles[m], col] = val
                add_sums(1, m, col, val)
            columns(second)
            u_out(1, m).start()
        statistics(1, stat2_ref)
        for m in range(2):
            x_out(m).wait()
            columns(lambda nb, col: activate(stat2_ref, m, col))
        for m in range(2):
            u_out(1, m).wait()

    views('own')
    w_start(0)
    meet([nc] + chips)
    views('send')
    pl.run_scoped(layers, pltpu.VMEM((rows, dim), F32))

    def block_of(o, g):
        b = 4 * g + o
        j = jnp.int32(0)
        for k in range(1, 8):
            j = j + jnp.where(b >= k * (k + 1) // 2, 1, 0)
        return b - j * (j + 1) // 2, j

    def s1(t):
        slot = t % 2
        return (remote(part.at[slot, :, 1 - x, lo, :], r1x.at[t], ssem.at[0, 0, t], rsem.at[0, 0, t], nx),
                remote(part.at[slot, 1 - y, :, hi, :], r1y.at[t], ssem.at[0, 1, t], rsem.at[0, 1, t], ny))

    def s2(t):
        slot = t % 2
        return (remote(s2x.at[slot], r2x.at[t], ssem.at[1, 0, t], rsem.at[1, 0, t], ny),
                remote(s2y.at[slot], r2y.at[t], ssem.at[1, 1, t], rsem.at[1, 1, t], nx))

    def a1(t):
        bx, by = gb.at[t, y, x, lo, :], gb.at[t, y, x, hi, :]
        return (remote(bx, bx, ssem.at[2, 0, t], rsem.at[2, 0, t], ny),
                remote(by, by, ssem.at[2, 1, t], rsem.at[2, 1, t], nx))

    def a2(t):
        bx, by = gb.at[t, :, x, lo, :], gb.at[t, y, :, hi, :]
        return (remote(bx, bx, ssem.at[3, 0, t], rsem.at[3, 0, t], nx),
                remote(by, by, ssem.at[3, 1, t], rsem.at[3, 1, t], ny))

    def z_sums(nb):
        return [remote(zs.at[nb], zs_all.at[q, nb], zsend.at[nb, i], zrecv.at[nb, i], dev)
                for i, dev in enumerate(chips)]

    def other_copies():
        first, second = pl.ds(0, half_rows), pl.ds(half_rows, half_rows)
        return [remote(z.at[second], zo_hbm.at[first], osend.at[0], orecv.at[0], nc),
                remote(z.at[first], zo_hbm.at[second], osend.at[1], orecv.at[1], nc),
                pltpu.make_async_copy(z, z_hbm, osem.at[0])]

    def gram(zt, gh, tin, tout, muc):
        mp_ref[...] = jnp.zeros_like(mp_ref)
        loss_ref[...] = jnp.zeros_like(loss_ref)

        def third(nb):
            col = blk_ds(nb)
            s = 16 + nb
            w_copies(s)[1][1].wait()
            w_start(s + 1)
            sums = jnp.zeros((1, BLK), F32)
            for m in range(2):
                val = jnp.dot(xb[m], wblk[s % 2], preferred_element_type=F32).astype(BF16)
                z[tiles[m], col] = val
                sums = sums + jnp.sum(val.astype(F32), axis=0, keepdims=True)
            zs[nb] = jnp.broadcast_to(sums, (8, BLK))
            start_all(z_sums(nb))
            zt[nb] = z[:, col].T

        def means(nb):
            wait_all(z_sums(nb))
            zs_all[q, nb] = zs[nb]
            total = (zs_all[0, nb] + zs_all[1, nb]) + (zs_all[2, nb] + zs_all[3, nb])
            mu = total[0:1] / all_rows
            mu_ref[:, blk_ds(nb)] = mu
            muc[blk_ds(nb), :] = jnp.broadcast_to(mu, (BLK, BLK)).T

        def each(lo_nb, hi_nb, fn):
            def step(nb, carry):
                fn(nb)
                return carry
            lax.fori_loop(lo_nb, hi_nb, step, 0)

        def new_col(t):
            return (jnp.logical_or(t < 4, jnp.logical_or(t == 5, t == 7)),
                    jnp.where(t < 4, t + 2, (t + 7) // 2))

        def x1_load(n):
            return pltpu.make_async_copy(x1_hbm.at[:, blk_ds(n)], tin, bsem.at[0])

        def store2(n):
            return pltpu.make_async_copy(tout.at[0], x2t_hbm.at[blk_ds(n), :], bsem.at[1])

        def store1(n):
            return pltpu.make_async_copy(tout.at[1], x1t_hbm.at[blk_ds(n), :], bsem.at[2])

        def store_h(n):
            return pltpu.make_async_copy(tout.at[n], ht_hbm.at[pl.ds(n * BLK, BLK), :], bsem.at[1 + n])

        each(0, 2, third)

        def body(t, carry):
            slot = t % 2
            old = (t + 1) % 2
            has_col, nb_new = new_col(t)

            @pl.when(jnp.logical_and(t >= 1, t < 9))
            def _():
                x1_load(t - 1).start()

            @pl.when(jnp.logical_and(t < 9, has_col))
            def _():
                third(nb_new)

            @pl.when(t == 7)
            def _():
                start_all(other_copies())

            @pl.when(t < 9)
            def _():
                for o in range(4):
                    i, j = block_of(o, t)
                    part[slot, o // 2, o % 2] = jnp.dot(zt[i], z[:, blk_ds(j)], preferred_element_type=F32)
                start_all(s1(t))

            @pl.when(jnp.logical_and(t >= 1, t < 10))
            def _():
                g = t - 1
                wait_all(s1(g))
                s2x[old] = part[old, 1 - y, x, lo, :] + r1x[g, 1 - y]
                s2y[old] = part[old, y, 1 - x, hi, :] + r1y[g, 1 - x]
                start_all(s2(g))
                kx[old] = part[old, y, x, lo, :] + r1x[g, y]
                ky[old] = part[old, y, x, hi, :] + r1y[g, x]

            @pl.when(jnp.logical_and(t >= 2, t < 11))
            def _():
                g = t - 2
                had_col, nb_old = new_col(g)

                @pl.when(g == 0)
                def _():
                    each(0, 2, means)

                @pl.when(had_col)
                def _():
                    means(nb_old)

                wait_all(s2(g))
                i, j = block_of(q, g)
                mu_j = mu_ref[:, blk_ds(j)]
                on_diag = i == j
                r_i = lax.broadcasted_iota(jnp.int32, (half, BLK), 0)
                k_i = lax.broadcasted_iota(jnp.int32, (half, BLK), 1)
                for off, k_ref, r_ref in ((0, kx, r2x), (half, ky, r2y)):
                    mu_i = muc[pl.ds(pl.multiple_of(i * BLK + off, half), half), :]
                    cov = (k_ref[slot] + r_ref[g] - all_rows * (mu_i * mu_j)) / (all_rows - 1)
                    diag = jnp.logical_and(r_i + off == k_i, on_diag)
                    std = jnp.sqrt(jnp.where(diag, cov, 1.0) + STD_EPS)
                    g_diag = jnp.where(std < 1.0, -VAR_WEIGHT, 0.0) / (2.0 * std)
                    g_val = jnp.where(diag, g_diag, (2.0 * COV_WEIGHT) * cov)
                    gb[g, y, x, pl.ds(off, half), :] = g_val.astype(BF16)
                    weight = jnp.where(on_diag, COV_WEIGHT, 2.0 * COV_WEIGHT)
                    terms = jnp.where(diag, VAR_WEIGHT * jnp.maximum(1.0 - std, 0.0), weight * cov * cov)
                    loss_ref[...] += jnp.sum(terms, axis=0, keepdims=True)
                start_all(a1(g))

            @pl.when(jnp.logical_and(t >= 3, t < 12))
            def _():
                wait_all(a1(t - 3))
                start_all(a2(t - 3))

            @pl.when(jnp.logical_and(t >= 2, t < 10))
            def _():
                store2(t - 2).wait()
                store1(t - 2).wait()

            @pl.when(jnp.logical_and(t >= 1, t < 9))
            def _():
                band = blk_ds(t - 1)
                for m in range(2):
                    tout[0, :, tiles[m]] = xb[m, :, band].T
                store2(t - 1).start()
                x1_load(t - 1).wait()
                tout[1] = tin[...].T
                store1(t - 1).start()

            @pl.when(t == 9)
            def _():
                for n in range(2):
                    tout[n] = hbuf[:, n * BLK:(n + 1) * BLK].T
                    store_h(n).start()

            @pl.when(t >= 4)
            def _():
                g = t - 4
                wait_all(a2(g))
                for o in range(4):
                    i, j = block_of(o, g)
                    blk = gb[g, o // 2, o % 2]
                    gh[blk_ds(i), blk_ds(j)] = blk
                    mp_ref[:, blk_ds(j)] += jnp.sum(muc[blk_ds(i), :] * blk.astype(F32), axis=0, keepdims=True)

                    @pl.when(i != j)
                    def _():
                        blk_t = gb[g, o // 2, o % 2].T
                        gh[blk_ds(j), blk_ds(i)] = blk_t
                        mp_ref[:, blk_ds(i)] += jnp.sum(muc[blk_ds(j), :] * blk_t.astype(F32), axis=0, keepdims=True)

            return carry

        lax.fori_loop(0, 13, body, 0)
        gh_out = pltpu.make_async_copy(gh, gh_hbm, osem.at[1])
        gh_out.start()
        for n in range(2):
            store_h(n).wait()
        wait_all(other_copies())
        gh_out.wait()

    pl.run_scoped(gram, pltpu.VMEM((8, BLK, rows), BF16), pltpu.VMEM((dim, dim), BF16), pltpu.VMEM((rows, BLK), BF16),
                  pltpu.VMEM((2, BLK, rows), BF16), pltpu.VMEM((dim, BLK), F32))


def front(h_a, h_b, w1, w2, w3, vec, all_rows):
    rows, feat = 2 * h_a.shape[0], h_a.shape[1]
    dim = w2.shape[0]
    half = BLK // 2
    hbm = pl.BlockSpec(memory_space=pl.ANY)
    vmem = pl.BlockSpec(memory_space=pltpu.VMEM)
    dma = pltpu.SemaphoreType.DMA
    shape = jax.ShapeDtypeStruct
    return pl.pallas_call(
        functools.partial(front_kernel, all_rows),
        out_shape=(shape((rows, dim), F32), shape((rows, dim), BF16), shape((rows, dim), F32),
                   shape((rows, dim), BF16), shape((rows, dim), BF16), shape((dim, dim), BF16),
                   shape((dim, rows), BF16), shape((dim, rows), BF16), shape((feat, rows), BF16),
                   shape((4, dim), F32), shape((4, dim), F32), shape((1, dim), F32), shape((1, BLK), F32)),
        in_specs=[hbm, hbm, vmem, hbm, hbm, vmem],
        out_specs=(hbm,) * 9 + (vmem,) * 4,
        scratch_shapes=[
            pltpu.VMEM((rows, feat), BF16), pltpu.VMEM((2, dim, BLK), BF16),
            pltpu.VMEM((2, rows // 2, dim), BF16), pltpu.VMEM((rows, dim), BF16),
            pltpu.VMEM((2, 2, dim), F32), pltpu.VMEM((2, 4, 2, dim), F32),
            pltpu.VMEM((8, 8, BLK), F32), pltpu.VMEM((4, 8, 8, BLK), F32), pltpu.VMEM((1, dim), F32),
            pltpu.VMEM((2, 2, 2, BLK, BLK), F32),
            pltpu.VMEM((9, 2, half, BLK), F32), pltpu.VMEM((9, 2, half, BLK), F32),
            pltpu.VMEM((9, half, BLK), F32), pltpu.VMEM((9, half, BLK), F32),
            pltpu.VMEM((2, half, BLK), F32), pltpu.VMEM((2, half, BLK), F32),
            pltpu.VMEM((2, half, BLK), F32), pltpu.VMEM((2, half, BLK), F32),
            pltpu.VMEM((9, 2, 2, BLK, BLK), BF16),
            dma((3,)), dma((2,)), dma((2,)), dma((2,)), dma((2,)), dma((3,)), dma((2, 3)), dma((2, 3)),
            dma((8, 3)), dma((8, 3)), dma((2,)), dma((2,)), dma((4, 2, 9)), dma((4, 2, 9)),
        ],
        compiler_params=pltpu.CompilerParams(collective_id=3, has_side_effects=True, vmem_limit_bytes=67043328),
        cost_estimate=pl.CostEstimate(flops=50 * 10 ** 9, bytes_accessed=120 << 20, transcendentals=0),
    )(h_a, h_b, w1, w2, w3, vec)


LAG = 2
SLOTS = 6 * LAG
LANE = 128
GROUPS = 36
TILE = 1024


def backward_kernel(all_rows, z_hbm, zo_hbm, gh_hbm, x2t_hbm, x1t_hbm, ht_hbm, w3_hbm, w2_hbm, u2_hbm, u1_hbm,
                    mp_ref, vec2_ref, vec1_ref, lossv_ref,
                    out_hbm, part_hbm, da_hbm, grads_ref, loss_ref,
                    buf_a, buf_b, buf_c, ht, sb, wb, zb, ub, db, ps, own, r0, r1, r2, st, sr, tot, lacc,
                    ssem, rsem, lsem, dsem, psem, bsem, dasem, tsend, trecv):
    idx = lax.axis_index('data')
    c, x, y = idx % 2, (idx // 2) % 2, idx // 4
    bits = (c, x, y)

    def peer(d):
        dev = idx
        for b in range(3):
            if (d >> b) & 1:
                dev = dev + (1 << b) - (2 << b) * bits[b]
        return dev

    nc, nx, ny = peer(1), peer(2), peer(4)
    dim = buf_a.shape[1]
    rows = buf_a.shape[0]

    def rds(start, size):
        return pl.ds(pl.multiple_of(start, size), size)

    row_x, row_y = x * 256 + y * 128, 512 + y * 256 + x * 128

    def s0(g):
        k = g % SLOTS
        return (remote(part_hbm.at[g, rds((1 - c) * 1024, 1024)], r0.at[k], ssem.at[0, k], rsem.at[0, k], nc),)

    def load_own(g):
        k = g % SLOTS
        return pltpu.make_async_copy(part_hbm.at[g, rds(c * 1024, 1024)], own.at[k], lsem.at[0, k])

    def s1(g):
        k = g % SLOTS
        return (remote(own.at[k, rds((1 - x) * 256, 256)], r1.at[0, k], ssem.at[1, k], rsem.at[1, k], nx),
                remote(own.at[k, rds(512 + (1 - y) * 256, 256)], r1.at[1, k], ssem.at[2, k], rsem.at[2, k], ny))

    def s2(g):
        k = g % SLOTS
        return (remote(own.at[k, rds(x * 256 + (1 - y) * 128, 128)], r2.at[0, k], ssem.at[3, k], rsem.at[3, k], ny),
                remote(own.at[k, rds(512 + y * 256 + (1 - x) * 128, 128)], r2.at[1, k], ssem.at[4, k], rsem.at[4, k],
                       nx))

    def a1(g):
        k = g % SLOTS
        ox, oy = out_hbm.at[g, rds(c * 1024 + row_x, 128)], out_hbm.at[g, rds(c * 1024 + row_y, 128)]
        return (remote(own.at[k, rds(row_x, 128)], ox, ssem.at[5, k], rsem.at[5, k], ny),
                remote(own.at[k, rds(row_y, 128)], oy, ssem.at[6, k], rsem.at[6, k], nx),
                pltpu.make_async_copy(own.at[k, rds(row_x, 128)], ox, lsem.at[1, k]),
                pltpu.make_async_copy(own.at[k, rds(row_y, 128)], oy, lsem.at[2, k]))

    def a2(g):
        k = g % SLOTS
        bx, by = out_hbm.at[g, rds(c * 1024 + x * 256, 256)], out_hbm.at[g, rds(c * 1024 + 512 + y * 256, 256)]
        return (remote(bx, bx, ssem.at[7, k], rsem.at[7, k], nx), remote(by, by, ssem.at[8, k], rsem.at[8, k], ny))

    def a0(g):
        k = g % SLOTS
        b = out_hbm.at[g, rds(c * 1024, 1024)]
        return (remote(b, b, ssem.at[9, k], rsem.at[9, k], nc),)

    def stage(g, fn):
        @pl.when(jnp.logical_and(g >= 0, g < GROUPS))
        def _():
            fn(g)

    def wait_all(cps):
        for cp in cps:
            cp.wait()

    def start_all(cps):
        for cp in cps:
            cp.start()

    def to_a0(g):
        wait_all(a2(g))
        start_all(a0(g))

    def to_a2(g):
        wait_all(a1(g))
        start_all(a2(g))

    def to_a1(g):
        wait_all(s2(g))
        k = g % SLOTS
        own[k, rds(row_x, 128)] += r2[0, k]
        own[k, rds(row_y, 128)] += r2[1, k]
        start_all(a1(g))

    def to_s2(g):
        wait_all(s1(g))
        k = g % SLOTS
        own[k, rds(x * 256, 256)] += r1[0, k]
        own[k, rds(512 + y * 256, 256)] += r1[1, k]
        start_all(s2(g))

    def to_s1(g):
        wait_all(s0(g))
        load_own(g).wait()
        k = g % SLOTS
        own[k] += r0[k]
        start_all(s1(g))

    def to_s0(g):
        start_all(s0(g))
        load_own(g).start()

    def streams(n):
        slot = n % 2
        blk = n % 8
        return ((n < 8, (pltpu.make_async_copy(gh_hbm.at[:, blk_ds(blk)], sb.at[slot], dsem.at[0, slot]),
                         pltpu.make_async_copy(zo_hbm.at[:, blk_ds(blk)], zb.at[slot], dsem.at[1, slot]))),
                (jnp.logical_and(n >= 8, n < 16),
                 (pltpu.make_async_copy(w3_hbm.at[blk_ds(blk), :], wb.at[slot], dsem.at[0, slot]),
                  pltpu.make_async_copy(u2_hbm.at[:, blk_ds(blk)], ub.at[slot], dsem.at[1, slot]))),
                (jnp.logical_and(n >= 16, n < 24),
                 (pltpu.make_async_copy(da_hbm.at[blk], db.at[slot], dsem.at[0, slot]),
                  pltpu.make_async_copy(u2_hbm.at[:, blk_ds(blk)], ub.at[slot], dsem.at[1, slot]))),
                (jnp.logical_and(n >= 24, n < 32),
                 (pltpu.make_async_copy(w2_hbm.at[blk_ds(blk), :], wb.at[slot], dsem.at[0, slot]),
                  pltpu.make_async_copy(u1_hbm.at[:, blk_ds(blk)], ub.at[slot], dsem.at[1, slot]))),
                (jnp.logical_and(n >= 32, n < 40),
                 (pltpu.make_async_copy(da_hbm.at[blk], db.at[slot], dsem.at[0, slot]),
                  pltpu.make_async_copy(u1_hbm.at[:, blk_ds(blk)], ub.at[slot], dsem.at[1, slot]))))

    def da_write(n):
        return pltpu.make_async_copy(db.at[n % 2], da_hbm.at[n % 8], dasem.at[n % 2])

    def start_streams(n):
        for cond, cps in streams(n):
            pl.when(cond)(functools.partial(start_all, cps))

    def wait_streams(n, which):
        wait_all(streams(n)[which][1])

    def part_writes(n):
        g = jnp.where(n < 8, 2 * n, 2 * n - 16)
        return tuple(pltpu.make_async_copy(ps.at[:, pl.ds(h * LANE, LANE)], part_hbm.at[g + h], psem.at[h])
                     for h in range(2))

    def part_writes_one(n):
        tile = 2 * (n - 32)
        return tuple(pltpu.make_async_copy(ps.at[rds((n % 2) * 512, 512), pl.ds(h * LANE, LANE)],
                                           part_hbm.at[32 + (tile + h) // 4, rds(((tile + h) % 4) * 512, 512)],
                                           psem.at[2 * (n % 2) + h]) for h in range(2))

    def loop_tiles(count, fn):
        def step(m, carry):
            fn(pl.ds(pl.multiple_of(m * TILE, TILE), TILE))
            return carry
        lax.fori_loop(0, count, step, 0)

    def nt(a, b):
        return lax.dot_general(a, b, (((1,), (1,)), ((), ())), preferred_element_type=F32)

    def piece_dz(n):
        slot, col = n % 2, blk_ds(n % 8)
        wait_streams(n, 0)
        start_streams(n + 1)

        def tile(r):
            rp = jnp.dot(buf_a[r, :], sb[slot], preferred_element_type=F32)
            zd = buf_a[r, col].astype(F32) - zb[slot, r, :].astype(F32)
            dz = (2.0 / (all_rows - 1)) * (rp - mp_ref[:, col]) + (2.0 * INV_WEIGHT / all_rows) * zd
            buf_c[r, col] = dz.astype(BF16)
            lacc[...] += jnp.sum(zd * zd, axis=0, keepdims=True)
        loop_tiles(rows // TILE, tile)

        @pl.when(n == 0)
        def _():
            big(1).wait()

        def grad(r):
            ps[r, :] = jnp.dot(buf_b[r, :], buf_c[:, col], preferred_element_type=F32)
        loop_tiles(dim // TILE, grad)
        start_all(part_writes(n))

    def normed(r, vec_ref, col, slot):
        return (ub[slot, r, :] - vec_ref[0:1, col]) * vec_ref[1:2, col]

    def piece_stats(n, d_ref, vec_ref, layer, which):
        slot, col = n % 2, blk_ds(n % 8)
        wait_streams(n, which)

        @pl.when(n % 8 != 7)
        def _():
            start_streams(n + 1)

        @pl.when(n % 8 >= 2)
        def _():
            da_write(n - 2).wait()
        st[layer, 0:2, col] = jnp.zeros((2, BLK), F32)

        def tile(r):
            dx = nt(d_ref[r, :], wb[slot])
            nrm = normed(r, vec_ref, col, slot)
            da = jnp.where(vec_ref[2:3, col] * nrm + vec_ref[3:4, col] > 0.0, dx, 0.0)
            db[slot, r, :] = da
            st[layer, 0:1, col] += jnp.sum(da, axis=0, keepdims=True)
            st[layer, 1:2, col] += jnp.sum(da * nrm, axis=0, keepdims=True)
        loop_tiles(rows // TILE, tile)
        da_write(n).start()

        @pl.when(n % 8 == 7)
        def _():
            da_write(n - 1).wait()
            da_write(n).wait()
            start_streams(n + 1)

    def piece_du(n, vec_ref, layer, which, du_ref):
        slot, col = n % 2, blk_ds(n % 8)
        wait_streams(n, which)
        start_streams(n + 1)
        scale = vec_ref[1:2, col] * vec_ref[2:3, col]
        mean_da, mean_dan = tot[layer, 0:1, col] / all_rows, tot[layer, 1:2, col] / all_rows

        def tile(r):
            nrm = normed(r, vec_ref, col, slot)
            du_ref[r, col] = (scale * (db[slot, r, :] - mean_da - nrm * mean_dan)).astype(BF16)
        loop_tiles(rows // TILE, tile)
        return col

    def stat_copies(layer):
        return tuple(remote(st.at[layer], sr.at[layer, idx], tsend.at[layer, d - 1], trecv.at[layer, d - 1], peer(d))
                     for d in range(1, 8))

    def send_stats(layer):
        start_all(stat_copies(layer))

    def finish_stats(layer):
        wait_all(stat_copies(layer))
        sr[layer, idx] = st[layer]
        va = (sr[layer, 0] + sr[layer, 2]) + (sr[layer, 4] + sr[layer, 6])
        vb = (sr[layer, 1] + sr[layer, 3]) + (sr[layer, 5] + sr[layer, 7])
        tot[layer] = jnp.where(c == 0, va, vb)
        grads_ref[layer] = va + vb

    def big(i):
        src = (z_hbm, x2t_hbm, x1t_hbm)[i]
        return pltpu.make_async_copy(src, (buf_a, buf_b, buf_a)[i], bsem.at[i])

    big(0).start()
    start_streams(0)
    ht_copy = pltpu.make_async_copy(ht_hbm, ht, bsem.at[3])
    lacc[...] = jnp.zeros_like(lacc)
    st[...] = jnp.zeros_like(st)
    meet([peer(d) for d in range(1, 8)])
    big(0).wait()
    big(1).start()
    ht_copy.start()

    def dz_at(t):
        return (jnp.logical_or(jnp.logical_or(t == 0, t == 2), jnp.logical_or(t == 4, jnp.logical_and(t >= 6, t < 11))),
                jnp.where(t < 6, t // 2, t - 3))

    def tick(it, carry):
        k = it - 1
        stage(k - 6 * LAG, lambda g: wait_all(a0(g)))
        stage(k - 5 * LAG, to_a0)
        stage(k - 4 * LAG, to_a2)
        stage(k - 3 * LAG, to_a1)
        stage(k - 2 * LAG, to_s2)
        stage(k - LAG, to_s1)

        wrote_dz, dz_piece = dz_at(it - 1)

        @pl.when(wrote_dz)
        def _():
            wait_all(part_writes(dz_piece))

        @pl.when(jnp.logical_and(it >= 17, it <= 24))
        def _():
            wait_all(part_writes(it - 1))

        @pl.when(jnp.logical_and(it >= 33, it <= 36))
        def _():
            wait_all(part_writes_one(2 * it - 34))
            wait_all(part_writes_one(2 * it - 33))

        stage(k, to_s0)

        has_dz, dz_now = dz_at(it)

        @pl.when(has_dz)
        def _():
            piece_dz(dz_now)

        @pl.when(jnp.logical_and(it >= 11, it < 16))
        def _():
            @pl.when(it == 11)
            def _():
                big(2).start()

            twice = it < 14
            first = jnp.where(it < 14, 2 * it - 14, it)

            def step(n, carry):
                piece_stats(n, buf_c, vec2_ref, 0, 1)
                return carry
            lax.fori_loop(first, first + jnp.where(twice, 2, 1), step, 0)

            @pl.when(it == 15)
            def _():
                st[0, 2:3, 0:BLK] = lossv_ref[...] + lacc[...] * (0.5 * INV_WEIGHT / all_rows)
                send_stats(0)

        @pl.when(jnp.logical_and(it >= 16, it < 24))
        def _():
            @pl.when(it == 16)
            def _():
                finish_stats(0)
                loss_ref[...] = jnp.broadcast_to(jnp.sum(grads_ref[0, 2:3, 0:BLK], axis=1, keepdims=True),
                                                 loss_ref.shape)
                big(2).wait()
                ht_copy.wait()

            col = piece_du(it, vec2_ref, 0, 2, buf_b)

            def grad(r):
                ps[r, :] = jnp.dot(buf_a[r, :], buf_b[:, col], preferred_element_type=F32)
            loop_tiles(dim // TILE, grad)
            start_all(part_writes(it))

        @pl.when(jnp.logical_and(it >= 24, it < 32))
        def _():
            piece_stats(it, buf_b, vec1_ref, 1, 3)

            @pl.when(it == 31)
            def _():
                send_stats(1)

        @pl.when(jnp.logical_and(it >= 32, it < 36))
        def _():
            @pl.when(it == 32)
            def _():
                finish_stats(1)

            def two(m, carry):
                n = 2 * it - 32 + m
                col = piece_du(n, vec1_ref, 1, 4, buf_c)
                ps[rds((n % 2) * 512, 512), :] = jnp.dot(ht[...], buf_c[:, col], preferred_element_type=F32)
                start_all(part_writes_one(n))
                return carry
            lax.fori_loop(0, 2, two, 0)

        return carry

    lax.fori_loop(0, GROUPS + 1 + 6 * LAG, tick, 0)


def backward(z, zo, gh, x2t, x1t, ht, w3, w2, u2, u1, mp, vec2, vec1, lossv, all_rows):
    rows, dim = z.shape
    feat = ht.shape[0]
    hbm = pl.BlockSpec(memory_space=pl.ANY)
    vmem = pl.BlockSpec(memory_space=pltpu.VMEM)
    dma = pltpu.SemaphoreType.DMA
    return pl.pallas_call(
        functools.partial(backward_kernel, all_rows),
        out_shape=(jax.ShapeDtypeStruct((GROUPS, dim, LANE), F32), jax.ShapeDtypeStruct((GROUPS, dim, LANE), F32),
                   jax.ShapeDtypeStruct((8, rows, BLK), F32),
                   jax.ShapeDtypeStruct((2, 4, dim), F32), jax.ShapeDtypeStruct((1, LANE), F32)),
        in_specs=[hbm] * 10 + [vmem] * 4,
        out_specs=(hbm, hbm, hbm, vmem, vmem),
        scratch_shapes=[
            pltpu.VMEM((rows, dim), BF16), pltpu.VMEM((rows, dim), BF16), pltpu.VMEM((rows, dim), BF16),
            pltpu.VMEM((feat, rows), BF16),
            pltpu.VMEM((2, dim, BLK), BF16), pltpu.VMEM((2, BLK, dim), BF16), pltpu.VMEM((2, rows, BLK), BF16),
            pltpu.VMEM((2, rows, BLK), F32), pltpu.VMEM((2, rows, BLK), F32), pltpu.VMEM((dim, BLK), F32),
            pltpu.VMEM((SLOTS, 1024, LANE), F32), pltpu.VMEM((SLOTS, 1024, LANE), F32),
            pltpu.VMEM((2, SLOTS, 256, LANE), F32), pltpu.VMEM((2, SLOTS, 128, LANE), F32),
            pltpu.VMEM((2, 4, dim), F32), pltpu.VMEM((2, 8, 4, dim), F32), pltpu.VMEM((2, 4, dim), F32),
            pltpu.VMEM((1, BLK), F32),
            dma((10, SLOTS)), dma((10, SLOTS)), dma((3, SLOTS)), dma((2, 2)), dma((4,)), dma((4,)), dma((2,)),
            dma((2, 7)), dma((2, 7)),
        ],
        compiler_params=pltpu.CompilerParams(collective_id=2, has_side_effects=True, vmem_limit_bytes=67043328),
        cost_estimate=pl.CostEstimate(flops=150 * 10 ** 9, bytes_accessed=200 << 20, transcendentals=0),
    )(z, zo, gh, x2t, x1t, ht, w3, w2, u2, u1, mp, vec2, vec1, lossv)


RING = 24
AHEAD = 14


def join_kernel(groups, w1_out, w2_out, w3_out, buf, lsem, ssem):
    def load(g):
        return pltpu.make_async_copy(groups.at[g], buf.at[g % RING], lsem.at[g % RING])

    def stores(g):
        k = g % RING
        if g < 32:
            out = (w3_out, w2_out)[g // 16]
            return [pltpu.make_async_copy(buf.at[k], out.at[:, pl.ds((g % 16) * LANE, LANE)], ssem.at[k, 0])]
        return [pltpu.make_async_copy(buf.at[k, pl.ds(i * 512, 512)],
                                      w1_out.at[:, pl.ds(((g - 32) * 4 + i) * LANE, LANE)], ssem.at[k, i])
                for i in range(4)]

    for g in range(AHEAD):
        load(g).start()
    for g in range(GROUPS):
        load(g).wait()
        for cp in stores(g):
            cp.start()
        n = g + AHEAD
        if n < GROUPS:
            if n >= RING:
                for cp in stores(n - RING):
                    cp.wait()
            load(n).start()
    for g in range(GROUPS - RING, GROUPS):
        for cp in stores(g):
            cp.wait()


def join(groups, dim):
    hbm = pl.BlockSpec(memory_space=pl.ANY)
    return pl.pallas_call(
        join_kernel,
        out_shape=(jax.ShapeDtypeStruct((512, dim), F32), jax.ShapeDtypeStruct((dim, dim), F32),
                   jax.ShapeDtypeStruct((dim, dim), F32)),
        in_specs=[hbm],
        out_specs=(hbm, hbm, hbm),
        scratch_shapes=[pltpu.VMEM((RING, dim, LANE), F32), pltpu.SemaphoreType.DMA((RING,)),
                        pltpu.SemaphoreType.DMA((RING, 4))],
        compiler_params=pltpu.CompilerParams(vmem_limit_bytes=40 << 20),
        cost_estimate=pl.CostEstimate(flops=0, bytes_accessed=8 * GROUPS * dim * LANE, transcendentals=0),
    )(groups)


def solution(mesh):
    group_devs = mesh.shape['data']

    def local_step(h_a, h_b, w_one, w_two, w_three, gain_one, bias_one, gain_two, bias_two):
        all_rows = h_a.shape[0] * group_devs
        dim = w_two.shape[0]
        vec = jnp.stack([gain_one, bias_one, gain_two, bias_two])
        (u1, _, u2, z, z_other, g_hat, x2t, x1t, ht, stat1, stat2, mean_part, loss_vec) = front(
            h_a, h_b, w_one, w_two, w_three, vec, all_rows)
        groups, _, _, grads, loss = backward(z, z_other, g_hat, x2t, x1t, ht, w_three, w_two, u2, u1, mean_part, stat2,
                                          stat1, loss_vec, all_rows)
        d_w1, d_w2, d_w3 = join(groups, dim)
        return (loss[0, 0], d_w1, d_w2, d_w3,
                grads[1, 1], grads[1, 0], grads[0, 1], grads[0, 0])

    row_spec = P('data', None)
    return jax.shard_map(local_step, mesh=mesh,
                         in_specs=(row_spec, row_spec, P(), P(), P(), P(), P(), P(), P()),
                         out_specs=(P(), P(), P(), P(), P(), P(), P(), P()),
                         check_vma=False)
```
